32 devices in a mesh: groups: 2 (over y), dp: 4 (over z), tensor: 4 (over x, core).
Axes of the slice: x: 2, y: 2, z: 4, core: 2. Of those that a mesh axis runs over, the one named last changes fastest.
Arguments:
- patches: bfloat16 [8192, 1280], P(('groups', 'dp')), parts along dimension 0, may hold values from -64 to 64
- grids: int32 [8, 2], P(('groups', 'dp')), parts along dimension 0, may hold values from 16 to 32, as said below
- dest: int32 [8, 256], P(('groups', 'dp')), parts along dimension 0, may hold values from 0 to 1535, as said below
- norm_gain: float32 [1280], replicated, may hold values from 0.1 to 1.9
- qkv_weight: bfloat16 [3, 1280, 1280], P(None, None, 'tensor'), may hold values from -8 to 8
- qkv_bias: float32 [3, 1280], P(None, 'tensor'), may hold values from -3 to 3
- proj_weight: bfloat16 [1280, 1280], P('tensor'), may hold values from -0.15625 to 0.15625
- proj_bias: float32 [1280], replicated, may hold values from -3 to 3
- merge_gain: float32 [1280], replicated, may hold values from 0.1 to 1.9
- w_first: bfloat16 [5120, 5120], P('dp', 'tensor'), may hold values from -0.078125 to 0.078125
- b_first: float32 [5120], P('tensor'), may hold values from -3 to 3
- w_second: bfloat16 [5120, 8192], P('tensor', 'dp'), may hold values from -0.078125 to 0.078125
- b_second: float32 [8192], P('tensor'), may hold values from -3 to 3
- text_embed: bfloat16 [3072, 8192], P(('groups', 'dp'), 'tensor'), parts along dimension 0, may hold values from -6 to 6
Outputs:
- sequence: bfloat16 [3072, 8192], P(('groups', 'dp'), 'tensor'), parts along dimension 0
The draws below stay inside these ranges and needn't reach their ends.
There are 2 independent parts, one for each index of `groups`. The reference program is written for one: setup_inputs(seed, part) draws one part's arguments, and reference() takes and returns one part's arrays. A program takes and returns all parts, laid end to end along the dimension named above; an argument that names none is the same for every part. Nothing has to cross between parts.
Inputs may be any that keep to these rules, and one draw needn't show every extreme that they name: `grids`: both sides of every grid are even, at least 16 and at most 32; in each part along `groups`, the first image (the one on dp index 0) has the full 32 x 32 grid. The rows dest[i, j] with j < grids[i, 0] * grids[i, 1] / 4 are distinct over all images; the live rows of one image reach at most 64 rows in each aligned block of 384 sequence rows, and exactly that many for a full grid.
All inputs are finite; a program needn't handle non-finite values.
Results may differ from the reference program's by a relative error of at most 0.014.
Values may be sent and summed in bfloat16 or wider, within the bound.
A program may use at most 128 MiB of HBM per device.

```python
import math
import jax
import jax.numpy as jnp
from jax import lax

V = 1280
HEADS = 16
HEAD_DIM = 80
D_LM = 8192
SIDE = 32
IMG_DEV = 1
IMAGES = 4
PATCHES = 1024
MERGED = 256
MERGE_W = 5120
ROWS = 4096
VIS = 1024
GAP = 128
SEQ_DP = 384
SEQ = 1536
BLOCK = 64
N_DP = 4
N_TENSOR = 4


def layout_helper(key):
    base = jax.random.fold_in(key, 4711)
    side_key, offset_key, order_key = jax.random.split(base, 3)
    halves = jax.random.randint(side_key, (IMAGES, 2), SIDE // 4, SIDE // 2 + 1)
    forced = jnp.arange(IMAGES)[:, None] < IMG_DEV
    halves = jnp.where(forced, SIDE // 2, halves)
    grid_sides = (2 * halves).astype(jnp.int32)
    offsets = jax.random.randint(offset_key, (IMAGES,), 0, GAP + 1)
    regions = jax.random.permutation(order_key, IMAGES)
    starts = regions * (MERGED + GAP) + offsets
    positions = starts[:, None] + jnp.arange(MERGED)[None, :]
    block_index = positions // BLOCK
    shard_index = block_index % N_DP
    local_row = block_index // N_DP * BLOCK + positions % BLOCK
    rows_out = (shard_index * SEQ_DP + local_row).astype(jnp.int32)
    return (grid_sides, rows_out)


def draw_grids(key, part):
    return layout_helper(key)[0]


def draw_dest(key, part):
    return layout_helper(key)[1]


def draw_patches(key, part):
    base_key = jax.random.fold_in(jax.random.fold_in(key, 31), 0)
    values = jax.random.normal(base_key, (ROWS, V), jnp.float32)
    return jnp.clip(values, -64.0, 64.0).astype(jnp.bfloat16)


def draw_qkv_weight(key, part):
    base_key = jax.random.fold_in(jax.random.fold_in(key, 57), 0)
    values = jax.random.normal(base_key, (3, V, V), jnp.float32) * V ** (-0.5)
    return jnp.clip(values, -8.0, 8.0).astype(jnp.bfloat16)


def levels(own_key, extent, pieces, low, top_value):
    def one(axis_at, parts):
        heights = jax.random.uniform(jax.random.fold_in(jax.random.fold_in(own_key, 6), axis_at), (parts,), jnp.float32, low / len(pieces), top_value / len(pieces))
        return jnp.repeat(jnp.exp(heights), extent[axis_at] // parts).reshape((-1,) + (1,) * (len(extent) - axis_at - 1))

    level = one(*pieces[0])
    for cut in pieces[1:]:
        level = level * one(*cut)
    return level


def centred(key, dims, spread, limit, shards=(), kind=jnp.bfloat16):
    result = spread * jax.random.normal(key, dims, jnp.float32)
    if shards:
        result = result * levels(key, dims, shards, -0.22, 0.18)
    return jnp.clip(result, -limit, limit).astype(kind)


def setup_inputs(seed: int = 0, part: int = 0) -> dict:
    key_list = jax.random.split(jax.random.key(seed), 15)
    part_splits = jax.random.split(jax.random.fold_in(key_list[14], part), 15)
    patches = draw_patches(jax.random.fold_in(jax.random.fold_in(key_list[14], part), 71), part)
    grids = draw_grids(jax.random.fold_in(jax.random.fold_in(key_list[14], part), 71), part)
    dest = draw_dest(jax.random.fold_in(jax.random.fold_in(key_list[14], part), 71), part)
    norm_gain = jnp.clip(1.0 + 0.18 * jax.random.normal(key_list[3], (V,), jnp.float32), 0.1, 1.9)
    qkv_weight = draw_qkv_weight(jax.random.fold_in(key_list[14], 71), part)
    qkv_bias = centred(key_list[5], (3, V), 0.5, 3.0, ((1, 4),), jnp.float32)
    proj_weight = centred(key_list[6], (V, V), V ** -0.5, 0.15625, ((0, 4),))
    proj_bias = centred(key_list[7], (V,), 0.5, 3.0, (), jnp.float32)
    merge_gain = jnp.clip(1.0 + 0.18 * jax.random.normal(key_list[8], (V,), jnp.float32), 0.1, 1.9)
    w_first = centred(key_list[9], (MERGE_W, MERGE_W), MERGE_W ** -0.5, 0.078125, ((0, 4), (1, 4)))
    b_first = centred(key_list[10], (MERGE_W,), 0.5, 3.0, ((0, 4),), jnp.float32)
    w_second = centred(key_list[11], (MERGE_W, D_LM), MERGE_W ** -0.5, 0.078125, ((0, 4), (1, 4)))
    b_second = centred(key_list[12], (D_LM,), 0.5, 3.0, ((0, 4),), jnp.float32)
    text_embed = centred(part_splits[13], (SEQ, D_LM), 1.0, 6.0, ((0, 4), (1, 4)))
    return dict(patches=patches, grids=grids, dest=dest, norm_gain=norm_gain, qkv_weight=qkv_weight, qkv_bias=qkv_bias, proj_weight=proj_weight, proj_bias=proj_bias, merge_gain=merge_gain, w_first=w_first, b_first=b_first, w_second=w_second, b_second=b_second, text_embed=text_embed)


def rms_scale(values, gain):
    return values * lax.rsqrt(lax.optimization_barrier(jnp.mean(values * values, axis=-1, keepdims=True)) + 1e-06) * gain

def reference(patches, grids, dest, norm_gain, qkv_weight, qkv_bias, proj_weight, proj_bias, merge_gain, w_first, b_first, w_second, b_second, text_embed):
    live_count = grids[:, 0] * grids[:, 1]
    image_rows = patches.reshape(IMAGES, PATCHES, V)

    def encode(image_item):
        rows_in, count_in = image_item
        normed = rms_scale(rows_in.astype(jnp.float32), norm_gain).astype(jnp.bfloat16)
        projected = jnp.einsum('rv,jvc->jrc', normed.astype(jnp.float32), qkv_weight.astype(jnp.float32)) + qkv_bias[:, None, :]
        projected = projected.astype(jnp.bfloat16).reshape(3, PATCHES, HEADS, HEAD_DIM)
        queries = projected[0].astype(jnp.float32)
        key_rows = projected[1].astype(jnp.float32)
        value_rows = projected[2].astype(jnp.float32)
        scores = jnp.einsum('qhd,khd->hqk', queries, key_rows) / math.sqrt(HEAD_DIM)
        live_keys = jnp.arange(PATCHES, dtype=jnp.int32) < count_in
        scores = jnp.where(live_keys[None, None, :], scores, jnp.float32(-1e+30))
        peak_score = lax.optimization_barrier(jnp.max(scores, axis=-1, keepdims=True))
        exponent = jnp.exp(scores - peak_score)
        weights = (exponent / lax.optimization_barrier(jnp.sum(exponent, axis=-1, keepdims=True))).astype(jnp.bfloat16)
        attended = jnp.einsum('hqk,khd->qhd', weights.astype(jnp.float32), value_rows)
        return attended.astype(jnp.bfloat16).reshape(PATCHES, V)
    attended = lax.map(encode, (image_rows, live_count)).reshape(ROWS, V)
    group_width = V // N_TENSOR
    summed = jnp.zeros((ROWS, V), jnp.float32)
    for group in range(N_TENSOR):
        part_rows = jnp.dot(attended[:, group * group_width:(group + 1) * group_width], proj_weight[group * group_width:(group + 1) * group_width], preferred_element_type=jnp.float32)
        summed = summed + part_rows.astype(jnp.bfloat16).astype(jnp.float32)
    resid = patches.astype(jnp.float32) + summed + proj_bias
    merged_in = rms_scale(resid, merge_gain).astype(jnp.bfloat16).reshape(VIS, MERGE_W)
    first_out = jnp.dot(merged_in, w_first, preferred_element_type=jnp.float32) + b_first
    hidden = jax.nn.gelu(first_out, approximate=False).astype(jnp.bfloat16)
    hidden_width = MERGE_W // N_TENSOR
    visual = jnp.zeros((VIS, D_LM), jnp.float32)
    for group in range(N_TENSOR):
        second_rows = jnp.dot(hidden[:, group * hidden_width:(group + 1) * hidden_width], w_second[group * hidden_width:(group + 1) * hidden_width], preferred_element_type=jnp.float32)
        visual = visual + second_rows.astype(jnp.bfloat16).astype(jnp.float32)
    visual = (visual + b_second).astype(jnp.bfloat16)
    live_rows = jnp.arange(MERGED, dtype=jnp.int32)[None, :] < (live_count // 4)[:, None]
    target = jnp.where(live_rows, dest, SEQ).astype(jnp.int32).reshape(VIS)
    sequence = text_embed.at[target].set(visual, mode='drop')
    return sequence
```

```python
import functools
import math

import jax
import jax.numpy as jnp
from jax import lax
from jax.experimental import pallas as pl
from jax.experimental.pallas import tpu as pltpu
from jax.sharding import PartitionSpec as P

MESH = pl.DeviceIdType.MESH

HEAD_DIM = 80
PATCHES = 1024
MERGED = 256


def rms_scale(values, gain):
    return values * lax.rsqrt(jnp.mean(values * values, axis=-1, keepdims=True) + 1e-06) * gain


def placement(dest, live_count, dp_count, seq_rows, capacity):
    merged_dev = dest.size
    live_rows = (jnp.arange(MERGED, dtype=jnp.int32)[None, :] < (live_count // 4)[:, None]).reshape(merged_dev)
    dest_flat = dest.reshape(merged_dev)
    shard_id = jnp.where(live_rows, dest_flat // seq_rows, dp_count)
    local_row = dest_flat % seq_rows
    index = jnp.arange(merged_dev, dtype=jnp.int32)
    earlier = (shard_id[:, None] == shard_id[None, :]) & (index[None, :] < index[:, None])
    rank = jnp.sum(earlier.astype(jnp.int32), axis=1)
    slot = jnp.where(live_rows & (rank < capacity), shard_id * capacity + rank, -1)
    hit = jnp.arange(dp_count * capacity, dtype=jnp.int32)[:, None] == slot[None, :]
    rows = jnp.max(jnp.where(hit, local_row[None, :], -1), axis=1)
    return hit.astype(jnp.bfloat16), rows


def attention(patches, live_count, norm_gain, qkv_weight, qkv_bias, images_dev, heads_dev):
    normed = rms_scale(patches.astype(jnp.float32), norm_gain).astype(jnp.bfloat16)
    projected = (
        jnp.einsum("rv,jvc->jrc", normed, qkv_weight, preferred_element_type=jnp.float32)
        + qkv_bias[:, None, :]
    )
    projected = projected.astype(jnp.bfloat16).reshape(3, images_dev, PATCHES, heads_dev, HEAD_DIM)
    scores = jnp.einsum(
        "iqhd,ikhd->ihqk", projected[0], projected[1], preferred_element_type=jnp.float32
    ) / math.sqrt(HEAD_DIM)
    live_keys = jnp.arange(PATCHES, dtype=jnp.int32)[None, :] < live_count[:, None]
    scores = jnp.where(live_keys[:, None, None, :], scores, jnp.float32(-1e30))
    peak_score = jnp.max(scores, axis=-1, keepdims=True)
    exponent = jnp.exp(scores - peak_score)
    weights = (exponent / jnp.sum(exponent, axis=-1, keepdims=True)).astype(jnp.bfloat16)
    attended = jnp.einsum(
        "ihqk,ikhd->iqhd", weights, projected[2], preferred_element_type=jnp.float32
    )
    return attended.astype(jnp.bfloat16).reshape(patches.shape[0], heads_dev * HEAD_DIM)


def merger_kernel(
    n, x_hbm, w1_hbm, bias, permute, w2_hbm, out_hbm,
    x, w1, w2, part, from_left, from_right, total, slots, acc, out,
    load_sem, sum_send, sum_recv, hid_send, hid_recv,
):
    chunks, _, block, wide = part.shape
    me = lax.axis_index("dp")
    left, right = lax.max(me - 1, 0), lax.min(me + 1, n - 1)
    has_left, has_right = me > 0, me < n - 1
    inner = has_left & has_right

    loads = [
        pltpu.make_async_copy(a, b, load_sem.at[i])
        for i, (a, b) in enumerate(((x_hbm, x), (w1_hbm, w1), (w2_hbm, w2)))
    ]
    for load in loads:
        load.start()

    barrier = pltpu.get_barrier_semaphore()

    @pl.when(has_left)
    def _():
        pl.semaphore_signal(barrier, inc=1, device_id={"dp": left}, device_id_type=MESH)

    @pl.when(has_right)
    def _():
        pl.semaphore_signal(barrier, inc=1, device_id={"dp": right}, device_id_type=MESH)

    pl.semaphore_wait(barrier, has_left.astype(jnp.int32) + has_right.astype(jnp.int32))

    def sum_right(c, b):
        return pltpu.make_async_remote_copy(
            part.at[c, b], from_left.at[c, b], sum_send.at[0, c, b], sum_recv.at[0, c, b],
            device_id={"dp": right}, device_id_type=MESH)

    def sum_left(c, b):
        return pltpu.make_async_remote_copy(
            part.at[c, b], from_right.at[c, b], sum_send.at[1, c, b], sum_recv.at[1, c, b],
            device_id={"dp": left}, device_id_type=MESH)

    def hid_right(c, b):
        return pltpu.make_async_remote_copy(
            slots.at[c, b], slots.at[c, b], hid_send.at[0, c, b], hid_recv.at[0, c, b],
            device_id={"dp": right}, device_id_type=MESH)

    def hid_left(c, b):
        return pltpu.make_async_remote_copy(
            slots.at[c, b], slots.at[c, b], hid_send.at[1, c, b], hid_recv.at[1, c, b],
            device_id={"dp": left}, device_id_type=MESH)

    def first(c):
        columns = pl.ds(pl.multiple_of(c * wide, wide), wide)

        def tile(b):
            part[c, b] = jnp.dot(
                x[pl.ds(pl.multiple_of(b * block, block), block), :], w1[:, columns],
                preferred_element_type=jnp.float32,
            ).astype(jnp.bfloat16)

        def up(i, carry):
            b = n - 1 - i
            tile(b)

            @pl.when((me == 0) & (b > 0))
            def _():
                sum_right(c, b).start()

            return carry

        def down(b, carry):
            tile(b)

            @pl.when((me == n - 1) & (b < n - 1))
            def _():
                sum_left(c, b).start()

            return carry

        @pl.when(me == 0)
        def _():
            lax.fori_loop(0, n, up, 0)

        @pl.when(me > 0)
        def _():
            lax.fori_loop(0, n, down, 0)

    def relay(c):
        def one(i, carry):
            b = n - 1 - i

            @pl.when(inner & (b > me))
            def _():
                sum_right(c, b).wait_recv()
                part[c, b] = (part[c, b].astype(jnp.float32) + from_left[c, b].astype(jnp.float32)).astype(jnp.bfloat16)
                sum_right(c, b).start()

            @pl.when(inner & (i < me))
            def _():
                sum_left(c, i).wait_recv()
                part[c, i] = (part[c, i].astype(jnp.float32) + from_right[c, i].astype(jnp.float32)).astype(jnp.bfloat16)
                sum_left(c, i).start()

            return carry

        lax.fori_loop(0, n, one, 0)

    def activate(c):
        total[...] = part[c, me].astype(jnp.float32) + bias[c]

        @pl.when(has_left)
        def _():
            sum_right(c, me).wait_recv()
            total[...] += from_left[c, me].astype(jnp.float32)

        @pl.when(has_right)
        def _():
            sum_left(c, me).wait_recv()
            total[...] += from_right[c, me].astype(jnp.float32)

        value = total[...]
        hidden = (0.5 * value * (1.0 + lax.erf(value * math.sqrt(0.5)))).astype(jnp.bfloat16)
        slots[c, me] = jnp.dot(permute[...], hidden, preferred_element_type=jnp.float32).astype(jnp.bfloat16)

        @pl.when(has_right)
        def _():
            hid_right(c, me).start()

        @pl.when(has_left)
        def _():
            hid_left(c, me).start()

    def spread(c):
        def one(k, carry):
            before, after = me - k, me + k

            @pl.when(before >= 0)
            def _():
                hid_right(c, before).wait_recv()

                @pl.when(has_right)
                def _():
                    hid_right(c, before).start()

            @pl.when(after < n)
            def _():
                hid_left(c, after).wait_recv()

                @pl.when(has_left)
                def _():
                    hid_left(c, after).start()

            return carry

        lax.fori_loop(1, n, one, 0)

    def second(c):
        depth = pl.ds(pl.multiple_of(c * wide, wide), wide)

        def one(b, carry):
            rows = pl.ds(pl.multiple_of(b * block, block), block)
            more = jnp.dot(slots[c, b], w2[depth, :], preferred_element_type=jnp.float32)

            @pl.when(c == 0)
            def _():
                acc[rows, :] = more

            @pl.when(c > 0)
            def _():
                acc[rows, :] += more

            return carry

        lax.fori_loop(0, n, one, 0)

    loads[0].wait()
    loads[1].wait()
    first(0)
    loads[2].wait()

    def step(s, carry):
        @pl.when(s + 1 < chunks)
        def _():
            first(s + 1)

        @pl.when(s < chunks)
        def _():
            relay(s)

        @pl.when((s >= 1) & (s <= chunks))
        def _():
            activate(s - 1)

        @pl.when(s >= 2)
        def _():
            spread(s - 2)
            second(s - 2)

        return carry

    lax.fori_loop(0, chunks + 2, step, 0)

    def finish(b, carry):
        rows = pl.ds(pl.multiple_of(b * block, block), block)
        out[rows, :] = acc[rows, :].astype(jnp.bfloat16)
        return carry

    lax.fori_loop(0, n, finish, 0)
    store = pltpu.make_async_copy(out, out_hbm, load_sem.at[0])
    store.start()

    def drain(c, carry):
        def one(b, inside):
            @pl.when(has_right & (b > me))
            def _():
                sum_right(c, b).wait_send()

            @pl.when(has_left & (b < me))
            def _():
                sum_left(c, b).wait_send()

            @pl.when(has_right & (b <= me))
            def _():
                hid_right(c, b).wait_send()

            @pl.when(has_left & (b >= me))
            def _():
                hid_left(c, b).wait_send()

            return inside

        return lax.fori_loop(0, n, one, carry)

    lax.fori_loop(0, chunks, drain, 0)
    store.wait()


def merger(x, w1, bias, permute, w2):
    n = lax.axis_size("dp")
    rows, depth = x.shape
    hidden, columns = w2.shape
    block = rows // n
    wide = 256 if hidden % 256 == 0 else 128
    chunks = hidden // wide
    any_space = pl.BlockSpec(memory_space=pl.ANY)
    vmem = pl.BlockSpec(memory_space=pltpu.VMEM)
    stack = pltpu.VMEM((chunks, n, block, wide), jnp.bfloat16)
    return pl.pallas_call(
        functools.partial(merger_kernel, n),
        out_shape=jax.ShapeDtypeStruct((rows, columns), jnp.bfloat16),
        in_specs=[any_space, any_space, vmem, vmem, any_space],
        out_specs=any_space,
        scratch_shapes=[
            pltpu.VMEM((rows, depth), jnp.bfloat16),
            pltpu.VMEM((depth, hidden), jnp.bfloat16),
            pltpu.VMEM((hidden, columns), jnp.bfloat16),
            stack,
            stack,
            stack,
            pltpu.VMEM((block, wide), jnp.float32),
            stack,
            pltpu.VMEM((rows, columns), jnp.float32),
            pltpu.VMEM((rows, columns), jnp.bfloat16),
            pltpu.SemaphoreType.DMA((3,)),
            pltpu.SemaphoreType.DMA((2, chunks, n)),
            pltpu.SemaphoreType.DMA((2, chunks, n)),
            pltpu.SemaphoreType.DMA((2, chunks, n)),
            pltpu.SemaphoreType.DMA((2, chunks, n)),
        ],
        compiler_params=pltpu.CompilerParams(
            collective_id=0, has_side_effects=True, vmem_limit_bytes=60 * 1024 * 1024
        ),
    )(x, w1, bias.reshape(chunks, 1, wide), permute, w2)


def place_kernel(
    n, y, out, half, across_sum, from_across, ready, landed, got,
    mate_send, mate_recv, across_send, across_recv, row_send, row_recv, end_send, end_recv,
):
    quarter = y.shape[3] // 4
    row, me = lax.axis_index("dp"), lax.axis_index("tensor")
    core, side = me % 2, me // 2
    mate, across = side * 2 + 1 - core, (1 - side) * 2 + core

    barrier = pltpu.get_barrier_semaphore()
    for k in range(1, 4):
        pl.semaphore_signal(barrier, inc=1, device_id={"tensor": (me + k) % 4}, device_id_type=MESH)
    for k in range(1, n):
        pl.semaphore_signal(barrier, inc=1, device_id={"dp": (row + k) % n}, device_id_type=MESH)
    pl.semaphore_wait(barrier, 3 + n - 1)

    def piece(index):
        return pl.ds(pl.multiple_of(index * quarter, quarter), quarter)

    def to_mate(i, j):
        return pltpu.make_async_remote_copy(
            y.at[i, :, :, piece((side + j) % 2 * 2 + 1 - core)], half.at[i, j], mate_send.at[i, j], mate_recv.at[i, j],
            device_id={"tensor": mate}, device_id_type=MESH)

    def to_across(i):
        return pltpu.make_async_remote_copy(
            across_sum.at[i], from_across.at[i], across_send.at[i], across_recv.at[i],
            device_id={"tensor": across}, device_id_type=MESH)

    def to_row(i, k):
        other = (row + k) % n
        return pltpu.make_async_remote_copy(
            ready.at[i, other], landed.at[row, i], row_send.at[i, k], row_recv.at[i, k],
            device_id={"dp": other}, device_id_type=MESH)

    def to_end(i, k, block):
        return pltpu.make_async_remote_copy(
            landed.at[block, i], got.at[me, i], end_send.at[i, k], end_recv.at[i, me],
            device_id={"tensor": block}, device_id_type=MESH)

    for i in range(n):
        for j in (1, 0):
            to_mate(i, j).start()

    for i in range(n):
        to_mate(i, 1).wait_recv()
        for s in range(n):
            across_sum[i, s] = (
                y[i, s, :, piece((1 - side) * 2 + core)].astype(jnp.float32) + half[i, 1, s].astype(jnp.float32)
            ).astype(jnp.bfloat16)
        to_across(i).start()

    for i in range(n):
        to_mate(i, 0).wait_recv()
        to_across(i).wait_recv()
        for s in range(n):
            ready[i, s] = (
                y[i, s, :, piece(me)].astype(jnp.float32)
                + half[i, 0, s].astype(jnp.float32)
                + from_across[i, s].astype(jnp.float32)
            ).astype(jnp.bfloat16)
        for k in range(1, n):
            to_row(i, k).start()
        landed[row, i] = ready[i, row]

    for i in range(n):
        for k in range(n):
            block = (row + n - k) % n
            if k:
                to_row(i, k).wait_recv()

            @pl.when(block == me)
            def _():
                got[me, i] = landed[block, i]

            @pl.when(block != me)
            def _():
                to_end(i, k, block).start()

    for i in range(n):
        for k in range(1, 4):
            other = (me + k) % 4
            pltpu.make_async_remote_copy(
                landed.at[0, i], got.at[other, i], end_send.at[i, 0], end_recv.at[i, other],
                device_id={"tensor": other}, device_id_type=MESH).wait_recv()
    for t in range(4):
        out[:, :, t * quarter:(t + 1) * quarter] = got[t]

    for i in range(n):
        for j in range(2):
            to_mate(i, j).wait_send()
        to_across(i).wait_send()
        for k in range(1, n):
            to_row(i, k).wait_send()
        for k in range(n):
            block = (row + n - k) % n

            @pl.when(block != me)
            def _():
                to_end(i, k, block).wait_send()


def place(second):
    n, _, capacity, columns = second.shape
    quarter = columns // 4
    vmem = pl.BlockSpec(memory_space=pltpu.VMEM)
    stack = pltpu.VMEM((n, n, capacity, quarter), jnp.bfloat16)
    return pl.pallas_call(
        functools.partial(place_kernel, n),
        out_shape=jax.ShapeDtypeStruct((n, capacity, columns), jnp.bfloat16),
        in_specs=[vmem],
        out_specs=vmem,
        scratch_shapes=[
            pltpu.VMEM((n, 2, n, capacity, quarter), jnp.bfloat16),
            stack,
            stack,
            stack,
            stack,
            stack,
            pltpu.SemaphoreType.DMA((n, 2)),
            pltpu.SemaphoreType.DMA((n, 2)),
            pltpu.SemaphoreType.DMA((n,)),
            pltpu.SemaphoreType.DMA((n,)),
            pltpu.SemaphoreType.DMA((n, n)),
            pltpu.SemaphoreType.DMA((n, n)),
            pltpu.SemaphoreType.DMA((n, n)),
            pltpu.SemaphoreType.DMA((n, n)),
        ],
        compiler_params=pltpu.CompilerParams(
            collective_id=1, has_side_effects=True, vmem_limit_bytes=40 * 1024 * 1024
        ),
    )(second)


def exchange(second, dp_count, tensor_count, capacity):
    if dp_count == tensor_count == 4 and capacity % 16 == 0 and second.shape[1] % 512 == 0:
        return place(second.reshape(dp_count, dp_count, capacity, -1)).reshape(dp_count * capacity, -1)
    second = lax.psum_scatter(second, "tensor", scatter_dimension=1, tiled=True)
    columns = second.shape[1]
    second = second.reshape(dp_count, dp_count, capacity, columns)
    second = lax.all_to_all(second, "dp", split_axis=1, concat_axis=0, tiled=False)
    blocks = dp_count // tensor_count
    second = second.reshape(tensor_count, blocks, dp_count * capacity, columns)
    second = lax.all_to_all(second, "tensor", split_axis=0, concat_axis=0, tiled=True)
    return second.transpose(2, 1, 0, 3).reshape(dp_count * capacity, -1)


def local(
    patches,
    grids,
    dest,
    norm_gain,
    qkv_weight,
    qkv_bias,
    proj_weight,
    proj_bias,
    merge_gain,
    w_first,
    b_first,
    w_second,
    b_second,
    text_embed,
):
    rows_dev, width = patches.shape
    images_dev = grids.shape[0]
    heads_dev = qkv_weight.shape[2] // HEAD_DIM
    dp_count = lax.axis_size("dp")
    tensor_count = lax.axis_size("tensor")
    seq_rows = text_embed.shape[0]
    capacity = images_dev * (MERGED // dp_count)
    live_count = grids[:, 0] * grids[:, 1]
    permute, slot_rows = placement(dest, live_count, dp_count, seq_rows, capacity)
    arrived_rows = lax.all_to_all(
        slot_rows.reshape(dp_count, capacity), "dp", split_axis=0, concat_axis=0, tiled=True
    ).reshape(-1)

    attended = attention(patches, live_count, norm_gain, qkv_weight, qkv_bias, images_dev, heads_dev)
    partial_value = jnp.dot(attended, proj_weight, preferred_element_type=jnp.float32).astype(jnp.bfloat16)
    summed = lax.psum_scatter(partial_value, "tensor", scatter_dimension=0, tiled=True).astype(jnp.float32)
    part = rows_dev // tensor_count
    own = lax.dynamic_slice_in_dim(patches, lax.axis_index("tensor") * part, part, 0)
    resid = own.astype(jnp.float32) + summed + proj_bias
    merged_in = rms_scale(resid, merge_gain).astype(jnp.bfloat16).reshape(part // 4, 4 * width)
    sliced = lax.all_to_all(
        merged_in.reshape(part // 4, dp_count, 4 * width // dp_count), "dp", split_axis=1, concat_axis=0, tiled=False
    )
    received = lax.all_gather(sliced, "tensor", axis=1, tiled=False)
    received = received.reshape(-1, 4 * width // dp_count)
    second = merger(received, w_first, b_first, permute, w_second)
    visual = exchange(second, dp_count, tensor_count, capacity)
    visual = (visual.astype(jnp.float32) + b_second).astype(jnp.bfloat16)
    hit = jnp.arange(seq_rows, dtype=jnp.int32)[:, None] == arrived_rows[None, :]
    placed = jnp.dot(hit.astype(jnp.bfloat16), visual, preferred_element_type=jnp.float32).astype(jnp.bfloat16)
    return jnp.where(jnp.any(hit, axis=1)[:, None], placed, text_embed)


def encode_kernel(
    seq_rows, patches_hbm, grids, dest, gain, wqkv_hbm, bqkv, wproj_hbm, bproj, mgain, x_out, arrived,
    patches, wqkv, wproj, target, normed, own_rows, qs, ks, vs, att_f32, att_out, att_in, slices, rows_tbl,
    load_sem, tbl_send, tbl_recv, pm_send, pa_send, py_send, pd_send, p_recv, pd_recv,
    att_send, att_recv, z_send, fm_send, fa_send, fx_send, x_recv,
):
    n, _, part, width = x_out.shape
    nt, block, span = att_in.shape
    rows = n * block
    merged = dest.shape[1]
    heads = qs.shape[0]
    half = wproj.shape[1] // 2
    row, me, group = lax.axis_index("dp"), lax.axis_index("tensor"), lax.axis_index("groups")
    core, side = me % 2, me // 2
    mate, across = side * 2 + 1 - core, (1 - side) * 2 + core
    diag = (1 - side) * 2 + 1 - core

    load_x = pltpu.make_async_copy(patches_hbm, patches, load_sem.at[0])
    load_p = pltpu.make_async_copy(wproj_hbm, wproj.at[me], load_sem.at[1])
    load_w = pltpu.make_async_copy(wqkv_hbm, wqkv, load_sem.at[2])
    load_x.start()
    load_p.start()
    load_w.start()

    barrier = pltpu.get_barrier_semaphore()
    for k in range(1, nt):
        pl.semaphore_signal(barrier, inc=1, device_id={"tensor": (me + k) % nt}, device_id_type=MESH)
    for k in range(1, n):
        pl.semaphore_signal(barrier, inc=1, device_id={"dp": (row + k) % n}, device_id_type=MESH)
    pl.semaphore_signal(barrier, inc=1, device_id={"groups": 1 - group}, device_id_type=MESH)
    pl.semaphore_wait(barrier, nt - 1 + n - 1 + 1)

    def remote(source, target_ref, send, recv, device):
        return pltpu.make_async_remote_copy(
            source, target_ref, send, recv, device_id=device, device_id_type=MESH)

    mine = pl.ds(pl.multiple_of(group * half, half), half)
    other = pl.ds(pl.multiple_of((1 - group) * half, half), half)
    proj_mate = remote(wproj.at[me], wproj.at[me], pm_send, p_recv.at[0], {"tensor": mate})
    proj_across = remote(wproj.at[me, mine], wproj.at[me, mine], pa_send, p_recv.at[1], {"tensor": across})
    proj_peer = remote(wproj.at[across, mine], wproj.at[across, mine], py_send, p_recv.at[2], {"groups": 1 - group})
    proj_diag = [
        remote(wproj.at[across, mine], wproj.at[across, mine], pd_send.at[0], pd_recv.at[0], {"tensor": mate}),
        remote(wproj.at[across, other], wproj.at[across, other], pd_send.at[1], pd_recv.at[1], {"tensor": mate}),
    ]
    load_p.wait()
    proj_across.start()
    proj_mate.start()

    live = grids[0, 0] * grids[0, 1]
    dest_row = dest[...].astype(jnp.float32)

    def shards(value):
        total = jnp.zeros_like(value)
        for s in range(1, n):
            total += jnp.where(value >= float(s * seq_rows), 1.0, 0.0)
        return total

    square = (merged, merged)
    first_at = lax.broadcasted_iota(jnp.int32, square, 0)
    second_at = lax.broadcasted_iota(jnp.int32, square, 1)
    dest_col = jnp.sum(jnp.where(first_at == second_at, dest_row, 0.0), axis=1, keepdims=True)
    shard_row, shard_col = shards(dest_row), shards(dest_col)
    rank_col = jnp.sum(
        jnp.where((shard_row == shard_col) & (second_at < first_at), 1.0, 0.0), axis=1, keepdims=True)
    live_col = lax.broadcasted_iota(jnp.int32, (merged, 1), 0) * 4 < live
    lanes = 128
    code_col = jnp.where(live_col, shard_col * lanes + rank_col, -1.0)
    lane_at = lax.broadcasted_iota(jnp.int32, (merged, n * lanes), 1).astype(jnp.float32)
    local_col = dest_col - shard_col * seq_rows
    table = jnp.sum(jnp.where(lane_at == code_col, local_col + 1.0, 0.0), axis=0, keepdims=True) - 1.0
    for s in range(n):
        rows_tbl[s] = jnp.broadcast_to(table[:, s * lanes:(s + 1) * lanes], (8, lanes)).astype(jnp.int32)
    arrived[row] = rows_tbl[row]

    def send_table(k):
        to = (row + k) % n
        return remote(rows_tbl.at[to], arrived.at[row], tbl_send.at[k], tbl_recv.at[row], {"dp": to})

    for k in range(1, n):
        send_table(k).start()

    wide = (merged, rows)
    at_row = lax.broadcasted_iota(jnp.int32, wide, 0)
    at_lane = lax.broadcasted_iota(jnp.int32, wide, 1)
    dest_rep = jnp.sum(jnp.where(at_row == at_lane // 4, dest_col, 0.0), axis=0, keepdims=True)
    shard_rep = shards(dest_rep)
    rank_rep = jnp.sum(
        jnp.where((shard_col == shard_rep) & (at_row < at_lane // 4), 1.0, 0.0), axis=0, keepdims=True)
    piece = part // n
    rank_i, shard_i = rank_rep.astype(jnp.int32), shard_rep.astype(jnp.int32)
    place_i = lax.broadcasted_iota(jnp.int32, (1, rows), 1)
    slot_i = rank_i // piece * block + place_i % 4 * part + shard_i * piece + rank_i % piece
    target[...] = jnp.broadcast_to(jnp.where(place_i < live, slot_i, -1), target.shape)

    load_x.wait()
    load_w.wait()
    lane80 = lax.broadcasted_iota(jnp.int32, (block, qs.shape[2]), 1)

    def project(b, carry):
        at = pl.ds(pl.multiple_of(b * block, block), block)
        hit = jnp.where(
            target[0:1, :] == lax.broadcasted_iota(jnp.int32, (block, rows), 0) + b * block, 1.0, 0.0)
        valid = jnp.sum(hit, axis=1, keepdims=True)
        raw = jnp.dot(hit.astype(jnp.bfloat16), patches[...], preferred_element_type=jnp.float32)

        @pl.when(b == me)
        def _():
            own_rows[...] = raw.astype(jnp.bfloat16)

        normed[...] = rms_scale(raw, gain[...]).astype(jnp.bfloat16)
        for j, store in enumerate((qs, ks, vs)):
            acc = jnp.dot(normed[...], wqkv[j], preferred_element_type=jnp.float32) + bqkv[j:j + 1, :]
            extra = jnp.where(valid > 0.5, 0.0, -1e30) if j == 1 else jnp.ones((block, 1), jnp.float32)
            fill = jnp.where(lane80 == HEAD_DIM, extra, 0.0).astype(jnp.bfloat16)
            for h in range(heads):
                store[h, at, :] = fill
                store[h, at, 0:HEAD_DIM] = acc[:, h * HEAD_DIM:(h + 1) * HEAD_DIM].astype(jnp.bfloat16)
        return carry

    lax.fori_loop(0, n, project, 0)

    proj_across.wait_recv()
    proj_peer.start()
    proj_diag[0].start()

    scale = math.log2(math.e) / math.sqrt(HEAD_DIM)

    def order(it):
        return it % 2 * 2 + it // 2

    def att_to(b):
        return remote(att_out.at[b], att_in.at[me], att_send.at[b], att_recv.at[me], {"tensor": b})

    def z_to(k):
        to = (row + k) % n
        return remote(slices.at[to], x_out.at[me, row], z_send.at[k], x_recv.at[me, row], {"dp": to})

    def to_mate(i):
        return remote(x_out.at[me, i], x_out.at[me, i], fm_send.at[i], x_recv.at[me, i], {"tensor": mate})

    def to_across(i):
        return remote(x_out.at[me, i], x_out.at[me, i], fa_send.at[i], x_recv.at[me, i], {"tensor": across})

    def relay_mate(i):
        return remote(
            x_out.at[across, i], x_out.at[across, i], fx_send.at[i], x_recv.at[across, i], {"tensor": mate})

    def landed(b, i):
        return remote(x_out.at[b, i], x_out.at[b, i], fm_send.at[0], x_recv.at[b, i], {"tensor": mate})

    def attend(it, carry):
        @pl.when(it < n)
        def _():
            b = order(it)
            at = pl.ds(pl.multiple_of(b * block, block), block)
            for h in range(heads):
                scores = lax.dot_general(
                    qs[h, at, :], ks[h], (((1,), (1,)), ((), ())), preferred_element_type=jnp.float32)
                peak = jnp.max(scores, axis=1, keepdims=True)
                weights = jnp.exp2((scores - peak) * scale).astype(jnp.bfloat16)
                mixed = jnp.dot(weights, vs[h], preferred_element_type=jnp.float32)
                mixed = mixed * (1.0 / mixed[:, HEAD_DIM:HEAD_DIM + 1])
                att_f32[:, h * HEAD_DIM:(h + 1) * HEAD_DIM] = mixed[:, 0:HEAD_DIM]
            att_out[b] = att_f32[...].astype(jnp.bfloat16)

            @pl.when(b != me)
            def _():
                att_to(b).start()

            @pl.when(b == me)
            def _():
                att_in[me] = att_f32[...].astype(jnp.bfloat16)

        @pl.when(it == 1)
        def _():
            proj_peer.wait_recv()
            proj_diag[1].start()
            proj_mate.wait_recv()
            for copy in proj_diag:
                copy.wait_recv()

        @pl.when((it >= 1) & (order(lax.max(it, 1) - 1) == me))
        def _():
            for k in range(1, nt):
                source = (me + k) % nt
                remote(att_out.at[0], att_in.at[source], att_send.at[0], att_recv.at[source], {"tensor": mate}).wait_recv()
            total = own_rows[...].astype(jnp.float32) + bproj[...]
            for s in range(nt):
                total += jnp.dot(att_in[s], wproj[s], preferred_element_type=jnp.float32)
            ready = rms_scale(total, mgain[...]).astype(jnp.bfloat16)
            for k in range(n):
                slices[k] = ready[k * part:(k + 1) * part, :]
            for k in range(1, n):
                z_to(k).start()
            x_out[me, row] = slices[row]
            to_across(row).start()
            to_mate(row).start()

        return carry

    lax.fori_loop(0, n + 1, attend, 0)

    for k in range(1, n):
        source = (row + n - k) % n
        landed(me, source).wait_recv()
        to_across(source).start()
        to_mate(source).start()
    for k in range(n):
        source = (row + n - k) % n
        landed(across, source).wait_recv()
        relay_mate(source).start()
    for k in range(n):
        source = (row + n - k) % n
        landed(mate, source).wait_recv()
        landed(diag, source).wait_recv()
    for k in range(1, n):
        source = (row + n - k) % n
        remote(rows_tbl.at[0], arrived.at[source], tbl_send.at[0], tbl_recv.at[source], {"dp": source}).wait_recv()

    proj_mate.wait_send()
    proj_across.wait_send()
    proj_peer.wait_send()
    for copy in proj_diag:
        copy.wait_send()
    for k in range(1, n):
        send_table(k).wait_send()
        z_to(k).wait_send()
        att_to((me + k) % nt).wait_send()
    for i in range(n):
        to_mate(i).wait_send()
        to_across(i).wait_send()
        relay_mate(i).wait_send()


def encode(patches, grids, dest, norm_gain, qkv_weight, qkv_bias, proj_weight, proj_bias, merge_gain, seq_rows):
    n, nt = lax.axis_size("dp"), lax.axis_size("tensor")
    rows, width = patches.shape
    span = qkv_weight.shape[2]
    heads = span // HEAD_DIM
    block = rows // n
    part = block // 4
    any_space = pl.BlockSpec(memory_space=pl.ANY)
    vmem = pl.BlockSpec(memory_space=pltpu.VMEM)
    smem = pl.BlockSpec(memory_space=pltpu.SMEM)
    dma = pltpu.SemaphoreType.DMA
    bf16 = jnp.bfloat16
    return pl.pallas_call(
        functools.partial(encode_kernel, seq_rows),
        out_shape=(
            jax.ShapeDtypeStruct((n, n, part, width), bf16),
            jax.ShapeDtypeStruct((n, 8, 128), jnp.int32),
        ),
        in_specs=[any_space, smem, vmem, vmem, any_space, vmem, any_space, vmem, vmem],
        out_specs=(vmem, vmem),
        scratch_shapes=[
            pltpu.VMEM((rows, width), bf16),
            pltpu.VMEM(qkv_weight.shape, bf16),
            pltpu.VMEM((nt, span, width), bf16),
            pltpu.VMEM((8, rows), jnp.int32),
            pltpu.VMEM((block, width), bf16),
            pltpu.VMEM((block, width), bf16),
            pltpu.VMEM((heads, rows, 128), bf16),
            pltpu.VMEM((heads, rows, 128), bf16),
            pltpu.VMEM((heads, rows, 128), bf16),
            pltpu.VMEM((block, span), jnp.float32),
            pltpu.VMEM((n, block, span), bf16),
            pltpu.VMEM((nt, block, span), bf16),
            pltpu.VMEM((n, part, width), bf16),
            pltpu.VMEM((n, 8, 128), jnp.int32),
            dma((3,)), dma((n,)), dma((n,)), dma, dma, dma, dma((2,)), dma((3,)), dma((2,)),
            dma((n,)), dma((nt,)), dma((n,)), dma((n,)), dma((n,)), dma((n,)), dma((nt, n)),
        ],
        compiler_params=pltpu.CompilerParams(
            collective_id=2, has_side_effects=True, vmem_limit_bytes=60 * 1024 * 1024
        ),
    )(
        patches, grids, dest, norm_gain.reshape(1, -1), qkv_weight, qkv_bias, proj_weight,
        proj_bias.reshape(1, -1), merge_gain.reshape(1, -1),
    )


def merge_kernel(
    lag, x, w1_hbm, bias, w2_hbm, out,
    w1, w2, own, to_r, to_l, from_l, from_r, total, hidden, keep, give, from_mate, cross, from_across, ready, landed,
    load_sem, r_send, r_recv, l_send, l_recv, mate_send, mate_recv, across_send, across_recv,
    row_send, row_recv, end_send, end_recv,
):
    count, block, wide = own.shape
    n, nt = x.shape[0], 4
    pieces = count // n
    quarter = keep.shape[3]
    piece = ready.shape[3]
    row, me = lax.axis_index("dp"), lax.axis_index("tensor")
    core, side = me % 2, me // 2
    mate, across = side * 2 + 1 - core, (1 - side) * 2 + core
    left, right = lax.max(row - 1, 0), lax.min(row + 1, n - 1)
    has_left, has_right = row > 0, row < n - 1

    loads = [
        pltpu.make_async_copy(a, b, load_sem.at[i]) for i, (a, b) in enumerate(((w1_hbm, w1), (w2_hbm, w2)))
    ]
    for load in loads:
        load.start()

    barrier = pltpu.get_barrier_semaphore()
    for k in range(1, nt):
        pl.semaphore_signal(barrier, inc=1, device_id={"tensor": (me + k) % nt}, device_id_type=MESH)
    for k in range(1, n):
        pl.semaphore_signal(barrier, inc=1, device_id={"dp": (row + k) % n}, device_id_type=MESH)
    pl.semaphore_wait(barrier, nt - 1 + n - 1)

    def remote(source, target, send, recv, device):
        return pltpu.make_async_remote_copy(
            source, target, send, recv, device_id=device, device_id_type=MESH)

    def go_right(c):
        return remote(to_r.at[c], from_l.at[c], r_send.at[c], r_recv.at[c], {"dp": right})

    def go_left(c):
        return remote(to_l.at[c], from_r.at[c], l_send.at[c], l_recv.at[c], {"dp": left})

    def first(c):
        columns = pl.ds(pl.multiple_of(c % pieces * wide, wide), wide)
        partial = jnp.dot(
            x[c // pieces].reshape(block, -1), w1[:, columns], preferred_element_type=jnp.float32)
        own[c] = partial

        @pl.when(row == 0)
        def _():
            to_r[c] = partial.astype(jnp.bfloat16)
            go_right(c).start()

        @pl.when(row == n - 1)
        def _():
            to_l[c] = partial.astype(jnp.bfloat16)
            go_left(c).start()

    def relay(stage, c):
        @pl.when(row == stage)
        def _():
            go_right(c).wait_recv()
            to_r[c] = (own[c] + from_l[c].astype(jnp.float32)).astype(jnp.bfloat16)
            go_right(c).start()

        @pl.when(row == n - 1 - stage)
        def _():
            go_left(c).wait_recv()
            to_l[c] = (own[c] + from_r[c].astype(jnp.float32)).astype(jnp.bfloat16)
            go_left(c).start()

    def activate(c):
        total[...] = own[c] + bias[c % pieces]

        @pl.when(row == n - 1)
        def _():
            go_right(c).wait_recv()

        @pl.when(row == 0)
        def _():
            go_left(c).wait_recv()

        @pl.when(has_left)
        def _():
            total[...] += from_l[c].astype(jnp.float32)

        @pl.when(has_right)
        def _():
            total[...] += from_r[c].astype(jnp.float32)

        value = total[...]
        hidden[c % pieces] = (0.5 * value * (1.0 + lax.erf(value * math.sqrt(0.5)))).astype(jnp.bfloat16)

    def columns_of(s, c):
        return pl.ds(pl.multiple_of((s * 2 + c) * quarter, quarter), quarter)

    def to_mate(b, s):
        return remote(give.at[b, s], from_mate.at[b, s], mate_send.at[b, s], mate_recv.at[b, s], {"tensor": mate})

    def to_across(b):
        return remote(cross.at[b], from_across.at[b], across_send.at[b], across_recv.at[b], {"tensor": across})

    def to_row(b, k):
        to = (row + k) % n
        return remote(ready.at[b, to], landed.at[b, row], row_send.at[b, k], row_recv.at[b, row], {"dp": to})

    def mine():
        return pl.ds(pl.multiple_of(me * quarter, quarter), quarter)

    def to_end(b, d):
        return remote(
            landed.at[b, d], out.at[:, b, :, mine()], end_send.at[b, d], end_recv.at[b, me], {"tensor": d})

    def second(b):
        def product(columns):
            acc = jnp.dot(hidden[0], w2[0:wide, columns], preferred_element_type=jnp.float32)
            for j in range(1, pieces):
                acc += jnp.dot(hidden[j], w2[j * wide:(j + 1) * wide, columns], preferred_element_type=jnp.float32)
            return acc

        for s in (1 - side, side):
            give[b, s] = product(columns_of(s, 1 - core)).astype(jnp.bfloat16)
            to_mate(b, s).start()
        for s in (1 - side, side):
            keep[b, s] = product(columns_of(s, core))

    def chip_sum(b):
        to_mate(b, 1 - side).wait_recv()
        cross[b] = (keep[b, 1 - side] + from_mate[b, 1 - side].astype(jnp.float32)).astype(jnp.bfloat16)
        to_across(b).start()

    def spread(b):
        to_mate(b, side).wait_recv()
        to_across(b).wait_recv()
        value = keep[b, side] + from_mate[b, side].astype(jnp.float32) + from_across[b].astype(jnp.float32)
        value = value.astype(jnp.bfloat16)
        for i in range(n):
            for s in range(n):
                at = (i * n + s) * piece
                ready[b, s, i] = value[at:at + piece, :]
        for k in range(1, n):
            to_row(b, k).start()
        landed[b, row] = ready[b, row]

    def deliver(b):
        for k in range(n):
            source = (row + n - k) % n
            if k:
                remote(
                    ready.at[b, 0], landed.at[b, source], row_send.at[b, 0], row_recv.at[b, source], {"dp": left}
                ).wait_recv()

            @pl.when(source == me)
            def _():
                out[:, b, :, mine()] = landed[b, source]

            @pl.when(source != me)
            def _():
                to_end(b, source).start()

    loads[0].wait()
    loads[1].wait()

    ahead = (n - 1) * lag
    after = ((0, second), (1, chip_sum), (3, spread), (5, deliver))

    def step(s, carry):
        @pl.when(s < count)
        def _():
            first(s)

        for stage in range(1, n - 1):
            @pl.when((s >= stage * lag) & (s < count + stage * lag))
            def _():
                relay(stage, s - stage * lag)

        @pl.when((s >= ahead) & (s < count + ahead))
        def _():
            activate(s - ahead)

        for offset, work in after:
            at = s - ahead - offset + 1

            @pl.when((at >= pieces) & (at <= count) & (lax.max(at, 0) % pieces == 0))
            def _():
                work(lax.max(at, pieces) // pieces - 1)

        return carry

    lax.fori_loop(0, count + ahead + 5, step, 0)

    for b in range(n):
        for k in range(1, nt):
            source = (me + k) % nt
            columns = pl.ds(pl.multiple_of(source * quarter, quarter), quarter)
            remote(
                landed.at[b, 0], out.at[:, b, :, columns], end_send.at[b, 0], end_recv.at[b, source], {"tensor": mate}
            ).wait_recv()

    def drain(c, carry):
        @pl.when(has_right)
        def _():
            go_right(c).wait_send()

        @pl.when(has_left)
        def _():
            go_left(c).wait_send()

        return carry

    lax.fori_loop(0, count, drain, 0)
    for b in range(n):
        for s in range(2):
            to_mate(b, s).wait_send()
        to_across(b).wait_send()
        for k in range(1, n):
            to_row(b, k).wait_send()
            to_end(b, (me + k) % nt).wait_send()


def merge(x, w1, bias, w2):
    n, _, part, depth = x.shape
    block = n * part
    hidden, columns = w2.shape
    wide = 256
    pieces = hidden // wide
    count = n * pieces
    quarter = columns // 4
    piece = part // n
    any_space = pl.BlockSpec(memory_space=pl.ANY)
    vmem = pl.BlockSpec(memory_space=pltpu.VMEM)
    dma = pltpu.SemaphoreType.DMA
    bf16, f32 = jnp.bfloat16, jnp.float32
    stack = pltpu.VMEM((count, block, wide), bf16)
    tiles = pltpu.VMEM((n, 2, block, quarter), bf16)
    one = pltpu.VMEM((n, block, quarter), bf16)
    moved = pltpu.VMEM((n, n, n, piece, quarter), bf16)
    return pl.pallas_call(
        functools.partial(merge_kernel, 2),
        out_shape=jax.ShapeDtypeStruct((n, n, piece, columns), bf16),
        in_specs=[vmem, any_space, vmem, any_space],
        out_specs=vmem,
        scratch_shapes=[
            pltpu.VMEM(w1.shape, bf16),
            pltpu.VMEM(w2.shape, bf16),
            pltpu.VMEM((count, block, wide), f32),
            stack, stack, stack, stack,
            pltpu.VMEM((block, wide), f32),
            pltpu.VMEM((pieces, block, wide), bf16),
            pltpu.VMEM((n, 2, block, quarter), f32),
            tiles, tiles, one, one, moved, moved,
            dma((2,)), dma((count,)), dma((count,)), dma((count,)), dma((count,)),
            dma((n, 2)), dma((n, 2)), dma((n,)), dma((n,)), dma((n, n)), dma((n, n)), dma((n, 4)), dma((n, 4)),
        ],
        compiler_params=pltpu.CompilerParams(
            collective_id=3, has_side_effects=True, vmem_limit_bytes=62 * 1024 * 1024
        ),
    )(x, w1, bias.reshape(pieces, 1, wide), w2)


def local_fast(
    patches,
    grids,
    dest,
    norm_gain,
    qkv_weight,
    qkv_bias,
    proj_weight,
    proj_bias,
    merge_gain,
    w_first,
    b_first,
    w_second,
    b_second,
    text_embed,
):
    seq_rows = text_embed.shape[0]
    x, arrived = encode(
        patches, grids, dest, norm_gain, qkv_weight, qkv_bias, proj_weight, proj_bias, merge_gain, seq_rows)
    visual = merge(x, w_first, b_first, w_second)
    capacity = x.shape[2]
    visual = visual.reshape(-1, visual.shape[3])
    arrived_rows = arrived[:, 0, :capacity].reshape(-1)
    visual = (visual.astype(jnp.float32) + b_second).astype(jnp.bfloat16)
    hit = jnp.arange(seq_rows, dtype=jnp.int32)[:, None] == arrived_rows[None, :]
    placed = jnp.dot(hit.astype(jnp.bfloat16), visual, preferred_element_type=jnp.float32).astype(jnp.bfloat16)
    return jnp.where(jnp.any(hit, axis=1)[:, None], placed, text_embed)


def fits(patches, grids, dest, qkv_weight, w_first, w_second):
    n, nt = lax.axis_size("dp"), lax.axis_size("tensor")
    rows, width = patches.shape
    return (
        n == nt == 4
        and lax.axis_size("groups") == 2
        and grids.shape[0] == 1
        and rows == PATCHES
        and dest.shape[1] == MERGED
        and w_first.shape[0] == width
        and w_second.shape[0] % 256 == 0
        and w_second.shape[1] % 512 == 0
        and qkv_weight.shape[2] % 32 == 0
    )


def chosen(*args):
    run = local_fast if fits(args[0], args[1], args[2], args[4], args[9], args[11]) else local
    return run(*args)


def solution(mesh):
    in_specs = (
        P(("groups", "dp"), None),
        P(("groups", "dp"), None),
        P(("groups", "dp"), None),
        P(),
        P(None, None, "tensor"),
        P(None, "tensor"),
        P("tensor", None),
        P(),
        P(),
        P("dp", "tensor"),
        P("tensor"),
        P("tensor", "dp"),
        P("tensor"),
        P(("groups", "dp"), "tensor"),
    )
    out_specs = P(("groups", "dp"), "tensor")
    return jax.shard_map(chosen, mesh=mesh, in_specs=in_specs, out_specs=out_specs, check_vma=False)
```

```python
import functools
import math

import jax
import jax.numpy as jnp
from jax import lax
from jax.experimental import pallas as pl
from jax.experimental.pallas import tpu as pltpu
from jax.sharding import PartitionSpec as P

MESH = pl.DeviceIdType.MESH

HEAD_DIM = 80
PATCHES = 1024
MERGED = 256


def rms_scale(values, gain):
    return values * lax.rsqrt(jnp.mean(values * values, axis=-1, keepdims=True) + 1e-06) * gain


def placement(dest, live_count, dp_count, seq_rows, capacity):
    merged_dev = dest.size
    live_rows = (jnp.arange(MERGED, dtype=jnp.int32)[None, :] < (live_count // 4)[:, None]).reshape(merged_dev)
    dest_flat = dest.reshape(merged_dev)
    shard_id = jnp.where(live_rows, dest_flat // seq_rows, dp_count)
    local_row = dest_flat % seq_rows
    index = jnp.arange(merged_dev, dtype=jnp.int32)
    earlier = (shard_id[:, None] == shard_id[None, :]) & (index[None, :] < index[:, None])
    rank = jnp.sum(earlier.astype(jnp.int32), axis=1)
    slot = jnp.where(live_rows & (rank < capacity), shard_id * capacity + rank, -1)
    hit = jnp.arange(dp_count * capacity, dtype=jnp.int32)[:, None] == slot[None, :]
    rows = jnp.max(jnp.where(hit, local_row[None, :], -1), axis=1)
    return hit.astype(jnp.bfloat16), rows


def attention(patches, live_count, norm_gain, qkv_weight, qkv_bias, images_dev, heads_dev):
    normed = rms_scale(patches.astype(jnp.float32), norm_gain).astype(jnp.bfloat16)
    projected = (
        jnp.einsum("rv,jvc->jrc", normed, qkv_weight, preferred_element_type=jnp.float32)
        + qkv_bias[:, None, :]
    )
    projected = projected.astype(jnp.bfloat16).reshape(3, images_dev, PATCHES, heads_dev, HEAD_DIM)
    scores = jnp.einsum(
        "iqhd,ikhd->ihqk", projected[0], projected[1], preferred_element_type=jnp.float32
    ) / math.sqrt(HEAD_DIM)
    live_keys = jnp.arange(PATCHES, dtype=jnp.int32)[None, :] < live_count[:, None]
    scores = jnp.where(live_keys[:, None, None, :], scores, jnp.float32(-1e30))
    peak_score = jnp.max(scores, axis=-1, keepdims=True)
    exponent = jnp.exp(scores - peak_score)
    weights = (exponent / jnp.sum(exponent, axis=-1, keepdims=True)).astype(jnp.bfloat16)
    attended = jnp.einsum(
        "ihqk,ikhd->iqhd", weights, projected[2], preferred_element_type=jnp.float32
    )
    return attended.astype(jnp.bfloat16).reshape(patches.shape[0], heads_dev * HEAD_DIM)


def merger_kernel(
    n, x_hbm, w1_hbm, bias, permute, w2_hbm, out_hbm,
    x, w1, w2, part, from_left, from_right, total, slots, acc, out,
    load_sem, sum_send, sum_recv, hid_send, hid_recv,
):
    chunks, _, block, wide = part.shape
    me = lax.axis_index("dp")
    left, right = lax.max(me - 1, 0), lax.min(me + 1, n - 1)
    has_left, has_right = me > 0, me < n - 1
    inner = has_left & has_right

    loads = [
        pltpu.make_async_copy(a, b, load_sem.at[i])
        for i, (a, b) in enumerate(((x_hbm, x), (w1_hbm, w1), (w2_hbm, w2)))
    ]
    for load in loads:
        load.start()

    barrier = pltpu.get_barrier_semaphore()

    @pl.when(has_left)
    def _():
        pl.semaphore_signal(barrier, inc=1, device_id={"dp": left}, device_id_type=MESH)

    @pl.when(has_right)
    def _():
        pl.semaphore_signal(barrier, inc=1, device_id={"dp": right}, device_id_type=MESH)

    pl.semaphore_wait(barrier, has_left.astype(jnp.int32) + has_right.astype(jnp.int32))

    def sum_right(c, b):
        return pltpu.make_async_remote_copy(
            part.at[c, b], from_left.at[c, b], sum_send.at[0, c, b], sum_recv.at[0, c, b],
            device_id={"dp": right}, device_id_type=MESH)

    def sum_left(c, b):
        return pltpu.make_async_remote_copy(
            part.at[c, b], from_right.at[c, b], sum_send.at[1, c, b], sum_recv.at[1, c, b],
            device_id={"dp": left}, device_id_type=MESH)

    def hid_right(c, b):
        return pltpu.make_async_remote_copy(
            slots.at[c, b], slots.at[c, b], hid_send.at[0, c, b], hid_recv.at[0, c, b],
            device_id={"dp": right}, device_id_type=MESH)

    def hid_left(c, b):
        return pltpu.make_async_remote_copy(
            slots.at[c, b], slots.at[c, b], hid_send.at[1, c, b], hid_recv.at[1, c, b],
            device_id={"dp": left}, device_id_type=MESH)

    def first(c):
        columns = pl.ds(pl.multiple_of(c * wide, wide), wide)

        def tile(b):
            part[c, b] = jnp.dot(
                x[pl.ds(pl.multiple_of(b * block, block), block), :], w1[:, columns],
                preferred_element_type=jnp.float32,
            ).astype(jnp.bfloat16)

        def up(i, carry):
            b = n - 1 - i
            tile(b)

            @pl.when((me == 0) & (b > 0))
            def _():
                sum_right(c, b).start()

            return carry

        def down(b, carry):
            tile(b)

            @pl.when((me == n - 1) & (b < n - 1))
            def _():
                sum_left(c, b).start()

            return carry

        @pl.when(me == 0)
        def _():
            lax.fori_loop(0, n, up, 0)

        @pl.when(me > 0)
        def _():
            lax.fori_loop(0, n, down, 0)

    def relay(c):
        def one(i, carry):
            b = n - 1 - i

            @pl.when(inner & (b > me))
            def _():
                sum_right(c, b).wait_recv()
                part[c, b] = (part[c, b].astype(jnp.float32) + from_left[c, b].astype(jnp.float32)).astype(jnp.bfloat16)
                sum_right(c, b).start()

            @pl.when(inner & (i < me))
            def _():
                sum_left(c, i).wait_recv()
                part[c, i] = (part[c, i].astype(jnp.float32) + from_right[c, i].astype(jnp.float32)).astype(jnp.bfloat16)
                sum_left(c, i).start()

            return carry

        lax.fori_loop(0, n, one, 0)

    def activate(c):
        total[...] = part[c, me].astype(jnp.float32) + bias[c]

        @pl.when(has_left)
        def _():
            sum_right(c, me).wait_recv()
            total[...] += from_left[c, me].astype(jnp.float32)

        @pl.when(has_right)
        def _():
            sum_left(c, me).wait_recv()
            total[...] += from_right[c, me].astype(jnp.float32)

        value = total[...]
        hidden = (0.5 * value * (1.0 + lax.erf(value * math.sqrt(0.5)))).astype(jnp.bfloat16)
        slots[c, me] = jnp.dot(permute[...], hidden, preferred_element_type=jnp.float32).astype(jnp.bfloat16)

        @pl.when(has_right)
        def _():
            hid_right(c, me).start()

        @pl.when(has_left)
        def _():
            hid_left(c, me).start()

    def spread(c):
        def one(k, carry):
            before, after = me - k, me + k

            @pl.when(before >= 0)
            def _():
                hid_right(c, before).wait_recv()

                @pl.when(has_right)
                def _():
                    hid_right(c, before).start()

            @pl.when(after < n)
            def _():
                hid_left(c, after).wait_recv()

                @pl.when(has_left)
                def _():
                    hid_left(c, after).start()

            return carry

        lax.fori_loop(1, n, one, 0)

    def second(c):
        depth = pl.ds(pl.multiple_of(c * wide, wide), wide)

        def one(b, carry):
            rows = pl.ds(pl.multiple_of(b * block, block), block)
            more = jnp.dot(slots[c, b], w2[depth, :], preferred_element_type=jnp.float32)

            @pl.when(c == 0)
            def _():
                acc[rows, :] = more

            @pl.when(c > 0)
            def _():
                acc[rows, :] += more

            return carry

        lax.fori_loop(0, n, one, 0)

    loads[0].wait()
    loads[1].wait()
    first(0)
    loads[2].wait()

    def step(s, carry):
        @pl.when(s + 1 < chunks)
        def _():
            first(s + 1)

        @pl.when(s < chunks)
        def _():
            relay(s)

        @pl.when((s >= 1) & (s <= chunks))
        def _():
            activate(s - 1)

        @pl.when(s >= 2)
        def _():
            spread(s - 2)
            second(s - 2)

        return carry

    lax.fori_loop(0, chunks + 2, step, 0)

    def finish(b, carry):
        rows = pl.ds(pl.multiple_of(b * block, block), block)
        out[rows, :] = acc[rows, :].astype(jnp.bfloat16)
        return carry

    lax.fori_loop(0, n, finish, 0)
    store = pltpu.make_async_copy(out, out_hbm, load_sem.at[0])
    store.start()

    def drain(c, carry):
        def one(b, inside):
            @pl.when(has_right & (b > me))
            def _():
                sum_right(c, b).wait_send()

            @pl.when(has_left & (b < me))
            def _():
                sum_left(c, b).wait_send()

            @pl.when(has_right & (b <= me))
            def _():
                hid_right(c, b).wait_send()

            @pl.when(has_left & (b >= me))
            def _():
                hid_left(c, b).wait_send()

            return inside

        return lax.fori_loop(0, n, one, carry)

    lax.fori_loop(0, chunks, drain, 0)
    store.wait()


def merger(x, w1, bias, permute, w2):
    n = lax.axis_size("dp")
    rows, depth = x.shape
    hidden, columns = w2.shape
    block = rows // n
    wide = 256 if hidden % 256 == 0 else 128
    chunks = hidden // wide
    any_space = pl.BlockSpec(memory_space=pl.ANY)
    vmem = pl.BlockSpec(memory_space=pltpu.VMEM)
    stack = pltpu.VMEM((chunks, n, block, wide), jnp.bfloat16)
    return pl.pallas_call(
        functools.partial(merger_kernel, n),
        out_shape=jax.ShapeDtypeStruct((rows, columns), jnp.bfloat16),
        in_specs=[any_space, any_space, vmem, vmem, any_space],
        out_specs=any_space,
        scratch_shapes=[
            pltpu.VMEM((rows, depth), jnp.bfloat16),
            pltpu.VMEM((depth, hidden), jnp.bfloat16),
            pltpu.VMEM((hidden, columns), jnp.bfloat16),
            stack,
            stack,
            stack,
            pltpu.VMEM((block, wide), jnp.float32),
            stack,
            pltpu.VMEM((rows, columns), jnp.float32),
            pltpu.VMEM((rows, columns), jnp.bfloat16),
            pltpu.SemaphoreType.DMA((3,)),
            pltpu.SemaphoreType.DMA((2, chunks, n)),
            pltpu.SemaphoreType.DMA((2, chunks, n)),
            pltpu.SemaphoreType.DMA((2, chunks, n)),
            pltpu.SemaphoreType.DMA((2, chunks, n)),
        ],
        compiler_params=pltpu.CompilerParams(
            collective_id=0, has_side_effects=True, vmem_limit_bytes=60 * 1024 * 1024
        ),
    )(x, w1, bias.reshape(chunks, 1, wide), permute, w2)


def place_kernel(
    n, y, out, half, across_sum, from_across, ready, landed, got,
    mate_send, mate_recv, across_send, across_recv, row_send, row_recv, end_send, end_recv,
):
    quarter = y.shape[3] // 4
    row, me = lax.axis_index("dp"), lax.axis_index("tensor")
    core, side = me % 2, me // 2
    mate, across = side * 2 + 1 - core, (1 - side) * 2 + core

    barrier = pltpu.get_barrier_semaphore()
    for k in range(1, 4):
        pl.semaphore_signal(barrier, inc=1, device_id={"tensor": (me + k) % 4}, device_id_type=MESH)
    for k in range(1, n):
        pl.semaphore_signal(barrier, inc=1, device_id={"dp": (row + k) % n}, device_id_type=MESH)
    pl.semaphore_wait(barrier, 3 + n - 1)

    def piece(index):
        return pl.ds(pl.multiple_of(index * quarter, quarter), quarter)

    def to_mate(i, j):
        return pltpu.make_async_remote_copy(
            y.at[i, :, :, piece((side + j) % 2 * 2 + 1 - core)], half.at[i, j], mate_send.at[i, j], mate_recv.at[i, j],
            device_id={"tensor": mate}, device_id_type=MESH)

    def to_across(i):
        return pltpu.make_async_remote_copy(
            across_sum.at[i], from_across.at[i], across_send.at[i], across_recv.at[i],
            device_id={"tensor": across}, device_id_type=MESH)

    def to_row(i, k):
        other = (row + k) % n
        return pltpu.make_async_remote_copy(
            ready.at[i, other], landed.at[row, i], row_send.at[i, k], row_recv.at[i, k],
            device_id={"dp": other}, device_id_type=MESH)

    def to_end(i, k, block):
        return pltpu.make_async_remote_copy(
            landed.at[block, i], got.at[me, i], end_send.at[i, k], end_recv.at[i, me],
            device_id={"tensor": block}, device_id_type=MESH)

    for i in range(n):
        for j in (1, 0):
            to_mate(i, j).start()

    for i in range(n):
        to_mate(i, 1).wait_recv()
        for s in range(n):
            across_sum[i, s] = (
                y[i, s, :, piece((1 - side) * 2 + core)].astype(jnp.float32) + half[i, 1, s].astype(jnp.float32)
            ).astype(jnp.bfloat16)
        to_across(i).start()

    for i in range(n):
        to_mate(i, 0).wait_recv()
        to_across(i).wait_recv()
        for s in range(n):
            ready[i, s] = (
                y[i, s, :, piece(me)].astype(jnp.float32)
                + half[i, 0, s].astype(jnp.float32)
                + from_across[i, s].astype(jnp.float32)
            ).astype(jnp.bfloat16)
        for k in range(1, n):
            to_row(i, k).start()
        landed[row, i] = ready[i, row]

    for i in range(n):
        for k in range(n):
            block = (row + n - k) % n
            if k:
                to_row(i, k).wait_recv()

            @pl.when(block == me)
            def _():
                got[me, i] = landed[block, i]

            @pl.when(block != me)
            def _():
                to_end(i, k, block).start()

    for i in range(n):
        for k in range(1, 4):
            other = (me + k) % 4
            pltpu.make_async_remote_copy(
                landed.at[0, i], got.at[other, i], end_send.at[i, 0], end_recv.at[i, other],
                device_id={"tensor": other}, device_id_type=MESH).wait_recv()
    for t in range(4):
        out[:, :, t * quarter:(t + 1) * quarter] = got[t]

    for i in range(n):
        for j in range(2):
            to_mate(i, j).wait_send()
        to_across(i).wait_send()
        for k in range(1, n):
            to_row(i, k).wait_send()
        for k in range(n):
            block = (row + n - k) % n

            @pl.when(block != me)
            def _():
                to_end(i, k, block).wait_send()


def place(second):
    n, _, capacity, columns = second.shape
    quarter = columns // 4
    vmem = pl.BlockSpec(memory_space=pltpu.VMEM)
    stack = pltpu.VMEM((n, n, capacity, quarter), jnp.bfloat16)
    return pl.pallas_call(
        functools.partial(place_kernel, n),
        out_shape=jax.ShapeDtypeStruct((n, capacity, columns), jnp.bfloat16),
        in_specs=[vmem],
        out_specs=vmem,
        scratch_shapes=[
            pltpu.VMEM((n, 2, n, capacity, quarter), jnp.bfloat16),
            stack,
            stack,
            stack,
            stack,
            stack,
            pltpu.SemaphoreType.DMA((n, 2)),
            pltpu.SemaphoreType.DMA((n, 2)),
            pltpu.SemaphoreType.DMA((n,)),
            pltpu.SemaphoreType.DMA((n,)),
            pltpu.SemaphoreType.DMA((n, n)),
            pltpu.SemaphoreType.DMA((n, n)),
            pltpu.SemaphoreType.DMA((n, n)),
            pltpu.SemaphoreType.DMA((n, n)),
        ],
        compiler_params=pltpu.CompilerParams(
            collective_id=1, has_side_effects=True, vmem_limit_bytes=40 * 1024 * 1024
        ),
    )(second)


def exchange(second, dp_count, tensor_count, capacity):
    if dp_count == tensor_count == 4 and capacity % 16 == 0 and second.shape[1] % 512 == 0:
        return place(second.reshape(dp_count, dp_count, capacity, -1)).reshape(dp_count * capacity, -1)
    second = lax.psum_scatter(second, "tensor", scatter_dimension=1, tiled=True)
    columns = second.shape[1]
    second = second.reshape(dp_count, dp_count, capacity, columns)
    second = lax.all_to_all(second, "dp", split_axis=1, concat_axis=0, tiled=False)
    blocks = dp_count // tensor_count
    second = second.reshape(tensor_count, blocks, dp_count * capacity, columns)
    second = lax.all_to_all(second, "tensor", split_axis=0, concat_axis=0, tiled=True)
    return second.transpose(2, 1, 0, 3).reshape(dp_count * capacity, -1)


def local(
    patches,
    grids,
    dest,
    norm_gain,
    qkv_weight,
    qkv_bias,
    proj_weight,
    proj_bias,
    merge_gain,
    w_first,
    b_first,
    w_second,
    b_second,
    text_embed,
):
    rows_dev, width = patches.shape
    images_dev = grids.shape[0]
    heads_dev = qkv_weight.shape[2] // HEAD_DIM
    dp_count = lax.axis_size("dp")
    tensor_count = lax.axis_size("tensor")
    seq_rows = text_embed.shape[0]
    capacity = images_dev * (MERGED // dp_count)
    live_count = grids[:, 0] * grids[:, 1]
    permute, slot_rows = placement(dest, live_count, dp_count, seq_rows, capacity)
    arrived_rows = lax.all_to_all(
        slot_rows.reshape(dp_count, capacity), "dp", split_axis=0, concat_axis=0, tiled=True
    ).reshape(-1)

    attended = attention(patches, live_count, norm_gain, qkv_weight, qkv_bias, images_dev, heads_dev)
    partial_value = jnp.dot(attended, proj_weight, preferred_element_type=jnp.float32).astype(jnp.bfloat16)
    summed = lax.psum_scatter(partial_value, "tensor", scatter_dimension=0, tiled=True).astype(jnp.float32)
    part = rows_dev // tensor_count
    own = lax.dynamic_slice_in_dim(patches, lax.axis_index("tensor") * part, part, 0)
    resid = own.astype(jnp.float32) + summed + proj_bias
    merged_in = rms_scale(resid, merge_gain).astype(jnp.bfloat16).reshape(part // 4, 4 * width)
    sliced = lax.all_to_all(
        merged_in.reshape(part // 4, dp_count, 4 * width // dp_count), "dp", split_axis=1, concat_axis=0, tiled=False
    )
    received = lax.all_gather(sliced, "tensor", axis=1, tiled=False)
    received = received.reshape(-1, 4 * width // dp_count)
    second = merger(received, w_first, b_first, permute, w_second)
    visual = exchange(second, dp_count, tensor_count, capacity)
    visual = (visual.astype(jnp.float32) + b_second).astype(jnp.bfloat16)
    hit = jnp.arange(seq_rows, dtype=jnp.int32)[:, None] == arrived_rows[None, :]
    placed = jnp.dot(hit.astype(jnp.bfloat16), visual, preferred_element_type=jnp.float32).astype(jnp.bfloat16)
    return jnp.where(jnp.any(hit, axis=1)[:, None], placed, text_embed)


def fused_kernel(
    seq_rows, lags,
    patches_hbm, grids, dest, gain, wqkv_hbm, bqkv, wproj_hbm, bproj, mgain, w1_hbm, bias, w2_hbm,
    out, arrived,
    patches, wqkv, bpad, wproj, target, normed, raws, qs, ks, vs, att_f32, att_out, att_in, slices, rows_tbl, x,
    w1, w2, own, to_r, to_l, from_l, from_r, hidden, keep, give, from_mate, cross, from_across, ready, landed,
    load_sem, head_sem, tbl_send, tbl_recv, pm_send, pm_recv, pa_send, pa_recv, py_send, py_recv, pd_send, pd_recv,
    att_send, att_recv, z_send, fm_send, fa_send, x_recv,
    r_send, r_recv, l_send, l_recv, mate_send, mate_recv, across_send, across_recv,
    row_send, row_recv, end_send, end_recv,
):
    n, sides, _, few, width = x.shape
    nt = 2 * sides
    rows = patches.shape[0]
    block = rows // n
    half = block // sides
    merged = dest.shape[1]
    heads = qs.shape[0]
    lanes = qs.shape[2]
    count, _, wide = own.shape
    steps = count // n
    pieces = steps // sides
    quarter = keep.shape[2]
    piece = ready.shape[3]
    row, me, group = lax.axis_index("dp"), lax.axis_index("tensor"), lax.axis_index("groups")
    core, side = me % 2, me // 2
    mate, across = side * 2 + 1 - core, (1 - side) * 2 + core
    left, right = lax.max(row - 1, 0), lax.min(row + 1, n - 1)
    has_left, has_right = row > 0, row < n - 1
    bf16, f32 = jnp.bfloat16, jnp.float32

    load_x = pltpu.make_async_copy(patches_hbm, patches, load_sem.at[0])
    load_p = pltpu.make_async_copy(wproj_hbm, wproj.at[me], load_sem.at[1])
    load_1 = pltpu.make_async_copy(w1_hbm, w1, load_sem.at[2])
    load_2 = pltpu.make_async_copy(w2_hbm, w2, load_sem.at[3])
    load_w = [
        pltpu.make_async_copy(
            wqkv_hbm.at[j, h * HEAD_DIM:(h + 1) * HEAD_DIM], wqkv.at[j, h * lanes:h * lanes + HEAD_DIM],
            head_sem.at[j, h])
        for j in range(3) for h in range(heads)
    ]
    load_p.start()
    load_x.start()
    for load in load_w:
        load.start()

    barrier = pltpu.get_barrier_semaphore()
    for k in range(1, nt):
        pl.semaphore_signal(barrier, inc=1, device_id={"tensor": (me + k) % nt}, device_id_type=MESH)
    for k in range(1, n):
        pl.semaphore_signal(barrier, inc=1, device_id={"dp": (row + k) % n}, device_id_type=MESH)
    pl.semaphore_signal(barrier, inc=1, device_id={"groups": 1 - group}, device_id_type=MESH)
    pl.semaphore_wait(barrier, nt - 1 + n - 1 + 1)

    def remote(source, to, send, recv, device):
        return pltpu.make_async_remote_copy(source, to, send, recv, device_id=device, device_id_type=MESH)

    span = wproj.shape[1] // 4

    def strip(g, a):
        return pl.ds(pl.multiple_of((g * 2 + a) * span, span), span)

    def same(ref, send, recv, device):
        return remote(ref, ref, send, recv, device)

    proj_mate = same(wproj.at[me], pm_send, pm_recv, {"tensor": mate})
    proj_across = [
        same(wproj.at[me, strip(group, a)], pa_send.at[a], pa_recv.at[a], {"tensor": across}) for a in range(2)]
    proj_got = [
        same(wproj.at[across, strip(group, a)], pa_send.at[a], pa_recv.at[a], {"tensor": across}) for a in range(2)]
    proj_peer = [
        same(wproj.at[across, strip(group, a)], py_send.at[a], py_recv.at[a], {"groups": 1 - group})
        for a in range(2)]
    proj_peer_got = [
        same(wproj.at[across, strip(1 - group, a)], py_send.at[a], py_recv.at[a], {"groups": 1 - group})
        for a in range(2)]

    def proj_diag(g, a, at):
        return same(wproj.at[across, strip(g, a)], pd_send.at[at, a], pd_recv.at[at, a], {"tensor": mate})

    load_p.wait()
    for copy in proj_across:
        copy.start()
    proj_mate.start()

    live = grids[0, 0] * grids[0, 1]
    dest_row = dest[...].astype(f32)

    def shards(value):
        total = jnp.zeros_like(value)
        for s in range(1, n):
            total += jnp.where(value >= float(s * seq_rows), 1.0, 0.0)
        return total

    square = (merged, merged)
    first_at = lax.broadcasted_iota(jnp.int32, square, 0)
    second_at = lax.broadcasted_iota(jnp.int32, square, 1)
    dest_col = jnp.sum(jnp.where(first_at == second_at, dest_row, 0.0), axis=1, keepdims=True)
    shard_row, shard_col = shards(dest_row), shards(dest_col)
    rank_col = jnp.sum(
        jnp.where((shard_row == shard_col) & (second_at < first_at), 1.0, 0.0), axis=1, keepdims=True)
    live_col = lax.broadcasted_iota(jnp.int32, (merged, 1), 0) * 4 < live
    code_col = jnp.where(live_col, shard_col * lanes + rank_col, -1.0)
    lane_at = lax.broadcasted_iota(jnp.int32, (merged, n * lanes), 1).astype(f32)
    local_col = dest_col - shard_col * seq_rows
    table = jnp.sum(jnp.where(lane_at == code_col, local_col + 1.0, 0.0), axis=0, keepdims=True) - 1.0
    for s in range(n):
        rows_tbl[s] = jnp.broadcast_to(table[:, s * lanes:(s + 1) * lanes], (8, lanes)).astype(jnp.int32)
    arrived[row] = rows_tbl[row]

    def send_table(k):
        to = (row + k) % n
        return remote(rows_tbl.at[to], arrived.at[row], tbl_send.at[k], tbl_recv.at[row], {"dp": to})

    for k in range(1, n):
        send_table(k).start()

    tall = (merged, rows)
    at_row = lax.broadcasted_iota(jnp.int32, tall, 0)
    at_lane = lax.broadcasted_iota(jnp.int32, tall, 1)
    dest_rep = jnp.sum(jnp.where(at_row == at_lane // 4, dest_col, 0.0), axis=0, keepdims=True)
    shard_rep = shards(dest_rep)
    rank_rep = jnp.sum(
        jnp.where((shard_col == shard_rep) & (at_row < at_lane // 4), 1.0, 0.0), axis=0, keepdims=True)
    rank_i, shard_i = rank_rep.astype(jnp.int32), shard_rep.astype(jnp.int32)
    place_i = lax.broadcasted_iota(jnp.int32, (1, rows), 1)
    slot_i = (
        rank_i // piece * block + shard_i // 2 * half + place_i % 4 * few + shard_i % 2 * piece + rank_i % piece)
    target[...] = jnp.broadcast_to(jnp.where(place_i < live, slot_i, -1), target.shape)

    ones_at = lax.broadcasted_iota(jnp.int32, (1, lanes), 1) == HEAD_DIM
    for j in range(3):
        for h in range(heads):
            bpad[j:j + 1, h * lanes:(h + 1) * lanes] = jnp.where(ones_at, 0.0 if j == 1 else 1.0, 0.0)
            bpad[j:j + 1, h * lanes:h * lanes + HEAD_DIM] = bqkv[j:j + 1, h * HEAD_DIM:(h + 1) * HEAD_DIM]
            wqkv[j, h * lanes + HEAD_DIM:(h + 1) * lanes, :] = jnp.zeros((lanes - HEAD_DIM, width), bf16)

    load_x.wait()
    for load in load_w:
        load.wait()
    load_1.start()
    load_2.start()

    mask_at = lax.broadcasted_iota(jnp.int32, (block, lanes), 1) == HEAD_DIM

    def project(b, carry):
        @pl.when(b == 2)
        def _():
            proj_got[0].wait_recv()
            proj_peer[0].start()
            proj_diag(group, 0, 0).start()

        at = pl.ds(pl.multiple_of(b * block, block), block)
        hit = jnp.where(
            target[0:1, :] == lax.broadcasted_iota(jnp.int32, (block, rows), 0) + b * block, 1.0, 0.0)
        valid = jnp.sum(hit, axis=1, keepdims=True)
        raw = jnp.dot(hit.astype(bf16), patches[...], preferred_element_type=f32)
        for s in range(sides):
            raws[b, s] = raw[s * half:(s + 1) * half, :].astype(bf16)
        normed[...] = rms_scale(raw, gain[...].reshape(1, width)).astype(bf16)
        for j, store in enumerate((qs, ks, vs)):
            acc = lax.dot_general(
                normed[...], wqkv[j], (((1,), (1,)), ((), ())), preferred_element_type=f32) + bpad[j:j + 1, :]
            for h in range(heads):
                value = acc[:, h * lanes:(h + 1) * lanes]
                if j == 1:
                    value = jnp.where(mask_at, jnp.where(valid > 0.5, 0.0, -1e30), value)
                store[h, at, :] = value.astype(bf16)
        return carry

    lax.fori_loop(0, n, project, 0)

    proj_got[1].wait_recv()
    proj_peer[1].start()
    proj_diag(group, 1, 0).start()

    scale = math.log2(math.e) / math.sqrt(HEAD_DIM)

    def att_to(b, s):
        return remote(
            att_out.at[b, s], att_in.at[b // 2, me], att_send.at[b, s], att_recv.at[b // 2, me],
            {"tensor": s * 2 + b % 2})

    def att_got(b, source):
        return remote(
            att_out.at[b, 0], att_in.at[b // 2, source], att_send.at[b, 0], att_recv.at[b // 2, source],
            {"tensor": mate})

    def z_to(b, k):
        to = (row + k) % n
        return remote(
            slices.at[b // 2, to], x.at[b, side, row], z_send.at[b // 2, k], x_recv.at[b, side, row], {"dp": to})

    def to_mate_x(b, s, i):
        return same(x.at[b, s, i], fm_send.at[b // 2, s, i], x_recv.at[b, s, i], {"tensor": mate})

    def to_across_x(b, i):
        return same(x.at[b, side, i], fa_send.at[b // 2, i], x_recv.at[b, side, i], {"tensor": across})

    def x_got(b, s, i):
        return same(x.at[b, s, i], fm_send.at[b // 2, s, i], x_recv.at[b, s, i], {"tensor": mate})

    def attend(it, carry):
        @pl.when(it < n)
        def _():
            b = lax.min(it, n - 1)
            at = pl.ds(pl.multiple_of(b * block, block), block)
            for h in range(heads):
                scores = lax.dot_general(
                    qs[h, at, :], ks[h], (((1,), (1,)), ((), ())), preferred_element_type=f32)
                peak = jnp.max(scores, axis=1, keepdims=True)
                weights = jnp.exp2((scores - peak) * scale).astype(bf16)
                mixed = jnp.dot(weights, vs[h], preferred_element_type=f32)
                mixed = mixed * (1.0 / mixed[:, HEAD_DIM:HEAD_DIM + 1])
                att_f32[:, h * HEAD_DIM:(h + 1) * HEAD_DIM] = mixed[:, 0:HEAD_DIM]
            for s in range(sides):
                att_out[b, s] = att_f32[s * half:(s + 1) * half, :].astype(bf16)
                owner = s * 2 + b % 2

                @pl.when(owner != me)
                def _():
                    att_to(b, s).start()

                @pl.when(owner == me)
                def _():
                    att_in[b // 2, me] = att_out[b, s]

        @pl.when(it == 1)
        def _():
            proj_mate.wait_recv()
            for a in range(2):
                proj_peer_got[a].wait_recv()
                proj_diag(1 - group, a, 1).start()
            for a in range(2):
                proj_diag(group, a, 0).wait_recv()
                proj_diag(1 - group, a, 1).wait_recv()

        last = lax.max(it, 1) - 1

        @pl.when((it >= 1) & (last % 2 == core))
        def _():
            for k in range(1, nt):
                att_got(last, (me + k) % nt).wait_recv()
            total = raws[last, side].astype(f32) + bproj[...].reshape(1, width)
            for t in range(nt):
                total += jnp.dot(att_in[last // 2, t], wproj[t], preferred_element_type=f32)
            done = rms_scale(total, mgain[...].reshape(1, width)).astype(bf16)
            for k in range(n):
                slices[last // 2, k] = done[k * few:(k + 1) * few, :]
            for k in range(n - 1, 0, -1):
                z_to(last, k).start()
            x[last, side, row] = slices[last // 2, row]
            to_across_x(last, row).start()
            to_mate_x(last, side, row).start()

        return carry

    lax.fori_loop(0, n + 1, attend, 0)

    def forward(b):
        for k in range(1, n):
            source = (row + n - k) % n
            x_got(b, side, source).wait_recv()
            to_across_x(b, source).start()
            to_mate_x(b, side, source).start()

    def forward_across(b):
        for k in range(n):
            source = (row + n - k) % n
            x_got(b, 1 - side, source).wait_recv()
            to_mate_x(b, 1 - side, source).start()

    def await_x(b):
        @pl.when(b % 2 != core)
        def _():
            for s in range(sides):
                for i in range(n):
                    x_got(b, s, i).wait_recv()

    def go_right(c):
        return remote(to_r.at[c], from_l.at[c], r_send.at[c], r_recv.at[c], {"dp": right})

    def go_left(c):
        return remote(to_l.at[c], from_r.at[c], l_send.at[c], l_recv.at[c], {"dp": left})

    def first(c):
        b, j = c // steps, c % steps // sides
        columns = pl.ds(pl.multiple_of(j * wide, wide), wide)
        partial = jnp.dot(x[b].reshape(block, width), w1[:, columns], preferred_element_type=f32)
        for s in range(sides):
            own[c + s] = partial[s * half:(s + 1) * half, :]

            @pl.when(row == 0)
            def _():
                to_r[c + s] = partial[s * half:(s + 1) * half, :].astype(bf16)
                go_right(c + s).start()

            @pl.when(row == n - 1)
            def _():
                to_l[c + s] = partial[s * half:(s + 1) * half, :].astype(bf16)
                go_left(c + s).start()

    def relay(stage, c):
        @pl.when(row == stage)
        def _():
            go_right(c).wait_recv()
            to_r[c] = (own[c] + from_l[c].astype(f32)).astype(bf16)
            go_right(c).start()

        @pl.when(row == n - 1 - stage)
        def _():
            go_left(c).wait_recv()
            to_l[c] = (own[c] + from_r[c].astype(f32)).astype(bf16)
            go_left(c).start()

    def activate(c):
        j = c % steps // sides

        @pl.when(row == n - 1)
        def _():
            go_right(c).wait_recv()

        @pl.when(row == 0)
        def _():
            go_left(c).wait_recv()

        @pl.when(has_left)
        def _():
            own[c] += from_l[c].astype(f32)

        @pl.when(has_right)
        def _():
            own[c] += from_r[c].astype(f32)

        value = own[c] + bias[j]
        at = pl.ds(pl.multiple_of(c % sides * half, half), half)
        hidden[j, at, :] = (0.5 * value * (1.0 + lax.erf(value * math.sqrt(0.5)))).astype(bf16)

    def columns_of(s, c):
        return pl.ds(pl.multiple_of((s * 2 + c) * quarter, quarter), quarter)

    def to_mate(b, s):
        return remote(give.at[b, s], from_mate.at[b, s], mate_send.at[b, s], mate_recv.at[b, s], {"tensor": mate})

    def to_across(b):
        return remote(cross.at[b], from_across.at[b], across_send.at[b], across_recv.at[b], {"tensor": across})

    def to_row(b, k):
        to = (row + k) % n
        return remote(ready.at[b, to], landed.at[b, row], row_send.at[b, k], row_recv.at[b, row], {"dp": to})

    def quarter_of(t):
        return pl.ds(pl.multiple_of(t * quarter, quarter), quarter)

    def to_end(b, d):
        return remote(
            landed.at[b, d], out.at[:, b, :, quarter_of(me)], end_send.at[b, d], end_recv.at[b, me], {"tensor": d})

    def second(b):
        def product(columns):
            acc = jnp.dot(hidden[0], w2[0:wide, columns], preferred_element_type=f32)
            for j in range(1, pieces):
                acc += jnp.dot(hidden[j], w2[j * wide:(j + 1) * wide, columns], preferred_element_type=f32)
            return acc

        for s in (1 - side, side):
            give[b, s] = product(columns_of(s, 1 - core)).astype(bf16)
            to_mate(b, s).start()
        for s in (1 - side, side):
            keep[s] = product(columns_of(s, core))

    def chip_sum(b):
        to_mate(b, 1 - side).wait_recv()
        cross[b] = (keep[1 - side] + from_mate[b, 1 - side].astype(f32)).astype(bf16)
        to_across(b).start()

    def spread(b):
        to_mate(b, side).wait_recv()
        to_across(b).wait_recv()
        value = keep[side] + from_mate[b, side].astype(f32) + from_across[b].astype(f32)
        value = value.astype(bf16)
        for s in range(n):
            for i in range(n):
                at = s // 2 * half + i * few + s % 2 * piece
                ready[b, s, i] = value[at:at + piece, :]
        for k in range(n - 1, 0, -1):
            to_row(b, k).start()
        landed[b, row] = ready[b, row]

    def deliver(b):
        for k in range(n):
            source = (row + n - k) % n
            if k:
                remote(
                    ready.at[b, 0], landed.at[b, source], row_send.at[b, 0], row_recv.at[b, source], {"dp": left}
                ).wait_recv()

            @pl.when(source == me)
            def _():
                out[:, b, :, quarter_of(me)] = landed[b, source]

            @pl.when(source != me)
            def _():
                to_end(b, source).start()

    lead, hop, fill, offsets = lags

    @pl.when(core == 0)
    def _():
        forward(0)
        forward_across(0)

    @pl.when(core == 1)
    def _():
        forward(1)

    load_1.wait()
    load_2.wait()
    after = tuple(zip(offsets, (second, chip_sum, spread, deliver)))

    def step(u, carry):
        @pl.when((u < count) & (u % sides == 0))
        def _():
            @pl.when(u % steps == 0)
            def _():
                await_x(u // steps)

            first(u)

        @pl.when((u == 1) & (core == 1))
        def _():
            forward_across(1)

        @pl.when(u == 3)
        def _():
            forward(2 + core)

        @pl.when(u == 5)
        def _():
            forward_across(2 + core)

        for stage in range(1, n - 1):
            late = lead + (stage - 1) * hop

            @pl.when((u >= late) & (u < count + late))
            def _():
                relay(stage, u - late)

        @pl.when((u >= lead + fill) & (u < count + lead + fill))
        def _():
            activate(u - lead - fill)

        for offset, work in after:
            late = lead + fill + offset + steps - 1

            @pl.when((u >= late) & (u < count + late) & (lax.max(u - late, 0) % steps == 0))
            def _():
                work((u - late) // steps)

        return carry

    lax.fori_loop(0, count + lead + fill + offsets[-1], step, 0)

    for b in range(n):
        for k in range(1, nt):
            source = (me + k) % nt
            remote(
                landed.at[b, 0], out.at[:, b, :, quarter_of(source)], end_send.at[b, 0], end_recv.at[b, source],
                {"tensor": mate},
            ).wait_recv()
    for k in range(1, n):
        source = (row + n - k) % n
        remote(rows_tbl.at[0], arrived.at[source], tbl_send.at[0], tbl_recv.at[source], {"dp": source}).wait_recv()

    def drain(c, carry):
        @pl.when(has_right)
        def _():
            go_right(c).wait_send()

        @pl.when(has_left)
        def _():
            go_left(c).wait_send()

        return carry

    lax.fori_loop(0, count, drain, 0)
    proj_mate.wait_send()
    for a in range(2):
        proj_across[a].wait_send()
        proj_peer[a].wait_send()
        proj_diag(group, a, 0).wait_send()
        proj_diag(1 - group, a, 1).wait_send()
    for k in range(1, n):
        send_table(k).wait_send()
    for b in range(n):
        for s in range(sides):
            @pl.when(s * 2 + b % 2 != me)
            def _():
                att_to(b, s).wait_send()

            to_mate(b, s).wait_send()
        to_across(b).wait_send()
        for k in range(1, n):
            to_row(b, k).wait_send()
            to_end(b, (me + k) % nt).wait_send()
    for q in range(2):
        b = 2 * q + core
        for k in range(1, n):
            z_to(b, k).wait_send()
        for i in range(n):
            to_across_x(b, i).wait_send()
            for s in range(sides):
                to_mate_x(b, s, i).wait_send()


def fused(
    patches, grids, dest, norm_gain, qkv_weight, qkv_bias, proj_weight, proj_bias, merge_gain,
    w_first, b_first, w_second, seq_rows,
):
    n, nt = lax.axis_size("dp"), lax.axis_size("tensor")
    sides = nt // 2
    rows, width = patches.shape
    span = qkv_weight.shape[2]
    heads = span // HEAD_DIM
    block = rows // n
    half = block // sides
    few = half // 4
    hidden, columns = w_second.shape
    wide, lanes = 256, 128
    pieces = hidden // wide
    steps = pieces * sides
    count = n * steps
    quarter = columns // nt
    piece = few // 2
    any_space = pl.BlockSpec(memory_space=pl.ANY)
    vmem = pl.BlockSpec(memory_space=pltpu.VMEM)
    smem = pl.BlockSpec(memory_space=pltpu.SMEM)
    dma = pltpu.SemaphoreType.DMA
    bf16, f32 = jnp.bfloat16, jnp.float32
    heads_shape = pltpu.VMEM((heads, rows, lanes), bf16)
    stack = pltpu.VMEM((count, half, wide), bf16)
    tiles = pltpu.VMEM((n, 2, block, quarter), bf16)
    one = pltpu.VMEM((n, block, quarter), bf16)
    moved = pltpu.VMEM((n, n, n, piece, quarter), bf16)
    lags = (4, 3, 6, (0, 2, 6, 10))
    return pl.pallas_call(
        functools.partial(fused_kernel, seq_rows, lags),
        out_shape=(
            jax.ShapeDtypeStruct((n, n, piece, columns), bf16),
            jax.ShapeDtypeStruct((n, 8, lanes), jnp.int32),
        ),
        in_specs=[
            any_space, smem, vmem, vmem, any_space, vmem, any_space, vmem, vmem, any_space, vmem, any_space],
        out_specs=(vmem, vmem),
        scratch_shapes=[
            pltpu.VMEM((rows, width), bf16),
            pltpu.VMEM((3, heads * lanes, width), bf16),
            pltpu.VMEM((3, heads * lanes), f32),
            pltpu.VMEM((nt, span, width), bf16),
            pltpu.VMEM((8, rows), jnp.int32),
            pltpu.VMEM((block, width), bf16),
            pltpu.VMEM((n, sides, half, width), bf16),
            heads_shape, heads_shape, heads_shape,
            pltpu.VMEM((block, span), f32),
            pltpu.VMEM((n, sides, half, span), bf16),
            pltpu.VMEM((n // 2, nt, half, span), bf16),
            pltpu.VMEM((n // 2, n, few, width), bf16),
            pltpu.VMEM((n, 8, lanes), jnp.int32),
            pltpu.VMEM((n, sides, n, few, width), bf16),
            pltpu.VMEM(w_first.shape, bf16),
            pltpu.VMEM(w_second.shape, bf16),
            pltpu.VMEM((count, half, wide), f32),
            stack, stack, stack, stack,
            pltpu.VMEM((pieces, block, wide), bf16),
            pltpu.VMEM((2, block, quarter), f32),
            tiles, tiles, one, one, moved, moved,
            dma((4,)), dma((3, heads)), dma((n,)), dma((n,)), dma, dma, dma((2,)), dma((2,)), dma((2,)), dma((2,)),
            dma((2, 2)), dma((2, 2)),
            dma((n, sides)), dma((n // 2, nt)), dma((n // 2, n)), dma((n // 2, sides, n)), dma((n // 2, n)),
            dma((n, sides, n)),
            dma((count,)), dma((count,)), dma((count,)), dma((count,)),
            dma((n, 2)), dma((n, 2)), dma((n,)), dma((n,)), dma((n, n)), dma((n, n)), dma((n, nt)), dma((n, nt)),
        ],
        compiler_params=pltpu.CompilerParams(
            collective_id=2, has_side_effects=True, vmem_limit_bytes=63 * 1024 * 1024
        ),
    )(
        patches, grids, dest, norm_gain, qkv_weight.swapaxes(1, 2), qkv_bias, proj_weight, proj_bias, merge_gain,
        w_first, b_first.reshape(pieces, 1, wide), w_second,
    )


def local_fast(
    patches,
    grids,
    dest,
    norm_gain,
    qkv_weight,
    qkv_bias,
    proj_weight,
    proj_bias,
    merge_gain,
    w_first,
    b_first,
    w_second,
    b_second,
    text_embed,
):
    seq_rows = text_embed.shape[0]
    visual, arrived = fused(
        patches, grids, dest, norm_gain, qkv_weight, qkv_bias, proj_weight, proj_bias, merge_gain,
        w_first, b_first, w_second, seq_rows)
    visual = visual.reshape(-1, visual.shape[3])
    arrived_rows = arrived[:, 0, :visual.shape[0] // arrived.shape[0]].reshape(-1)
    visual = (visual.astype(jnp.float32) + b_second).astype(jnp.bfloat16)
    hit = jnp.arange(seq_rows, dtype=jnp.int32)[:, None] == arrived_rows[None, :]
    placed = jnp.dot(hit.astype(jnp.bfloat16), visual, preferred_element_type=jnp.float32).astype(jnp.bfloat16)
    return jnp.where(jnp.any(hit, axis=1)[:, None], placed, text_embed)


def fits(patches, grids, dest, qkv_weight, w_first, w_second):
    n, nt = lax.axis_size("dp"), lax.axis_size("tensor")
    rows, width = patches.shape
    return (
        n == nt == 4
        and lax.axis_size("groups") == 2
        and grids.shape[0] == 1
        and rows == PATCHES
        and dest.shape[1] == MERGED
        and w_first.shape[0] == width
        and w_second.shape[0] % 256 == 0
        and w_second.shape[1] % 512 == 0
        and qkv_weight.shape[2] % 64 == 0
    )


def chosen(*args):
    run = local_fast if fits(args[0], args[1], args[2], args[4], args[9], args[11]) else local
    return run(*args)


def solution(mesh):
    in_specs = (
        P(("groups", "dp"), None),
        P(("groups", "dp"), None),
        P(("groups", "dp"), None),
        P(),
        P(None, None, "tensor"),
        P(None, "tensor"),
        P("tensor", None),
        P(),
        P(),
        P("dp", "tensor"),
        P("tensor"),
        P("tensor", "dp"),
        P("tensor"),
        P(("groups", "dp"), "tensor"),
    )
    out_specs = P(("groups", "dp"), "tensor")
    return jax.shard_map(chosen, mesh=mesh, in_specs=in_specs, out_specs=out_specs, check_vma=False)
```

```python
import functools
import math

import jax
import jax.numpy as jnp
from jax import lax
from jax.experimental import pallas as pl
from jax.experimental.pallas import tpu as pltpu
from jax.sharding import PartitionSpec as P

MESH = pl.DeviceIdType.MESH

HEAD_DIM = 80
PATCHES = 1024
MERGED = 256


def rms_scale(values, gain):
    return values * lax.rsqrt(jnp.mean(values * values, axis=-1, keepdims=True) + 1e-06) * gain


def placement(dest, live_count, dp_count, seq_rows, capacity):
    merged_dev = dest.size
    live_rows = (jnp.arange(MERGED, dtype=jnp.int32)[None, :] < (live_count // 4)[:, None]).reshape(merged_dev)
    dest_flat = dest.reshape(merged_dev)
    shard_id = jnp.where(live_rows, dest_flat // seq_rows, dp_count)
    local_row = dest_flat % seq_rows
    index = jnp.arange(merged_dev, dtype=jnp.int32)
    earlier = (shard_id[:, None] == shard_id[None, :]) & (index[None, :] < index[:, None])
    rank = jnp.sum(earlier.astype(jnp.int32), axis=1)
    slot = jnp.where(live_rows & (rank < capacity), shard_id * capacity + rank, -1)
    hit = jnp.arange(dp_count * capacity, dtype=jnp.int32)[:, None] == slot[None, :]
    rows = jnp.max(jnp.where(hit, local_row[None, :], -1), axis=1)
    return hit.astype(jnp.bfloat16), rows


def attention(patches, live_count, norm_gain, qkv_weight, qkv_bias, images_dev, heads_dev):
    normed = rms_scale(patches.astype(jnp.float32), norm_gain).astype(jnp.bfloat16)
    projected = (
        jnp.einsum("rv,jvc->jrc", normed, qkv_weight, preferred_element_type=jnp.float32)
        + qkv_bias[:, None, :]
    )
    projected = projected.astype(jnp.bfloat16).reshape(3, images_dev, PATCHES, heads_dev, HEAD_DIM)
    scores = jnp.einsum(
        "iqhd,ikhd->ihqk", projected[0], projected[1], preferred_element_type=jnp.float32
    ) / math.sqrt(HEAD_DIM)
    live_keys = jnp.arange(PATCHES, dtype=jnp.int32)[None, :] < live_count[:, None]
    scores = jnp.where(live_keys[:, None, None, :], scores, jnp.float32(-1e30))
    peak_score = jnp.max(scores, axis=-1, keepdims=True)
    exponent = jnp.exp(scores - peak_score)
    weights = (exponent / jnp.sum(exponent, axis=-1, keepdims=True)).astype(jnp.bfloat16)
    attended = jnp.einsum(
        "ihqk,ikhd->iqhd", weights, projected[2], preferred_element_type=jnp.float32
    )
    return attended.astype(jnp.bfloat16).reshape(patches.shape[0], heads_dev * HEAD_DIM)


def merger_kernel(
    n, x_hbm, w1_hbm, bias, permute, w2_hbm, out_hbm,
    x, w1, w2, part, from_left, from_right, total, slots, acc, out,
    load_sem, sum_send, sum_recv, hid_send, hid_recv,
):
    chunks, _, block, wide = part.shape
    me = lax.axis_index("dp")
    left, right = lax.max(me - 1, 0), lax.min(me + 1, n - 1)
    has_left, has_right = me > 0, me < n - 1
    inner = has_left & has_right

    loads = [
        pltpu.make_async_copy(a, b, load_sem.at[i])
        for i, (a, b) in enumerate(((x_hbm, x), (w1_hbm, w1), (w2_hbm, w2)))
    ]
    for load in loads:
        load.start()

    barrier = pltpu.get_barrier_semaphore()

    @pl.when(has_left)
    def _():
        pl.semaphore_signal(barrier, inc=1, device_id={"dp": left}, device_id_type=MESH)

    @pl.when(has_right)
    def _():
        pl.semaphore_signal(barrier, inc=1, device_id={"dp": right}, device_id_type=MESH)

    pl.semaphore_wait(barrier, has_left.astype(jnp.int32) + has_right.astype(jnp.int32))

    def sum_right(c, b):
        return pltpu.make_async_remote_copy(
            part.at[c, b], from_left.at[c, b], sum_send.at[0, c, b], sum_recv.at[0, c, b],
            device_id={"dp": right}, device_id_type=MESH)

    def sum_left(c, b):
        return pltpu.make_async_remote_copy(
            part.at[c, b], from_right.at[c, b], sum_send.at[1, c, b], sum_recv.at[1, c, b],
            device_id={"dp": left}, device_id_type=MESH)

    def hid_right(c, b):
        return pltpu.make_async_remote_copy(
            slots.at[c, b], slots.at[c, b], hid_send.at[0, c, b], hid_recv.at[0, c, b],
            device_id={"dp": right}, device_id_type=MESH)

    def hid_left(c, b):
        return pltpu.make_async_remote_copy(
            slots.at[c, b], slots.at[c, b], hid_send.at[1, c, b], hid_recv.at[1, c, b],
            device_id={"dp": left}, device_id_type=MESH)

    def first(c):
        columns = pl.ds(pl.multiple_of(c * wide, wide), wide)

        def tile(b):
            part[c, b] = jnp.dot(
                x[pl.ds(pl.multiple_of(b * block, block), block), :], w1[:, columns],
                preferred_element_type=jnp.float32,
            ).astype(jnp.bfloat16)

        def up(i, carry):
            b = n - 1 - i
            tile(b)

            @pl.when((me == 0) & (b > 0))
            def _():
                sum_right(c, b).start()

            return carry

        def down(b, carry):
            tile(b)

            @pl.when((me == n - 1) & (b < n - 1))
            def _():
                sum_left(c, b).start()

            return carry

        @pl.when(me == 0)
        def _():
            lax.fori_loop(0, n, up, 0)

        @pl.when(me > 0)
        def _():
            lax.fori_loop(0, n, down, 0)

    def relay(c):
        def one(i, carry):
            b = n - 1 - i

            @pl.when(inner & (b > me))
            def _():
                sum_right(c, b).wait_recv()
                part[c, b] = (part[c, b].astype(jnp.float32) + from_left[c, b].astype(jnp.float32)).astype(jnp.bfloat16)
                sum_right(c, b).start()

            @pl.when(inner & (i < me))
            def _():
                sum_left(c, i).wait_recv()
                part[c, i] = (part[c, i].astype(jnp.float32) + from_right[c, i].astype(jnp.float32)).astype(jnp.bfloat16)
                sum_left(c, i).start()

            return carry

        lax.fori_loop(0, n, one, 0)

    def activate(c):
        total[...] = part[c, me].astype(jnp.float32) + bias[c]

        @pl.when(has_left)
        def _():
            sum_right(c, me).wait_recv()
            total[...] += from_left[c, me].astype(jnp.float32)

        @pl.when(has_right)
        def _():
            sum_left(c, me).wait_recv()
            total[...] += from_right[c, me].astype(jnp.float32)

        value = total[...]
        hidden = (0.5 * value * (1.0 + lax.erf(value * math.sqrt(0.5)))).astype(jnp.bfloat16)
        slots[c, me] = jnp.dot(permute[...], hidden, preferred_element_type=jnp.float32).astype(jnp.bfloat16)

        @pl.when(has_right)
        def _():
            hid_right(c, me).start()

        @pl.when(has_left)
        def _():
            hid_left(c, me).start()

    def spread(c):
        def one(k, carry):
            before, after = me - k, me + k

            @pl.when(before >= 0)
            def _():
                hid_right(c, before).wait_recv()

                @pl.when(has_right)
                def _():
                    hid_right(c, before).start()

            @pl.when(after < n)
            def _():
                hid_left(c, after).wait_recv()

                @pl.when(has_left)
                def _():
                    hid_left(c, after).start()

            return carry

        lax.fori_loop(1, n, one, 0)

    def second(c):
        depth = pl.ds(pl.multiple_of(c * wide, wide), wide)

        def one(b, carry):
            rows = pl.ds(pl.multiple_of(b * block, block), block)
            more = jnp.dot(slots[c, b], w2[depth, :], preferred_element_type=jnp.float32)

            @pl.when(c == 0)
            def _():
                acc[rows, :] = more

            @pl.when(c > 0)
            def _():
                acc[rows, :] += more

            return carry

        lax.fori_loop(0, n, one, 0)

    loads[0].wait()
    loads[1].wait()
    first(0)
    loads[2].wait()

    def step(s, carry):
        @pl.when(s + 1 < chunks)
        def _():
            first(s + 1)

        @pl.when(s < chunks)
        def _():
            relay(s)

        @pl.when((s >= 1) & (s <= chunks))
        def _():
            activate(s - 1)

        @pl.when(s >= 2)
        def _():
            spread(s - 2)
            second(s - 2)

        return carry

    lax.fori_loop(0, chunks + 2, step, 0)

    def finish(b, carry):
        rows = pl.ds(pl.multiple_of(b * block, block), block)
        out[rows, :] = acc[rows, :].astype(jnp.bfloat16)
        return carry

    lax.fori_loop(0, n, finish, 0)
    store = pltpu.make_async_copy(out, out_hbm, load_sem.at[0])
    store.start()

    def drain(c, carry):
        def one(b, inside):
            @pl.when(has_right & (b > me))
            def _():
                sum_right(c, b).wait_send()

            @pl.when(has_left & (b < me))
            def _():
                sum_left(c, b).wait_send()

            @pl.when(has_right & (b <= me))
            def _():
                hid_right(c, b).wait_send()

            @pl.when(has_left & (b >= me))
            def _():
                hid_left(c, b).wait_send()

            return inside

        return lax.fori_loop(0, n, one, carry)

    lax.fori_loop(0, chunks, drain, 0)
    store.wait()


def merger(x, w1, bias, permute, w2):
    n = lax.axis_size("dp")
    rows, depth = x.shape
    hidden, columns = w2.shape
    block = rows // n
    wide = 256 if hidden % 256 == 0 else 128
    chunks = hidden // wide
    any_space = pl.BlockSpec(memory_space=pl.ANY)
    vmem = pl.BlockSpec(memory_space=pltpu.VMEM)
    stack = pltpu.VMEM((chunks, n, block, wide), jnp.bfloat16)
    return pl.pallas_call(
        functools.partial(merger_kernel, n),
        out_shape=jax.ShapeDtypeStruct((rows, columns), jnp.bfloat16),
        in_specs=[any_space, any_space, vmem, vmem, any_space],
        out_specs=any_space,
        scratch_shapes=[
            pltpu.VMEM((rows, depth), jnp.bfloat16),
            pltpu.VMEM((depth, hidden), jnp.bfloat16),
            pltpu.VMEM((hidden, columns), jnp.bfloat16),
            stack,
            stack,
            stack,
            pltpu.VMEM((block, wide), jnp.float32),
            stack,
            pltpu.VMEM((rows, columns), jnp.float32),
            pltpu.VMEM((rows, columns), jnp.bfloat16),
            pltpu.SemaphoreType.DMA((3,)),
            pltpu.SemaphoreType.DMA((2, chunks, n)),
            pltpu.SemaphoreType.DMA((2, chunks, n)),
            pltpu.SemaphoreType.DMA((2, chunks, n)),
            pltpu.SemaphoreType.DMA((2, chunks, n)),
        ],
        compiler_params=pltpu.CompilerParams(
            collective_id=0, has_side_effects=True, vmem_limit_bytes=60 * 1024 * 1024
        ),
    )(x, w1, bias.reshape(chunks, 1, wide), permute, w2)


def place_kernel(
    n, y, out, half, across_sum, from_across, ready, landed, got,
    mate_send, mate_recv, across_send, across_recv, row_send, row_recv, end_send, end_recv,
):
    quarter = y.shape[3] // 4
    row, me = lax.axis_index("dp"), lax.axis_index("tensor")
    core, side = me % 2, me // 2
    mate, across = side * 2 + 1 - core, (1 - side) * 2 + core

    barrier = pltpu.get_barrier_semaphore()
    for k in range(1, 4):
        pl.semaphore_signal(barrier, inc=1, device_id={"tensor": (me + k) % 4}, device_id_type=MESH)
    for k in range(1, n):
        pl.semaphore_signal(barrier, inc=1, device_id={"dp": (row + k) % n}, device_id_type=MESH)
    pl.semaphore_wait(barrier, 3 + n - 1)

    def piece(index):
        return pl.ds(pl.multiple_of(index * quarter, quarter), quarter)

    def to_mate(i, j):
        return pltpu.make_async_remote_copy(
            y.at[i, :, :, piece((side + j) % 2 * 2 + 1 - core)], half.at[i, j], mate_send.at[i, j], mate_recv.at[i, j],
            device_id={"tensor": mate}, device_id_type=MESH)

    def to_across(i):
        return pltpu.make_async_remote_copy(
            across_sum.at[i], from_across.at[i], across_send.at[i], across_recv.at[i],
            device_id={"tensor": across}, device_id_type=MESH)

    def to_row(i, k):
        other = (row + k) % n
        return pltpu.make_async_remote_copy(
            ready.at[i, other], landed.at[row, i], row_send.at[i, k], row_recv.at[i, k],
            device_id={"dp": other}, device_id_type=MESH)

    def to_end(i, k, block):
        return pltpu.make_async_remote_copy(
            landed.at[block, i], got.at[me, i], end_send.at[i, k], end_recv.at[i, me],
            device_id={"tensor": block}, device_id_type=MESH)

    for i in range(n):
        for j in (1, 0):
            to_mate(i, j).start()

    for i in range(n):
        to_mate(i, 1).wait_recv()
        for s in range(n):
            across_sum[i, s] = (
                y[i, s, :, piece((1 - side) * 2 + core)].astype(jnp.float32) + half[i, 1, s].astype(jnp.float32)
            ).astype(jnp.bfloat16)
        to_across(i).start()

    for i in range(n):
        to_mate(i, 0).wait_recv()
        to_across(i).wait_recv()
        for s in range(n):
            ready[i, s] = (
                y[i, s, :, piece(me)].astype(jnp.float32)
                + half[i, 0, s].astype(jnp.float32)
                + from_across[i, s].astype(jnp.float32)
            ).astype(jnp.bfloat16)
        for k in range(1, n):
            to_row(i, k).start()
        landed[row, i] = ready[i, row]

    for i in range(n):
        for k in range(n):
            block = (row + n - k) % n
            if k:
                to_row(i, k).wait_recv()

            @pl.when(block == me)
            def _():
                got[me, i] = landed[block, i]

            @pl.when(block != me)
            def _():
                to_end(i, k, block).start()

    for i in range(n):
        for k in range(1, 4):
            other = (me + k) % 4
            pltpu.make_async_remote_copy(
                landed.at[0, i], got.at[other, i], end_send.at[i, 0], end_recv.at[i, other],
                device_id={"tensor": other}, device_id_type=MESH).wait_recv()
    for t in range(4):
        out[:, :, t * quarter:(t + 1) * quarter] = got[t]

    for i in range(n):
        for j in range(2):
            to_mate(i, j).wait_send()
        to_across(i).wait_send()
        for k in range(1, n):
            to_row(i, k).wait_send()
        for k in range(n):
            block = (row + n - k) % n

            @pl.when(block != me)
            def _():
                to_end(i, k, block).wait_send()


def place(second):
    n, _, capacity, columns = second.shape
    quarter = columns // 4
    vmem = pl.BlockSpec(memory_space=pltpu.VMEM)
    stack = pltpu.VMEM((n, n, capacity, quarter), jnp.bfloat16)
    return pl.pallas_call(
        functools.partial(place_kernel, n),
        out_shape=jax.ShapeDtypeStruct((n, capacity, columns), jnp.bfloat16),
        in_specs=[vmem],
        out_specs=vmem,
        scratch_shapes=[
            pltpu.VMEM((n, 2, n, capacity, quarter), jnp.bfloat16),
            stack,
            stack,
            stack,
            stack,
            stack,
            pltpu.SemaphoreType.DMA((n, 2)),
            pltpu.SemaphoreType.DMA((n, 2)),
            pltpu.SemaphoreType.DMA((n,)),
            pltpu.SemaphoreType.DMA((n,)),
            pltpu.SemaphoreType.DMA((n, n)),
            pltpu.SemaphoreType.DMA((n, n)),
            pltpu.SemaphoreType.DMA((n, n)),
            pltpu.SemaphoreType.DMA((n, n)),
        ],
        compiler_params=pltpu.CompilerParams(
            collective_id=1, has_side_effects=True, vmem_limit_bytes=40 * 1024 * 1024
        ),
    )(second)


def exchange(second, dp_count, tensor_count, capacity):
    if dp_count == tensor_count == 4 and capacity % 16 == 0 and second.shape[1] % 512 == 0:
        return place(second.reshape(dp_count, dp_count, capacity, -1)).reshape(dp_count * capacity, -1)
    second = lax.psum_scatter(second, "tensor", scatter_dimension=1, tiled=True)
    columns = second.shape[1]
    second = second.reshape(dp_count, dp_count, capacity, columns)
    second = lax.all_to_all(second, "dp", split_axis=1, concat_axis=0, tiled=False)
    blocks = dp_count // tensor_count
    second = second.reshape(tensor_count, blocks, dp_count * capacity, columns)
    second = lax.all_to_all(second, "tensor", split_axis=0, concat_axis=0, tiled=True)
    return second.transpose(2, 1, 0, 3).reshape(dp_count * capacity, -1)


def local(
    patches,
    grids,
    dest,
    norm_gain,
    qkv_weight,
    qkv_bias,
    proj_weight,
    proj_bias,
    merge_gain,
    w_first,
    b_first,
    w_second,
    b_second,
    text_embed,
):
    rows_dev, width = patches.shape
    images_dev = grids.shape[0]
    heads_dev = qkv_weight.shape[2] // HEAD_DIM
    dp_count = lax.axis_size("dp")
    tensor_count = lax.axis_size("tensor")
    seq_rows = text_embed.shape[0]
    capacity = images_dev * (MERGED // dp_count)
    live_count = grids[:, 0] * grids[:, 1]
    permute, slot_rows = placement(dest, live_count, dp_count, seq_rows, capacity)
    arrived_rows = lax.all_to_all(
        slot_rows.reshape(dp_count, capacity), "dp", split_axis=0, concat_axis=0, tiled=True
    ).reshape(-1)

    attended = attention(patches, live_count, norm_gain, qkv_weight, qkv_bias, images_dev, heads_dev)
    partial_value = jnp.dot(attended, proj_weight, preferred_element_type=jnp.float32).astype(jnp.bfloat16)
    summed = lax.psum_scatter(partial_value, "tensor", scatter_dimension=0, tiled=True).astype(jnp.float32)
    part = rows_dev // tensor_count
    own = lax.dynamic_slice_in_dim(patches, lax.axis_index("tensor") * part, part, 0)
    resid = own.astype(jnp.float32) + summed + proj_bias
    merged_in = rms_scale(resid, merge_gain).astype(jnp.bfloat16).reshape(part // 4, 4 * width)
    sliced = lax.all_to_all(
        merged_in.reshape(part // 4, dp_count, 4 * width // dp_count), "dp", split_axis=1, concat_axis=0, tiled=False
    )
    received = lax.all_gather(sliced, "tensor", axis=1, tiled=False)
    received = received.reshape(-1, 4 * width // dp_count)
    second = merger(received, w_first, b_first, permute, w_second)
    visual = exchange(second, dp_count, tensor_count, capacity)
    visual = (visual.astype(jnp.float32) + b_second).astype(jnp.bfloat16)
    hit = jnp.arange(seq_rows, dtype=jnp.int32)[:, None] == arrived_rows[None, :]
    placed = jnp.dot(hit.astype(jnp.bfloat16), visual, preferred_element_type=jnp.float32).astype(jnp.bfloat16)
    return jnp.where(jnp.any(hit, axis=1)[:, None], placed, text_embed)


def fused_kernel(
    seq_rows, lags,
    patches_hbm, grids, dest, gain, wqkv_hbm, bqkv, wproj_hbm, bproj, mgain, w1_hbm, bias, w2_hbm,
    out, hit_out, any_out,
    patches, wqkv, bpad, wproj, target, normed, raws, qs, ks, vs, att_f32, att_out, att_in, slices, rows_tbl, arrived, x,
    w1, w2, own, to_r, to_l, from_l, from_r, hidden, keep, give, from_mate, cross, from_across, ready, landed,
    load_sem, head_sem, tbl_send, tbl_recv, pm_send, pm_recv, pa_send, pa_recv, py_send, py_recv, pd_send, pd_recv,
    att_send, att_recv, z_send, fm_send, fa_send, x_recv,
    r_send, r_recv, l_send, l_recv, mate_send, mate_recv, across_send, across_recv,
    row_send, row_recv, end_send, end_recv,
):
    n, _, sides, few, width = x.shape
    nt = 2 * sides
    rows = patches.shape[0]
    block = rows // n
    half = block // sides
    merged = dest.shape[1]
    heads = qs.shape[0]
    lanes = qs.shape[2]
    count, _, wide = own.shape
    steps = count // n
    pieces = steps // sides
    pair = n // sides
    quarter = keep.shape[3]
    piece = ready.shape[3]
    row, me, group = lax.axis_index("dp"), lax.axis_index("tensor"), lax.axis_index("groups")
    core, side = me % 2, me // 2
    mate, across = side * 2 + 1 - core, (1 - side) * 2 + core
    left, right = lax.max(row - 1, 0), lax.min(row + 1, n - 1)
    has_left, has_right = row > 0, row < n - 1
    bf16, f32 = jnp.bfloat16, jnp.float32

    load_x = pltpu.make_async_copy(patches_hbm, patches, load_sem.at[0])
    load_p = pltpu.make_async_copy(wproj_hbm, wproj.at[me], load_sem.at[1])
    load_1 = pltpu.make_async_copy(w1_hbm, w1, load_sem.at[2])
    load_2 = pltpu.make_async_copy(w2_hbm, w2, load_sem.at[3])
    load_w = [
        pltpu.make_async_copy(
            wqkv_hbm.at[j, h * HEAD_DIM:(h + 1) * HEAD_DIM], wqkv.at[j, h * lanes:h * lanes + HEAD_DIM],
            head_sem.at[j, h])
        for j in range(3) for h in range(heads)
    ]
    load_p.start()
    load_x.start()
    for load in load_w:
        load.start()

    barrier = pltpu.get_barrier_semaphore()
    for k in range(1, nt):
        pl.semaphore_signal(barrier, inc=1, device_id={"tensor": (me + k) % nt}, device_id_type=MESH)
    for k in range(1, n):
        pl.semaphore_signal(barrier, inc=1, device_id={"dp": (row + k) % n}, device_id_type=MESH)
    pl.semaphore_signal(barrier, inc=1, device_id={"groups": 1 - group}, device_id_type=MESH)

    live = grids[0, 0] * grids[0, 1]
    dest_row = dest[...].astype(f32)

    def shards(value):
        total = jnp.zeros_like(value)
        for s in range(1, n):
            total += jnp.where(value >= float(s * seq_rows), 1.0, 0.0)
        return total

    square = (merged, merged)
    first_at = lax.broadcasted_iota(jnp.int32, square, 0)
    second_at = lax.broadcasted_iota(jnp.int32, square, 1)
    dest_col = jnp.sum(jnp.where(first_at == second_at, dest_row, 0.0), axis=1, keepdims=True)
    shard_row, shard_col = shards(dest_row), shards(dest_col)
    rank_col = jnp.sum(
        jnp.where((shard_row == shard_col) & (second_at < first_at), 1.0, 0.0), axis=1, keepdims=True)
    live_col = lax.broadcasted_iota(jnp.int32, (merged, 1), 0) * 4 < live
    rank_i, shard_i = rank_col.astype(jnp.int32), shard_col.astype(jnp.int32)
    slot_i = rank_i // piece * block + shard_i // 2 * half + shard_i % 2 * piece + rank_i % piece
    base_col = jnp.where(live_col, slot_i, -rows).astype(f32)

    ones_at = lax.broadcasted_iota(jnp.int32, (1, lanes), 1) == HEAD_DIM
    for j in range(3):
        for h in range(heads):
            bpad[j:j + 1, h * lanes:(h + 1) * lanes] = jnp.where(ones_at, 0.0 if j == 1 else 1.0, 0.0)
            bpad[j:j + 1, h * lanes:h * lanes + HEAD_DIM] = bqkv[j:j + 1, h * HEAD_DIM:(h + 1) * HEAD_DIM]
            wqkv[j, h * lanes + HEAD_DIM:(h + 1) * lanes, :] = jnp.zeros((lanes - HEAD_DIM, width), bf16)

    pl.semaphore_wait(barrier, nt - 1 + n - 1 + 1)

    def remote(source, to, send, recv, device):
        return pltpu.make_async_remote_copy(source, to, send, recv, device_id=device, device_id_type=MESH)

    span = wproj.shape[1] // 4

    def strip(g, a):
        return pl.ds(pl.multiple_of((g * 2 + a) * span, span), span)

    def same(ref, send, recv, device):
        return remote(ref, ref, send, recv, device)

    proj_mate = same(wproj.at[me], pm_send, pm_recv, {"tensor": mate})
    proj_across = [
        same(wproj.at[me, strip(group, a)], pa_send.at[a], pa_recv.at[a], {"tensor": across}) for a in range(2)]
    proj_got = [
        same(wproj.at[across, strip(group, a)], pa_send.at[a], pa_recv.at[a], {"tensor": across}) for a in range(2)]
    proj_peer = [
        same(wproj.at[across, strip(group, a)], py_send.at[a], py_recv.at[a], {"groups": 1 - group})
        for a in range(2)]
    proj_peer_got = [
        same(wproj.at[across, strip(1 - group, a)], py_send.at[a], py_recv.at[a], {"groups": 1 - group})
        for a in range(2)]

    def proj_diag(g, a, at):
        return same(wproj.at[across, strip(g, a)], pd_send.at[at, a], pd_recv.at[at, a], {"tensor": mate})

    load_p.wait()
    for copy in proj_across:
        copy.start()
    proj_mate.start()

    patch_at = lax.broadcasted_iota(jnp.int32, (1, rows), 1)
    row4 = lax.broadcasted_iota(jnp.int32, (merged, 1), 0) * 4
    inside = (patch_at >= row4) & (patch_at < row4 + 4)
    base_row = jnp.sum(jnp.where(inside, base_col, 0.0), axis=0, keepdims=True).astype(jnp.int32)
    target[...] = jnp.broadcast_to(base_row + patch_at % 4 * few, target.shape)

    slots = rows_tbl.shape[2]
    code_col = jnp.where(live_col, shard_col * slots + rank_col + (row * (slots // n)).astype(f32), -1.0)
    lane_at = lax.broadcasted_iota(jnp.int32, (merged, n * slots), 1).astype(f32)
    local_col = dest_col - shard_col * seq_rows
    table = jnp.sum(jnp.where(lane_at == code_col, local_col + 1.0, 0.0), axis=0, keepdims=True) - 1.0
    for s in range(n):
        rows_tbl[s] = jnp.broadcast_to(table[:, s * slots:(s + 1) * slots], (8, slots)).astype(jnp.int32)
    arrived[row] = rows_tbl[row]

    def send_table(k):
        to = (row + k) % n
        return remote(rows_tbl.at[to], arrived.at[row], tbl_send.at[k], tbl_recv.at[row], {"dp": to})

    for k in range(1, n):
        send_table(k).start()

    load_x.wait()
    for load in load_w:
        load.wait()
    load_1.start()
    load_2.start()

    mask_at = lax.broadcasted_iota(jnp.int32, (block, lanes), 1) == HEAD_DIM

    def project(b, carry):
        @pl.when(b == 2)
        def _():
            proj_got[0].wait_recv()
            proj_peer[0].start()
            proj_diag(group, 0, 0).start()

        at = pl.ds(pl.multiple_of(b * block, block), block)
        hit = jnp.where(
            target[0:1, :] == lax.broadcasted_iota(jnp.int32, (block, rows), 0) + b * block, 1.0, 0.0)
        valid = jnp.sum(hit, axis=1, keepdims=True)
        raw = jnp.dot(hit.astype(bf16), patches[...], preferred_element_type=f32)
        for s in range(sides):
            raws[b, s] = raw[s * half:(s + 1) * half, :].astype(bf16)
        normed[...] = rms_scale(raw, gain[...].reshape(1, width)).astype(bf16)
        for j, store in enumerate((qs, ks, vs)):
            acc = lax.dot_general(
                normed[...], wqkv[j], (((1,), (1,)), ((), ())), preferred_element_type=f32) + bpad[j:j + 1, :]
            for h in range(heads):
                value = acc[:, h * lanes:(h + 1) * lanes]
                if j == 1:
                    value = jnp.where(mask_at, jnp.where(valid > 0.5, 0.0, -1e30), value)
                store[h, at, :] = value.astype(bf16)
        return carry

    lax.fori_loop(0, n, project, 0)

    proj_got[1].wait_recv()
    proj_peer[1].start()
    proj_diag(group, 1, 0).start()

    scale = math.log2(math.e) / math.sqrt(HEAD_DIM)

    def att_to(b, s):
        return remote(
            att_out.at[b, s], att_in.at[b // 2, me], att_send.at[b, s], att_recv.at[b // 2, me],
            {"tensor": s * 2 + b % 2})

    def att_got(b, source):
        return remote(
            att_out.at[b, 0], att_in.at[b // 2, source], att_send.at[b, 0], att_recv.at[b // 2, source],
            {"tensor": mate})

    def z_to(b, k):
        to = (row + k) % n
        return remote(
            slices.at[b // 2, to], x.at[b, row, side], z_send.at[b // 2, k], x_recv.at[b, row, side], {"dp": to})

    def to_mate_x(b, s, i):
        return same(x.at[b, i, s], fm_send.at[b // 2, i, s], x_recv.at[b, i, s], {"tensor": mate})

    def to_across_x(b, i):
        return same(x.at[b, i, side], fa_send.at[b // 2, i], x_recv.at[b, i, side], {"tensor": across})

    def x_got(b, s, i):
        return same(x.at[b, i, s], fm_send.at[b // 2, i, s], x_recv.at[b, i, s], {"tensor": mate})

    def forward(b):
        for k in range(1, n):
            source = (row + n - k) % n
            x_got(b, side, source).wait_recv()
            to_across_x(b, source).start()
            to_mate_x(b, side, source).start()

    def attend(it, carry):
        @pl.when(it < n)
        def _():
            b = lax.min(it, n - 1)
            at = pl.ds(pl.multiple_of(b * block, block), block)
            for h in range(heads):
                scores = lax.dot_general(
                    qs[h, at, :], ks[h], (((1,), (1,)), ((), ())), preferred_element_type=f32)
                peak = jnp.max(scores, axis=1, keepdims=True)
                weights = jnp.exp2((scores - peak) * scale).astype(bf16)
                mixed = jnp.dot(weights, vs[h], preferred_element_type=f32)
                mixed = mixed * (1.0 / mixed[:, HEAD_DIM:HEAD_DIM + 1])
                att_f32[:, h * HEAD_DIM:(h + 1) * HEAD_DIM] = mixed[:, 0:HEAD_DIM]
            for s in range(sides):
                att_out[b, s] = att_f32[s * half:(s + 1) * half, :].astype(bf16)
                owner = s * 2 + b % 2

                @pl.when(owner != me)
                def _():
                    att_to(b, s).start()

                @pl.when(owner == me)
                def _():
                    att_in[b // 2, me] = att_out[b, s]

        @pl.when(it == 1)
        def _():
            proj_mate.wait_recv()
            for a in range(2):
                proj_peer_got[a].wait_recv()
                proj_diag(1 - group, a, 1).start()
            for a in range(2):
                proj_diag(group, a, 0).wait_recv()
                proj_diag(1 - group, a, 1).wait_recv()

        @pl.when((it == n - 1) & (core == 0))
        def _():
            forward(0)

        last = lax.max(it, 1) - 1

        @pl.when((it >= 1) & (last % 2 == core))
        def _():
            for k in range(1, nt):
                att_got(last, (me + k) % nt).wait_recv()
            total = raws[last, side].astype(f32) + bproj[...].reshape(1, width)
            for t in range(nt):
                total += jnp.dot(att_in[last // 2, t], wproj[t], preferred_element_type=f32)
            done = rms_scale(total, mgain[...].reshape(1, width)).astype(bf16)
            for k in range(n):
                slices[last // 2, k] = done[k * few:(k + 1) * few, :]
            for k in range(n - 1, 0, -1):
                z_to(last, k).start()
            x[last, row, side] = slices[last // 2, row]
            to_across_x(last, row).start()
            to_mate_x(last, side, row).start()

        return carry

    lax.fori_loop(0, n + 1, attend, 0)

    def forward_across(b):
        for k in range(n):
            source = (row + n - k) % n
            x_got(b, 1 - side, source).wait_recv()
            to_mate_x(b, 1 - side, source).start()

    def await_x(b):
        @pl.when(b % 2 != core)
        def _():
            for s in range(sides):
                for i in range(n):
                    x_got(b, s, i).wait_recv()

    def go_right(c):
        return remote(to_r.at[c], from_l.at[c], r_send.at[c], r_recv.at[c], {"dp": right})

    def go_left(c):
        return remote(to_l.at[c], from_r.at[c], l_send.at[c], l_recv.at[c], {"dp": left})

    def first(b, j):
        columns = pl.ds(pl.multiple_of(j * wide, wide), wide)
        partial = jnp.dot(x[b].reshape(block, width), w1[:, columns], preferred_element_type=f32)
        for h in range(sides):
            own[b * steps + h * pieces + j] = partial[h * half:(h + 1) * half, :]

    def begin(c):
        @pl.when(row == 0)
        def _():
            to_r[c] = own[c].astype(bf16)
            go_right(c).start()

        @pl.when(row == n - 1)
        def _():
            to_l[c] = own[c].astype(bf16)
            go_left(c).start()

    def relay(stage, c):
        @pl.when(row == stage)
        def _():
            go_right(c).wait_recv()
            to_r[c] = (own[c] + from_l[c].astype(f32)).astype(bf16)
            go_right(c).start()

        @pl.when(row == n - 1 - stage)
        def _():
            go_left(c).wait_recv()
            to_l[c] = (own[c] + from_r[c].astype(f32)).astype(bf16)
            go_left(c).start()

    def activate(c):
        columns = pl.ds(pl.multiple_of(c % pieces * wide, wide), wide)

        @pl.when(row == n - 1)
        def _():
            go_right(c).wait_recv()

        @pl.when(row == 0)
        def _():
            go_left(c).wait_recv()

        @pl.when(has_left)
        def _():
            own[c] += from_l[c].astype(f32)

        @pl.when(has_right)
        def _():
            own[c] += from_r[c].astype(f32)

        value = own[c] + bias[columns].reshape(1, wide)
        hidden[:, columns] = (0.5 * value * (1.0 + lax.erf(value * math.sqrt(0.5)))).astype(bf16)

    def columns_of(s, c):
        return pl.ds(pl.multiple_of((s * 2 + c) * quarter, quarter), quarter)

    def to_mate(b, s):
        return remote(give.at[b, s], from_mate.at[b, s], mate_send.at[b, s], mate_recv.at[b, s], {"tensor": mate})

    def to_across(b):
        return remote(cross.at[b], from_across.at[b], across_send.at[b], across_recv.at[b], {"tensor": across})

    def to_row(b, k):
        to = (row + k) % n
        return remote(ready.at[b, to], landed.at[b, row], row_send.at[b, k], row_recv.at[b, row], {"dp": to})

    def quarter_of(t):
        return pl.ds(pl.multiple_of(t * quarter, quarter), quarter)

    def to_end(g, d):
        at = pl.ds(g % sides * pair, pair)
        return remote(
            landed.at[g, d], out.at[at, g // sides, :, quarter_of(me)], end_send.at[g, d], end_recv.at[g, me],
            {"tensor": d})

    def second(g):
        def product(columns):
            return jnp.dot(hidden[...], w2[:, columns], preferred_element_type=f32)

        for s in (1 - side, side):
            give[g, s] = product(columns_of(s, 1 - core)).astype(bf16)
            to_mate(g, s).start()
        for s in (1 - side, side):
            keep[g % 2, s] = product(columns_of(s, core))

    def chip_sum(b):
        to_mate(b, 1 - side).wait_recv()
        cross[b] = (keep[b % 2, 1 - side] + from_mate[b, 1 - side].astype(f32)).astype(bf16)
        to_across(b).start()

    def spread(b):
        to_mate(b, side).wait_recv()
        to_across(b).wait_recv()
        value = keep[b % 2, side] + from_mate[b, side].astype(f32) + from_across[b].astype(f32)
        value = value.astype(bf16)
        for s in range(n):
            for i in range(pair):
                at = (i * n + s) * piece
                ready[b, s, i] = value[at:at + piece, :]
        for k in range(n - 1, 0, -1):
            to_row(b, k).start()
        landed[b, row] = ready[b, row]

    def deliver(b):
        for k in range(n):
            source = (row + n - k) % n
            if k:
                remote(
                    ready.at[b, 0], landed.at[b, source], row_send.at[b, 0], row_recv.at[b, source], {"dp": left}
                ).wait_recv()

            @pl.when(source == me)
            def _():
                out[pl.ds(b % sides * pair, pair), b // sides, :, quarter_of(me)] = landed[b, source]

            @pl.when(source != me)
            def _():
                to_end(b, source).start()

    lead, hop, fill, offsets = lags

    @pl.when(core == 0)
    def _():
        forward_across(0)

    @pl.when(core == 1)
    def _():
        forward(1)

    for k in range(1, n):
        source = (row + n - k) % n
        remote(rows_tbl.at[0], arrived.at[source], tbl_send.at[0], tbl_recv.at[source], {"dp": source}).wait_recv()

    at_slot = arrived[0, 0:1, :]
    for i in range(1, n):
        at_slot = jnp.maximum(at_slot, arrived[i, 0:1, :])
    match = jnp.where(
        lax.broadcasted_iota(jnp.int32, hit_out.shape, 0) == at_slot, 1.0, 0.0)
    hit_out[...] = match.astype(bf16)
    any_out[...] = jnp.broadcast_to(jnp.max(match, axis=1, keepdims=True), any_out.shape)

    load_1.wait()
    load_2.wait()
    after = tuple(zip(offsets, (second, chip_sum, spread, deliver)))

    def step(u, carry):
        @pl.when((u < count) & (u % steps < pieces))
        def _():
            @pl.when(u % steps == 0)
            def _():
                await_x(u // steps)

            first(u // steps, u % steps)

        @pl.when(u < count)
        def _():
            begin(u)

        @pl.when((u == 1) & (core == 1))
        def _():
            forward_across(1)

        @pl.when(u == 8)
        def _():
            forward(2 + core)

        @pl.when(u == 12)
        def _():
            forward_across(2 + core)

        for stage in range(1, n - 1):
            late = lead + (stage - 1) * hop

            @pl.when((u >= late) & (u < count + late))
            def _():
                relay(stage, u - late)

        @pl.when((u >= lead + fill) & (u < count + lead + fill))
        def _():
            activate(u - lead - fill)

        for offset, work in after:
            late = lead + fill + offset + pieces - 1

            @pl.when((u >= late) & (u < count + late) & (lax.max(u - late, 0) % pieces == 0))
            def _():
                work((u - late) // pieces)

        return carry

    lax.fori_loop(0, count + lead + fill + offsets[-1], step, 0)

    for g in range(n * sides):
        for k in range(1, nt):
            source = (me + k) % nt
            remote(
                landed.at[g, 0], out.at[g % sides * pair:(g % sides + 1) * pair, g // sides, :, quarter_of(source)],
                end_send.at[g, 0], end_recv.at[g, source], {"tensor": mate},
            ).wait_recv()
    def drain(c, carry):
        @pl.when(has_right)
        def _():
            go_right(c).wait_send()

        @pl.when(has_left)
        def _():
            go_left(c).wait_send()

        return carry

    lax.fori_loop(0, count, drain, 0)
    proj_mate.wait_send()
    for a in range(2):
        proj_across[a].wait_send()
        proj_peer[a].wait_send()
        proj_diag(group, a, 0).wait_send()
        proj_diag(1 - group, a, 1).wait_send()
    for k in range(1, n):
        send_table(k).wait_send()
    for b in range(n):
        for s in range(sides):
            @pl.when(s * 2 + b % 2 != me)
            def _():
                att_to(b, s).wait_send()

    for g in range(n * sides):
        for s in range(sides):
            to_mate(g, s).wait_send()
        to_across(g).wait_send()
        for k in range(1, n):
            to_row(g, k).wait_send()
            to_end(g, (me + k) % nt).wait_send()
    for q in range(2):
        b = 2 * q + core
        for k in range(1, n):
            z_to(b, k).wait_send()
        for i in range(n):
            to_across_x(b, i).wait_send()
            for s in range(sides):
                to_mate_x(b, s, i).wait_send()


def fused(
    patches, grids, dest, norm_gain, qkv_weight, qkv_bias, proj_weight, proj_bias, merge_gain,
    w_first, b_first, w_second, seq_rows,
):
    n, nt = lax.axis_size("dp"), lax.axis_size("tensor")
    sides = nt // 2
    rows, width = patches.shape
    span = qkv_weight.shape[2]
    heads = span // HEAD_DIM
    block = rows // n
    half = block // sides
    few = half // 4
    hidden, columns = w_second.shape
    wide, lanes = 256, 128
    pieces = hidden // wide
    steps = pieces * sides
    count = n * steps
    quarter = columns // nt
    piece = few // 2
    any_space = pl.BlockSpec(memory_space=pl.ANY)
    vmem = pl.BlockSpec(memory_space=pltpu.VMEM)
    smem = pl.BlockSpec(memory_space=pltpu.SMEM)
    dma = pltpu.SemaphoreType.DMA
    bf16, f32 = jnp.bfloat16, jnp.float32
    heads_shape = pltpu.VMEM((heads, rows, lanes), bf16)
    stack = pltpu.VMEM((count, half, wide), bf16)
    units = n * sides
    slots = n * n * piece
    tiles = pltpu.VMEM((units, 2, half, quarter), bf16)
    one = pltpu.VMEM((units, half, quarter), bf16)
    moved = pltpu.VMEM((units, n, n // sides, piece, quarter), bf16)
    lags = (4, 3, 6, (0, 2, 6, 12))
    return pl.pallas_call(
        functools.partial(fused_kernel, seq_rows, lags),
        out_shape=(
            jax.ShapeDtypeStruct((n, n, piece, columns), bf16),
            jax.ShapeDtypeStruct((seq_rows, slots), bf16),
            jax.ShapeDtypeStruct((seq_rows, lanes), f32),
        ),
        in_specs=[
            any_space, smem, vmem, vmem, any_space, vmem, any_space, vmem, vmem, any_space, vmem, any_space],
        out_specs=(vmem, vmem, vmem),
        scratch_shapes=[
            pltpu.VMEM((rows, width), bf16),
            pltpu.VMEM((3, heads * lanes, width), bf16),
            pltpu.VMEM((3, heads * lanes), f32),
            pltpu.VMEM((nt, span, width), bf16),
            pltpu.VMEM((8, rows), jnp.int32),
            pltpu.VMEM((block, width), bf16),
            pltpu.VMEM((n, sides, half, width), bf16),
            heads_shape, heads_shape, heads_shape,
            pltpu.VMEM((block, span), f32),
            pltpu.VMEM((n, sides, half, span), bf16),
            pltpu.VMEM((n // 2, nt, half, span), bf16),
            pltpu.VMEM((n // 2, n, few, width), bf16),
            pltpu.VMEM((n, 8, slots), jnp.int32),
            pltpu.VMEM((n, 8, slots), jnp.int32),
            pltpu.VMEM((n, n, sides, few, width), bf16),
            pltpu.VMEM(w_first.shape, bf16),
            pltpu.VMEM(w_second.shape, bf16),
            pltpu.VMEM((count, half, wide), f32),
            stack, stack, stack, stack,
            pltpu.VMEM((half, hidden), bf16),
            pltpu.VMEM((2, 2, half, quarter), f32),
            tiles, tiles, one, one, moved, moved,
            dma((4,)), dma((3, heads)), dma((n,)), dma((n,)), dma, dma, dma((2,)), dma((2,)), dma((2,)), dma((2,)),
            dma((2, 2)), dma((2, 2)),
            dma((n, sides)), dma((n // 2, nt)), dma((n // 2, n)), dma((n // 2, n, sides)), dma((n // 2, n)),
            dma((n, n, sides)),
            dma((count,)), dma((count,)), dma((count,)), dma((count,)),
            dma((units, 2)), dma((units, 2)), dma((units,)), dma((units,)), dma((units, n)), dma((units, n)),
            dma((units, nt)), dma((units, nt)),
        ],
        compiler_params=pltpu.CompilerParams(
            collective_id=2, has_side_effects=True, vmem_limit_bytes=63 * 1024 * 1024
        ),
    )(
        patches, grids, dest, norm_gain, qkv_weight.swapaxes(1, 2), qkv_bias, proj_weight, proj_bias, merge_gain,
        w_first, b_first, w_second,
    )


def local_fast(
    patches,
    grids,
    dest,
    norm_gain,
    qkv_weight,
    qkv_bias,
    proj_weight,
    proj_bias,
    merge_gain,
    w_first,
    b_first,
    w_second,
    b_second,
    text_embed,
):
    seq_rows = text_embed.shape[0]
    visual, hit, taken = fused(
        patches, grids, dest, norm_gain, qkv_weight, qkv_bias, proj_weight, proj_bias, merge_gain,
        w_first, b_first, w_second, seq_rows)
    visual = visual.reshape(-1, visual.shape[3])
    placed = jnp.dot(hit, visual, preferred_element_type=jnp.float32)
    return jnp.where(taken[:, :1] > 0.5, (placed + b_second).astype(jnp.bfloat16), text_embed)


def fits(patches, grids, dest, qkv_weight, w_first, w_second):
    n, nt = lax.axis_size("dp"), lax.axis_size("tensor")
    rows, width = patches.shape
    return (
        n == nt == 4
        and lax.axis_size("groups") == 2
        and grids.shape[0] == 1
        and rows == PATCHES
        and dest.shape[1] == MERGED
        and w_first.shape[0] == width
        and w_second.shape[0] % 256 == 0
        and w_second.shape[1] % 512 == 0
        and qkv_weight.shape[2] % 64 == 0
    )


def chosen(*args):
    run = local_fast if fits(args[0], args[1], args[2], args[4], args[9], args[11]) else local
    return run(*args)


def solution(mesh):
    in_specs = (
        P(("groups", "dp"), None),
        P(("groups", "dp"), None),
        P(("groups", "dp"), None),
        P(),
        P(None, None, "tensor"),
        P(None, "tensor"),
        P("tensor", None),
        P(),
        P(),
        P("dp", "tensor"),
        P("tensor"),
        P("tensor", "dp"),
        P("tensor"),
        P(("groups", "dp"), "tensor"),
    )
    out_specs = P(("groups", "dp"), "tensor")
    return jax.shard_map(chosen, mesh=mesh, in_specs=in_specs, out_specs=out_specs, check_vma=False)
```

```python
import functools
import math

import jax
import jax.numpy as jnp
from jax import lax
from jax.experimental import pallas as pl
from jax.experimental.pallas import tpu as pltpu
from jax.sharding import PartitionSpec as P

MESH = pl.DeviceIdType.MESH

HEAD_DIM = 80
PATCHES = 1024
MERGED = 256


def rms_scale(values, gain):
    return values * lax.rsqrt(jnp.mean(values * values, axis=-1, keepdims=True) + 1e-06) * gain


def placement(dest, live_count, dp_count, seq_rows, capacity):
    merged_dev = dest.size
    live_rows = (jnp.arange(MERGED, dtype=jnp.int32)[None, :] < (live_count // 4)[:, None]).reshape(merged_dev)
    dest_flat = dest.reshape(merged_dev)
    shard_id = jnp.where(live_rows, dest_flat // seq_rows, dp_count)
    local_row = dest_flat % seq_rows
    index = jnp.arange(merged_dev, dtype=jnp.int32)
    earlier = (shard_id[:, None] == shard_id[None, :]) & (index[None, :] < index[:, None])
    rank = jnp.sum(earlier.astype(jnp.int32), axis=1)
    slot = jnp.where(live_rows & (rank < capacity), shard_id * capacity + rank, -1)
    hit = jnp.arange(dp_count * capacity, dtype=jnp.int32)[:, None] == slot[None, :]
    rows = jnp.max(jnp.where(hit, local_row[None, :], -1), axis=1)
    return hit.astype(jnp.bfloat16), rows


def attention(patches, live_count, norm_gain, qkv_weight, qkv_bias, images_dev, heads_dev):
    normed = rms_scale(patches.astype(jnp.float32), norm_gain).astype(jnp.bfloat16)
    projected = (
        jnp.einsum("rv,jvc->jrc", normed, qkv_weight, preferred_element_type=jnp.float32)
        + qkv_bias[:, None, :]
    )
    projected = projected.astype(jnp.bfloat16).reshape(3, images_dev, PATCHES, heads_dev, HEAD_DIM)
    scores = jnp.einsum(
        "iqhd,ikhd->ihqk", projected[0], projected[1], preferred_element_type=jnp.float32
    ) / math.sqrt(HEAD_DIM)
    live_keys = jnp.arange(PATCHES, dtype=jnp.int32)[None, :] < live_count[:, None]
    scores = jnp.where(live_keys[:, None, None, :], scores, jnp.float32(-1e30))
    peak_score = jnp.max(scores, axis=-1, keepdims=True)
    exponent = jnp.exp(scores - peak_score)
    weights = (exponent / jnp.sum(exponent, axis=-1, keepdims=True)).astype(jnp.bfloat16)
    attended = jnp.einsum(
        "ihqk,ikhd->iqhd", weights, projected[2], preferred_element_type=jnp.float32
    )
    return attended.astype(jnp.bfloat16).reshape(patches.shape[0], heads_dev * HEAD_DIM)


def merger_kernel(
    n, x_hbm, w1_hbm, bias, permute, w2_hbm, out_hbm,
    x, w1, w2, part, from_left, from_right, total, slots, acc, out,
    load_sem, sum_send, sum_recv, hid_send, hid_recv,
):
    chunks, _, block, wide = part.shape
    me = lax.axis_index("dp")
    left, right = lax.max(me - 1, 0), lax.min(me + 1, n - 1)
    has_left, has_right = me > 0, me < n - 1
    inner = has_left & has_right

    loads = [
        pltpu.make_async_copy(a, b, load_sem.at[i])
        for i, (a, b) in enumerate(((x_hbm, x), (w1_hbm, w1), (w2_hbm, w2)))
    ]
    for load in loads:
        load.start()

    barrier = pltpu.get_barrier_semaphore()

    @pl.when(has_left)
    def _():
        pl.semaphore_signal(barrier, inc=1, device_id={"dp": left}, device_id_type=MESH)

    @pl.when(has_right)
    def _():
        pl.semaphore_signal(barrier, inc=1, device_id={"dp": right}, device_id_type=MESH)

    pl.semaphore_wait(barrier, has_left.astype(jnp.int32) + has_right.astype(jnp.int32))

    def sum_right(c, b):
        return pltpu.make_async_remote_copy(
            part.at[c, b], from_left.at[c, b], sum_send.at[0, c, b], sum_recv.at[0, c, b],
            device_id={"dp": right}, device_id_type=MESH)

    def sum_left(c, b):
        return pltpu.make_async_remote_copy(
            part.at[c, b], from_right.at[c, b], sum_send.at[1, c, b], sum_recv.at[1, c, b],
            device_id={"dp": left}, device_id_type=MESH)

    def hid_right(c, b):
        return pltpu.make_async_remote_copy(
            slots.at[c, b], slots.at[c, b], hid_send.at[0, c, b], hid_recv.at[0, c, b],
            device_id={"dp": right}, device_id_type=MESH)

    def hid_left(c, b):
        return pltpu.make_async_remote_copy(
            slots.at[c, b], slots.at[c, b], hid_send.at[1, c, b], hid_recv.at[1, c, b],
            device_id={"dp": left}, device_id_type=MESH)

    def first(c):
        columns = pl.ds(pl.multiple_of(c * wide, wide), wide)

        def tile(b):
            part[c, b] = jnp.dot(
                x[pl.ds(pl.multiple_of(b * block, block), block), :], w1[:, columns],
                preferred_element_type=jnp.float32,
            ).astype(jnp.bfloat16)

        def up(i, carry):
            b = n - 1 - i
            tile(b)

            @pl.when((me == 0) & (b > 0))
            def _():
                sum_right(c, b).start()

            return carry

        def down(b, carry):
            tile(b)

            @pl.when((me == n - 1) & (b < n - 1))
            def _():
                sum_left(c, b).start()

            return carry

        @pl.when(me == 0)
        def _():
            lax.fori_loop(0, n, up, 0)

        @pl.when(me > 0)
        def _():
            lax.fori_loop(0, n, down, 0)

    def relay(c):
        def one(i, carry):
            b = n - 1 - i

            @pl.when(inner & (b > me))
            def _():
                sum_right(c, b).wait_recv()
                part[c, b] = (part[c, b].astype(jnp.float32) + from_left[c, b].astype(jnp.float32)).astype(jnp.bfloat16)
                sum_right(c, b).start()

            @pl.when(inner & (i < me))
            def _():
                sum_left(c, i).wait_recv()
                part[c, i] = (part[c, i].astype(jnp.float32) + from_right[c, i].astype(jnp.float32)).astype(jnp.bfloat16)
                sum_left(c, i).start()

            return carry

        lax.fori_loop(0, n, one, 0)

    def activate(c):
        total[...] = part[c, me].astype(jnp.float32) + bias[c]

        @pl.when(has_left)
        def _():
            sum_right(c, me).wait_recv()
            total[...] += from_left[c, me].astype(jnp.float32)

        @pl.when(has_right)
        def _():
            sum_left(c, me).wait_recv()
            total[...] += from_right[c, me].astype(jnp.float32)

        value = total[...]
        hidden = (0.5 * value * (1.0 + lax.erf(value * math.sqrt(0.5)))).astype(jnp.bfloat16)
        slots[c, me] = jnp.dot(permute[...], hidden, preferred_element_type=jnp.float32).astype(jnp.bfloat16)

        @pl.when(has_right)
        def _():
            hid_right(c, me).start()

        @pl.when(has_left)
        def _():
            hid_left(c, me).start()

    def spread(c):
        def one(k, carry):
            before, after = me - k, me + k

            @pl.when(before >= 0)
            def _():
                hid_right(c, before).wait_recv()

                @pl.when(has_right)
                def _():
                    hid_right(c, before).start()

            @pl.when(after < n)
            def _():
                hid_left(c, after).wait_recv()

                @pl.when(has_left)
                def _():
                    hid_left(c, after).start()

            return carry

        lax.fori_loop(1, n, one, 0)

    def second(c):
        depth = pl.ds(pl.multiple_of(c * wide, wide), wide)

        def one(b, carry):
            rows = pl.ds(pl.multiple_of(b * block, block), block)
            more = jnp.dot(slots[c, b], w2[depth, :], preferred_element_type=jnp.float32)

            @pl.when(c == 0)
            def _():
                acc[rows, :] = more

            @pl.when(c > 0)
            def _():
                acc[rows, :] += more

            return carry

        lax.fori_loop(0, n, one, 0)

    loads[0].wait()
    loads[1].wait()
    first(0)
    loads[2].wait()

    def step(s, carry):
        @pl.when(s + 1 < chunks)
        def _():
            first(s + 1)

        @pl.when(s < chunks)
        def _():
            relay(s)

        @pl.when((s >= 1) & (s <= chunks))
        def _():
            activate(s - 1)

        @pl.when(s >= 2)
        def _():
            spread(s - 2)
            second(s - 2)

        return carry

    lax.fori_loop(0, chunks + 2, step, 0)

    def finish(b, carry):
        rows = pl.ds(pl.multiple_of(b * block, block), block)
        out[rows, :] = acc[rows, :].astype(jnp.bfloat16)
        return carry

    lax.fori_loop(0, n, finish, 0)
    store = pltpu.make_async_copy(out, out_hbm, load_sem.at[0])
    store.start()

    def drain(c, carry):
        def one(b, inside):
            @pl.when(has_right & (b > me))
            def _():
                sum_right(c, b).wait_send()

            @pl.when(has_left & (b < me))
            def _():
                sum_left(c, b).wait_send()

            @pl.when(has_right & (b <= me))
            def _():
                hid_right(c, b).wait_send()

            @pl.when(has_left & (b >= me))
            def _():
                hid_left(c, b).wait_send()

            return inside

        return lax.fori_loop(0, n, one, carry)

    lax.fori_loop(0, chunks, drain, 0)
    store.wait()


def merger(x, w1, bias, permute, w2):
    n = lax.axis_size("dp")
    rows, depth = x.shape
    hidden, columns = w2.shape
    block = rows // n
    wide = 256 if hidden % 256 == 0 else 128
    chunks = hidden // wide
    any_space = pl.BlockSpec(memory_space=pl.ANY)
    vmem = pl.BlockSpec(memory_space=pltpu.VMEM)
    stack = pltpu.VMEM((chunks, n, block, wide), jnp.bfloat16)
    return pl.pallas_call(
        functools.partial(merger_kernel, n),
        out_shape=jax.ShapeDtypeStruct((rows, columns), jnp.bfloat16),
        in_specs=[any_space, any_space, vmem, vmem, any_space],
        out_specs=any_space,
        scratch_shapes=[
            pltpu.VMEM((rows, depth), jnp.bfloat16),
            pltpu.VMEM((depth, hidden), jnp.bfloat16),
            pltpu.VMEM((hidden, columns), jnp.bfloat16),
            stack,
            stack,
            stack,
            pltpu.VMEM((block, wide), jnp.float32),
            stack,
            pltpu.VMEM((rows, columns), jnp.float32),
            pltpu.VMEM((rows, columns), jnp.bfloat16),
            pltpu.SemaphoreType.DMA((3,)),
            pltpu.SemaphoreType.DMA((2, chunks, n)),
            pltpu.SemaphoreType.DMA((2, chunks, n)),
            pltpu.SemaphoreType.DMA((2, chunks, n)),
            pltpu.SemaphoreType.DMA((2, chunks, n)),
        ],
        compiler_params=pltpu.CompilerParams(
            collective_id=0, has_side_effects=True, vmem_limit_bytes=60 * 1024 * 1024
        ),
    )(x, w1, bias.reshape(chunks, 1, wide), permute, w2)


def place_kernel(
    n, y, out, half, across_sum, from_across, ready, landed, got,
    mate_send, mate_recv, across_send, across_recv, row_send, row_recv, end_send, end_recv,
):
    quarter = y.shape[3] // 4
    row, me = lax.axis_index("dp"), lax.axis_index("tensor")
    core, side = me % 2, me // 2
    mate, across = side * 2 + 1 - core, (1 - side) * 2 + core

    barrier = pltpu.get_barrier_semaphore()
    for k in range(1, 4):
        pl.semaphore_signal(barrier, inc=1, device_id={"tensor": (me + k) % 4}, device_id_type=MESH)
    for k in range(1, n):
        pl.semaphore_signal(barrier, inc=1, device_id={"dp": (row + k) % n}, device_id_type=MESH)
    pl.semaphore_wait(barrier, 3 + n - 1)

    def piece(index):
        return pl.ds(pl.multiple_of(index * quarter, quarter), quarter)

    def to_mate(i, j):
        return pltpu.make_async_remote_copy(
            y.at[i, :, :, piece((side + j) % 2 * 2 + 1 - core)], half.at[i, j], mate_send.at[i, j], mate_recv.at[i, j],
            device_id={"tensor": mate}, device_id_type=MESH)

    def to_across(i):
        return pltpu.make_async_remote_copy(
            across_sum.at[i], from_across.at[i], across_send.at[i], across_recv.at[i],
            device_id={"tensor": across}, device_id_type=MESH)

    def to_row(i, k):
        other = (row + k) % n
        return pltpu.make_async_remote_copy(
            ready.at[i, other], landed.at[row, i], row_send.at[i, k], row_recv.at[i, k],
            device_id={"dp": other}, device_id_type=MESH)

    def to_end(i, k, block):
        return pltpu.make_async_remote_copy(
            landed.at[block, i], got.at[me, i], end_send.at[i, k], end_recv.at[i, me],
            device_id={"tensor": block}, device_id_type=MESH)

    for i in range(n):
        for j in (1, 0):
            to_mate(i, j).start()

    for i in range(n):
        to_mate(i, 1).wait_recv()
        for s in range(n):
            across_sum[i, s] = (
                y[i, s, :, piece((1 - side) * 2 + core)].astype(jnp.float32) + half[i, 1, s].astype(jnp.float32)
            ).astype(jnp.bfloat16)
        to_across(i).start()

    for i in range(n):
        to_mate(i, 0).wait_recv()
        to_across(i).wait_recv()
        for s in range(n):
            ready[i, s] = (
                y[i, s, :, piece(me)].astype(jnp.float32)
                + half[i, 0, s].astype(jnp.float32)
                + from_across[i, s].astype(jnp.float32)
            ).astype(jnp.bfloat16)
        for k in range(1, n):
            to_row(i, k).start()
        landed[row, i] = ready[i, row]

    for i in range(n):
        for k in range(n):
            block = (row + n - k) % n
            if k:
                to_row(i, k).wait_recv()

            @pl.when(block == me)
            def _():
                got[me, i] = landed[block, i]

            @pl.when(block != me)
            def _():
                to_end(i, k, block).start()

    for i in range(n):
        for k in range(1, 4):
            other = (me + k) % 4
            pltpu.make_async_remote_copy(
                landed.at[0, i], got.at[other, i], end_send.at[i, 0], end_recv.at[i, other],
                device_id={"tensor": other}, device_id_type=MESH).wait_recv()
    for t in range(4):
        out[:, :, t * quarter:(t + 1) * quarter] = got[t]

    for i in range(n):
        for j in range(2):
            to_mate(i, j).wait_send()
        to_across(i).wait_send()
        for k in range(1, n):
            to_row(i, k).wait_send()
        for k in range(n):
            block = (row + n - k) % n

            @pl.when(block != me)
            def _():
                to_end(i, k, block).wait_send()


def place(second):
    n, _, capacity, columns = second.shape
    quarter = columns // 4
    vmem = pl.BlockSpec(memory_space=pltpu.VMEM)
    stack = pltpu.VMEM((n, n, capacity, quarter), jnp.bfloat16)
    return pl.pallas_call(
        functools.partial(place_kernel, n),
        out_shape=jax.ShapeDtypeStruct((n, capacity, columns), jnp.bfloat16),
        in_specs=[vmem],
        out_specs=vmem,
        scratch_shapes=[
            pltpu.VMEM((n, 2, n, capacity, quarter), jnp.bfloat16),
            stack,
            stack,
            stack,
            stack,
            stack,
            pltpu.SemaphoreType.DMA((n, 2)),
            pltpu.SemaphoreType.DMA((n, 2)),
            pltpu.SemaphoreType.DMA((n,)),
            pltpu.SemaphoreType.DMA((n,)),
            pltpu.SemaphoreType.DMA((n, n)),
            pltpu.SemaphoreType.DMA((n, n)),
            pltpu.SemaphoreType.DMA((n, n)),
            pltpu.SemaphoreType.DMA((n, n)),
        ],
        compiler_params=pltpu.CompilerParams(
            collective_id=1, has_side_effects=True, vmem_limit_bytes=40 * 1024 * 1024
        ),
    )(second)


def exchange(second, dp_count, tensor_count, capacity):
    if dp_count == tensor_count == 4 and capacity % 16 == 0 and second.shape[1] % 512 == 0:
        return place(second.reshape(dp_count, dp_count, capacity, -1)).reshape(dp_count * capacity, -1)
    second = lax.psum_scatter(second, "tensor", scatter_dimension=1, tiled=True)
    columns = second.shape[1]
    second = second.reshape(dp_count, dp_count, capacity, columns)
    second = lax.all_to_all(second, "dp", split_axis=1, concat_axis=0, tiled=False)
    blocks = dp_count // tensor_count
    second = second.reshape(tensor_count, blocks, dp_count * capacity, columns)
    second = lax.all_to_all(second, "tensor", split_axis=0, concat_axis=0, tiled=True)
    return second.transpose(2, 1, 0, 3).reshape(dp_count * capacity, -1)


def local(
    patches,
    grids,
    dest,
    norm_gain,
    qkv_weight,
    qkv_bias,
    proj_weight,
    proj_bias,
    merge_gain,
    w_first,
    b_first,
    w_second,
    b_second,
    text_embed,
):
    rows_dev, width = patches.shape
    images_dev = grids.shape[0]
    heads_dev = qkv_weight.shape[2] // HEAD_DIM
    dp_count = lax.axis_size("dp")
    tensor_count = lax.axis_size("tensor")
    seq_rows = text_embed.shape[0]
    capacity = images_dev * (MERGED // dp_count)
    live_count = grids[:, 0] * grids[:, 1]
    permute, slot_rows = placement(dest, live_count, dp_count, seq_rows, capacity)
    arrived_rows = lax.all_to_all(
        slot_rows.reshape(dp_count, capacity), "dp", split_axis=0, concat_axis=0, tiled=True
    ).reshape(-1)

    attended = attention(patches, live_count, norm_gain, qkv_weight, qkv_bias, images_dev, heads_dev)
    partial_value = jnp.dot(attended, proj_weight, preferred_element_type=jnp.float32).astype(jnp.bfloat16)
    summed = lax.psum_scatter(partial_value, "tensor", scatter_dimension=0, tiled=True).astype(jnp.float32)
    part = rows_dev // tensor_count
    own = lax.dynamic_slice_in_dim(patches, lax.axis_index("tensor") * part, part, 0)
    resid = own.astype(jnp.float32) + summed + proj_bias
    merged_in = rms_scale(resid, merge_gain).astype(jnp.bfloat16).reshape(part // 4, 4 * width)
    sliced = lax.all_to_all(
        merged_in.reshape(part // 4, dp_count, 4 * width // dp_count), "dp", split_axis=1, concat_axis=0, tiled=False
    )
    received = lax.all_gather(sliced, "tensor", axis=1, tiled=False)
    received = received.reshape(-1, 4 * width // dp_count)
    second = merger(received, w_first, b_first, permute, w_second)
    visual = exchange(second, dp_count, tensor_count, capacity)
    visual = (visual.astype(jnp.float32) + b_second).astype(jnp.bfloat16)
    hit = jnp.arange(seq_rows, dtype=jnp.int32)[:, None] == arrived_rows[None, :]
    placed = jnp.dot(hit.astype(jnp.bfloat16), visual, preferred_element_type=jnp.float32).astype(jnp.bfloat16)
    return jnp.where(jnp.any(hit, axis=1)[:, None], placed, text_embed)


def fused_kernel(
    seq_rows, lags,
    patches_hbm, grids, dest, gain, wqkv_hbm, bqkv, wproj_hbm, bproj, mgain, w1_hbm, bias, w2_hbm, bias2, text_hbm,
    final,
    patches, wqkv, bpad, wproj, target, normed, raws, qs, ks, vs, att_f32, att_out, att_in, slices, rows_tbl, arrived, hit_out, any_out, out, x,
    w1, w2, own, to_r, to_l, from_l, from_r, hidden, keep, give, from_mate, cross, from_across, ready, landed,
    load_sem, head_sem, tbl_send, tbl_recv, pm_send, pm_recv, pa_send, pa_recv, py_send, py_recv, pd_send, pd_recv,
    att_send, att_recv, z_send, fm_send, fa_send, x_recv,
    r_send, r_recv, l_send, l_recv, mate_send, mate_recv, across_send, across_recv,
    row_send, row_recv, end_send, end_recv,
):
    n, _, sides, few, width = x.shape
    nt = 2 * sides
    rows = patches.shape[0]
    block = rows // n
    half = block // sides
    merged = dest.shape[1]
    heads = qs.shape[0]
    lanes = qs.shape[2]
    count, _, wide = own.shape
    steps = count // n
    pieces = steps // sides
    pair = n // sides
    quarter = keep.shape[3]
    piece = ready.shape[4]
    row, me, group = lax.axis_index("dp"), lax.axis_index("tensor"), lax.axis_index("groups")
    core, side = me % 2, me // 2
    mate, across = side * 2 + 1 - core, (1 - side) * 2 + core
    left, right = lax.max(row - 1, 0), lax.min(row + 1, n - 1)
    has_left, has_right = row > 0, row < n - 1
    bf16, f32 = jnp.bfloat16, jnp.float32

    load_x = pltpu.make_async_copy(patches_hbm, patches, load_sem.at[0])
    load_p = pltpu.make_async_copy(wproj_hbm, wproj.at[me], load_sem.at[1])
    load_1 = pltpu.make_async_copy(w1_hbm, w1, load_sem.at[2])
    load_2 = pltpu.make_async_copy(w2_hbm, w2, load_sem.at[3])
    load_t = pltpu.make_async_copy(text_hbm, final, load_sem.at[4])
    load_w = [
        pltpu.make_async_copy(
            wqkv_hbm.at[j, h * HEAD_DIM:(h + 1) * HEAD_DIM], wqkv.at[j, h * lanes:h * lanes + HEAD_DIM],
            head_sem.at[j, h])
        for j in range(3) for h in range(heads)
    ]
    load_p.start()
    load_x.start()
    for load in load_w:
        load.start()

    barrier = pltpu.get_barrier_semaphore()
    for k in range(1, nt):
        pl.semaphore_signal(barrier, inc=1, device_id={"tensor": (me + k) % nt}, device_id_type=MESH)
    for k in range(1, n):
        pl.semaphore_signal(barrier, inc=1, device_id={"dp": (row + k) % n}, device_id_type=MESH)
    pl.semaphore_signal(barrier, inc=1, device_id={"groups": 1 - group}, device_id_type=MESH)

    pl.semaphore_wait(barrier, nt - 1 + n - 1 + 1)

    def remote(source, to, send, recv, device):
        return pltpu.make_async_remote_copy(source, to, send, recv, device_id=device, device_id_type=MESH)

    strips = pa_send.shape[0]
    span = wproj.shape[1] // (2 * strips)

    def strip(g, a):
        return pl.ds(pl.multiple_of((g * strips + a) * span, span), span)

    def same(ref, send, recv, device):
        return remote(ref, ref, send, recv, device)

    proj_mate = same(wproj.at[me], pm_send, pm_recv, {"tensor": mate})
    proj_across = [
        same(wproj.at[me, strip(group, a)], pa_send.at[a], pa_recv.at[a], {"tensor": across}) for a in range(strips)]

    def proj_got(a):
        return same(wproj.at[across, strip(group, a)], pa_send.at[a], pa_recv.at[a], {"tensor": across})

    def proj_peer(a):
        return same(wproj.at[across, strip(group, a)], py_send.at[a], py_recv.at[a], {"groups": 1 - group})

    def proj_peer_got(a):
        return same(wproj.at[across, strip(1 - group, a)], py_send.at[a], py_recv.at[a], {"groups": 1 - group})

    def proj_diag(g, a, at):
        return same(wproj.at[across, strip(g, a)], pd_send.at[at, a], pd_recv.at[at, a], {"tensor": mate})

    def proj_pass(a):
        proj_got(a).wait_recv()
        proj_peer(a).start()
        proj_diag(group, a, 0).start()

    load_p.wait()
    for copy in proj_across:
        copy.start()
    proj_mate.start()

    live = grids[0, 0] * grids[0, 1]
    dest_row = dest[...].astype(f32)

    def shards(value):
        total = jnp.zeros_like(value)
        for s in range(1, n):
            total += jnp.where(value >= float(s * seq_rows), 1.0, 0.0)
        return total

    square = (merged, merged)
    first_at = lax.broadcasted_iota(jnp.int32, square, 0)
    second_at = lax.broadcasted_iota(jnp.int32, square, 1)
    dest_col = jnp.sum(jnp.where(first_at == second_at, dest_row, 0.0), axis=1, keepdims=True)
    shard_row, shard_col = shards(dest_row), shards(dest_col)
    rank_col = jnp.sum(
        jnp.where((shard_row == shard_col) & (second_at < first_at), 1.0, 0.0), axis=1, keepdims=True)
    live_col = lax.broadcasted_iota(jnp.int32, (merged, 1), 0) * 4 < live
    rank_i, shard_i = rank_col.astype(jnp.int32), shard_col.astype(jnp.int32)
    slot_i = rank_i // piece * block + shard_i // 2 * half + shard_i % 2 * piece + rank_i % piece
    base_col = jnp.where(live_col, slot_i, -rows).astype(f32)

    ones_at = lax.broadcasted_iota(jnp.int32, (1, lanes), 1) == HEAD_DIM
    for j in range(3):
        for h in range(heads):
            bpad[j:j + 1, h * lanes:(h + 1) * lanes] = jnp.where(ones_at, 0.0 if j == 1 else 1.0, 0.0)
            bpad[j:j + 1, h * lanes:h * lanes + HEAD_DIM] = bqkv[j:j + 1, h * HEAD_DIM:(h + 1) * HEAD_DIM]
            wqkv[j, h * lanes + HEAD_DIM:(h + 1) * lanes, :] = jnp.zeros((lanes - HEAD_DIM, width), bf16)

    patch_at = lax.broadcasted_iota(jnp.int32, (1, rows), 1)
    row4 = lax.broadcasted_iota(jnp.int32, (merged, 1), 0) * 4
    inside = (patch_at >= row4) & (patch_at < row4 + 4)
    base_row = jnp.sum(jnp.where(inside, base_col, 0.0), axis=0, keepdims=True).astype(jnp.int32)
    target[...] = jnp.broadcast_to(base_row + patch_at % 4 * few, target.shape)

    slots = rows_tbl.shape[2]
    code_col = jnp.where(live_col, shard_col * slots + rank_col + (row * (slots // n)).astype(f32), -1.0)
    lane_at = lax.broadcasted_iota(jnp.int32, (merged, n * slots), 1).astype(f32)
    local_col = dest_col - shard_col * seq_rows
    table = jnp.sum(jnp.where(lane_at == code_col, local_col + 1.0, 0.0), axis=0, keepdims=True) - 1.0
    for s in range(n):
        rows_tbl[s] = jnp.broadcast_to(table[:, s * slots:(s + 1) * slots], (8, slots)).astype(jnp.int32)
    arrived[row] = rows_tbl[row]

    def send_table(k):
        to = (row + k) % n
        return remote(rows_tbl.at[to], arrived.at[row], tbl_send.at[k], tbl_recv.at[row], {"dp": to})

    for k in range(1, n):
        send_table(k).start()

    load_x.wait()
    for load in load_w:
        load.wait()
    load_1.start()
    load_2.start()
    load_t.start()

    mask_at = lax.broadcasted_iota(jnp.int32, (block, lanes), 1) == HEAD_DIM

    def project(b, carry):
        proj_pass(b)
        at = pl.ds(pl.multiple_of(b * block, block), block)
        hit = jnp.where(
            target[0:1, :] == lax.broadcasted_iota(jnp.int32, (block, rows), 0) + b * block, 1.0, 0.0)
        valid = jnp.sum(hit, axis=1, keepdims=True)
        raw = jnp.dot(hit.astype(bf16), patches[...], preferred_element_type=f32)
        for s in range(sides):
            raws[b, s] = raw[s * half:(s + 1) * half, :].astype(bf16)
        normed[...] = rms_scale(raw, gain[...].reshape(1, width)).astype(bf16)
        for j, store in enumerate((qs, ks, vs)):
            acc = lax.dot_general(
                normed[...], wqkv[j], (((1,), (1,)), ((), ())), preferred_element_type=f32) + bpad[j:j + 1, :]
            for h in range(heads):
                value = acc[:, h * lanes:(h + 1) * lanes]
                if j == 1:
                    value = jnp.where(mask_at, jnp.where(valid > 0.5, 0.0, -1e30), value)
                store[h, at, :] = value.astype(bf16)
        return carry

    lax.fori_loop(0, n, project, 0)

    for a in range(n, strips):
        proj_pass(a)

    scale = math.log2(math.e) / math.sqrt(HEAD_DIM)

    def att_to(b, s):
        return remote(
            att_out.at[b, s], att_in.at[b // 2, me], att_send.at[b, s], att_recv.at[b // 2, me],
            {"tensor": s * 2 + b % 2})

    def att_got(b, source):
        return remote(
            att_out.at[b, 0], att_in.at[b // 2, source], att_send.at[b, 0], att_recv.at[b // 2, source],
            {"tensor": mate})

    def z_to(b, k):
        to = (row + k) % n
        return remote(
            slices.at[b // 2, to], x.at[b, row, side], z_send.at[b // 2, k], x_recv.at[b, row, side], {"dp": to})

    def to_mate_x(b, s, i):
        return same(x.at[b, i, s], fm_send.at[b // 2, i, s], x_recv.at[b, i, s], {"tensor": mate})

    def to_across_x(b, i):
        return same(x.at[b, i, side], fa_send.at[b // 2, i], x_recv.at[b, i, side], {"tensor": across})

    def x_got(b, s, i):
        return same(x.at[b, i, s], fm_send.at[b // 2, i, s], x_recv.at[b, i, s], {"tensor": mate})

    def forward(b):
        for k in range(1, n):
            source = (row + n - k) % n
            x_got(b, side, source).wait_recv()
            to_across_x(b, source).start()
            to_mate_x(b, side, source).start()

    def attend(it, carry):
        @pl.when(it < n)
        def _():
            b = lax.min(it, n - 1)
            at = pl.ds(pl.multiple_of(b * block, block), block)
            for h in range(heads):
                scores = lax.dot_general(
                    qs[h, at, :], ks[h], (((1,), (1,)), ((), ())), preferred_element_type=f32)
                peak = jnp.max(scores, axis=1, keepdims=True)
                weights = jnp.exp2((scores - peak) * scale).astype(bf16)
                mixed = jnp.dot(weights, vs[h], preferred_element_type=f32)
                mixed = mixed * (1.0 / mixed[:, HEAD_DIM:HEAD_DIM + 1])
                att_f32[:, h * HEAD_DIM:(h + 1) * HEAD_DIM] = mixed[:, 0:HEAD_DIM]
            for s in range(sides):
                att_out[b, s] = att_f32[s * half:(s + 1) * half, :].astype(bf16)
                owner = s * 2 + b % 2

                @pl.when(owner != me)
                def _():
                    att_to(b, s).start()

                @pl.when(owner == me)
                def _():
                    att_in[b // 2, me] = att_out[b, s]

        @pl.when(it == 0)
        def _():
            for a in range(strips):
                proj_peer_got(a).wait_recv()
                proj_diag(1 - group, a, 1).start()

        @pl.when(it == 1)
        def _():
            proj_mate.wait_recv()
            for a in range(strips):
                proj_diag(group, a, 0).wait_recv()
                proj_diag(1 - group, a, 1).wait_recv()

        @pl.when((it == n - 1) & (core == 0))
        def _():
            forward(0)

        last = lax.max(it, 1) - 1

        @pl.when((it >= 1) & (last % 2 == core))
        def _():
            for k in range(1, nt):
                att_got(last, (me + k) % nt).wait_recv()
            total = raws[last, side].astype(f32) + bproj[...].reshape(1, width)
            for t in range(nt):
                total += jnp.dot(att_in[last // 2, t], wproj[t], preferred_element_type=f32)
            done = rms_scale(total, mgain[...].reshape(1, width)).astype(bf16)
            for k in range(n):
                slices[last // 2, k] = done[k * few:(k + 1) * few, :]
            for k in range(n - 1, 0, -1):
                z_to(last, k).start()
            x[last, row, side] = slices[last // 2, row]
            to_across_x(last, row).start()
            to_mate_x(last, side, row).start()

        return carry

    lax.fori_loop(0, n + 1, attend, 0)

    def forward_across(b):
        for k in range(n):
            source = (row + n - k) % n
            x_got(b, 1 - side, source).wait_recv()
            to_mate_x(b, 1 - side, source).start()

    def await_x(b):
        @pl.when(b % 2 != core)
        def _():
            for s in range(sides):
                for i in range(n):
                    x_got(b, s, i).wait_recv()

    def go_right(c):
        return remote(to_r.at[c], from_l.at[c], r_send.at[c], r_recv.at[c], {"dp": right})

    def go_left(c):
        return remote(to_l.at[c], from_r.at[c], l_send.at[c], l_recv.at[c], {"dp": left})

    def first(b, j):
        columns = pl.ds(pl.multiple_of(j * wide, wide), wide)
        partial = jnp.dot(x[b].reshape(block, width), w1[:, columns], preferred_element_type=f32)
        for h in range(sides):
            own[b * steps + h * pieces + j] = partial[h * half:(h + 1) * half, :]

    def begin(c):
        @pl.when(row == 0)
        def _():
            to_r[c] = own[c].astype(bf16)
            go_right(c).start()

        @pl.when(row == n - 1)
        def _():
            to_l[c] = own[c].astype(bf16)
            go_left(c).start()

    def relay(stage, c):
        @pl.when(row == stage)
        def _():
            go_right(c).wait_recv()
            to_r[c] = (own[c] + from_l[c].astype(f32)).astype(bf16)
            go_right(c).start()

        @pl.when(row == n - 1 - stage)
        def _():
            go_left(c).wait_recv()
            to_l[c] = (own[c] + from_r[c].astype(f32)).astype(bf16)
            go_left(c).start()

    def activate(c):
        columns = pl.ds(pl.multiple_of(c % pieces * wide, wide), wide)

        @pl.when(row == n - 1)
        def _():
            go_right(c).wait_recv()

        @pl.when(row == 0)
        def _():
            go_left(c).wait_recv()

        @pl.when(has_left)
        def _():
            own[c] += from_l[c].astype(f32)

        @pl.when(has_right)
        def _():
            own[c] += from_r[c].astype(f32)

        value = own[c] + bias[columns].reshape(1, wide)
        hidden[c // pieces % 2, :, columns] = (0.5 * value * (1.0 + lax.erf(value * math.sqrt(0.5)))).astype(bf16)

    def columns_of(s, c):
        return pl.ds(pl.multiple_of((s * 2 + c) * quarter, quarter), quarter)

    def to_mate(b, s):
        return remote(give.at[b, s], from_mate.at[b, s], mate_send.at[b, s], mate_recv.at[b, s], {"tensor": mate})

    def to_across(g, p):
        return remote(
            cross.at[g, p], from_across.at[g, p], across_send.at[g, p], across_recv.at[g, p], {"tensor": across})

    def to_row(g, p, k):
        to = (row + k) % n
        return remote(
            ready.at[g, p, to], landed.at[g, p, row], row_send.at[g, p, k], row_recv.at[g, p, row], {"dp": to})

    def quarter_of(t):
        return pl.ds(pl.multiple_of(t * quarter, quarter), quarter)

    thin = cross.shape[3]

    def columns_in(t, p):
        return pl.ds(pl.multiple_of(t * quarter + p * thin, thin), thin)

    def to_end(g, p, d):
        at = pl.ds(g % sides * pair, pair)
        return remote(
            landed.at[g, p, d], out.at[at, g // sides, :, columns_in(me, p)], end_send.at[g, p, d],
            end_recv.at[g, p, me], {"tensor": d})

    def product(g, s, c):
        return jnp.dot(hidden[g % 2], w2[:, columns_of(s, c)], preferred_element_type=f32)

    def second(g):
        give[g, 1 - side] = product(g, 1 - side, 1 - core).astype(bf16)
        to_mate(g, 1 - side).start()
        keep[g % 2, 1 - side] = product(g, 1 - side, core)

    def chip_sum(g):
        to_mate(g, 1 - side).wait_recv()
        for p in range(2):
            at = slice(p * thin, (p + 1) * thin)
            cross[g, p] = (
                keep[g % 2, 1 - side, :, at] + from_mate[g, 1 - side, :, at].astype(f32)).astype(bf16)
            to_across(g, p).start()
        give[g, side] = product(g, side, 1 - core).astype(bf16)
        to_mate(g, side).start()
        keep[g % 2, side] = product(g, side, core)

    def spread(g):
        to_mate(g, side).wait_recv()
        for p in range(2):
            at = slice(p * thin, (p + 1) * thin)
            value = keep[g % 2, side, :, at] + from_mate[g, side, :, at].astype(f32)
            to_across(g, p).wait_recv()
            value = (value + from_across[g, p].astype(f32)).astype(bf16)
            for s in range(n):
                for i in range(pair):
                    begin_at = (i * n + s) * piece
                    ready[g, p, s, i] = value[begin_at:begin_at + piece, :]
            for k in range(n - 1, 0, -1):
                to_row(g, p, k).start()
            landed[g, p, row] = ready[g, p, row]

    def deliver(g):
        for p in range(2):
            for k in range(n):
                source = (row + n - k) % n
                if k:
                    remote(
                        ready.at[g, p, 0], landed.at[g, p, source], row_send.at[g, p, 0],
                        row_recv.at[g, p, source], {"dp": left},
                    ).wait_recv()

                @pl.when(source == me)
                def _():
                    out[pl.ds(g % sides * pair, pair), g // sides, :, columns_in(me, p)] = landed[g, p, source]

                @pl.when(source != me)
                def _():
                    to_end(g, p, source).start()

    lead, hop, fill, offsets = lags

    @pl.when(core == 0)
    def _():
        forward_across(0)

    @pl.when(core == 1)
    def _():
        forward(1)

    for k in range(1, n):
        source = (row + n - k) % n
        remote(rows_tbl.at[0], arrived.at[source], tbl_send.at[0], tbl_recv.at[source], {"dp": source}).wait_recv()

    at_slot = arrived[0, 0:1, :]
    for i in range(1, n):
        at_slot = jnp.maximum(at_slot, arrived[i, 0:1, :])
    match = jnp.where(
        lax.broadcasted_iota(jnp.int32, hit_out.shape, 0) == at_slot, 1.0, 0.0)
    hit_out[...] = match.astype(bf16)
    any_out[...] = jnp.broadcast_to(jnp.max(match, axis=1, keepdims=True), any_out.shape)

    load_1.wait()
    load_2.wait()
    load_t.wait()
    after = tuple(zip(offsets, (second, chip_sum, spread, deliver)))

    def step(u, carry):
        @pl.when((u < count) & (u % steps < pieces))
        def _():
            @pl.when(u % steps == 0)
            def _():
                await_x(u // steps)

            first(u // steps, u % steps)

        @pl.when(u < count)
        def _():
            begin(u)

        @pl.when((u == 1) & (core == 1))
        def _():
            forward_across(1)

        @pl.when(u == 8)
        def _():
            forward(2 + core)

        @pl.when(u == 12)
        def _():
            forward_across(2 + core)

        for stage in range(1, n - 1):
            late = lead + (stage - 1) * hop

            @pl.when((u >= late) & (u < count + late))
            def _():
                relay(stage, u - late)

        @pl.when((u >= lead + fill) & (u < count + lead + fill))
        def _():
            activate(u - lead - fill)

        for offset, work in after:
            late = lead + fill + offset + pieces - 1

            @pl.when((u >= late) & (u < count + late) & (lax.max(u - late, 0) % pieces == 0))
            def _():
                work((u - late) // pieces)

        return carry

    lax.fori_loop(0, count + lead + fill + offsets[-1], step, 0)

    for k in range(nt):
        source = (me + k) % nt

        if k:
            def gather(g, carry):
                for p in range(2):
                    remote(
                        landed.at[g, p, 0],
                        out.at[pl.ds(g % sides * pair, pair), g // sides, :, columns_in(source, p)],
                        end_send.at[g, p, 0], end_recv.at[g, p, source], {"tensor": mate},
                    ).wait_recv()
                return carry

            lax.fori_loop(0, n * sides, gather, 0)
        columns = pl.ds(pl.multiple_of(source * quarter, quarter), quarter)
        rows_in = out[:, :, :, columns].reshape(hit_out.shape[1], quarter)
        placed = jnp.dot(hit_out[...], rows_in, preferred_element_type=f32) + bias2[columns].reshape(1, quarter)
        final[:, columns] = jnp.where(any_out[:, 0:1] > 0.5, placed.astype(bf16), final[:, columns])

    def drain(c, carry):
        @pl.when(has_right)
        def _():
            go_right(c).wait_send()

        @pl.when(has_left)
        def _():
            go_left(c).wait_send()

        return carry

    lax.fori_loop(0, count, drain, 0)
    proj_mate.wait_send()
    for a in range(strips):
        proj_across[a].wait_send()
        proj_peer(a).wait_send()
        proj_diag(group, a, 0).wait_send()
        proj_diag(1 - group, a, 1).wait_send()
    for k in range(1, n):
        send_table(k).wait_send()
    for b in range(n):
        for s in range(sides):
            @pl.when(s * 2 + b % 2 != me)
            def _():
                att_to(b, s).wait_send()


    def drain_place(g, carry):
        for p in range(2):
            to_mate(g, p).wait_send()
            to_across(g, p).wait_send()
            for k in range(1, n):
                to_row(g, p, k).wait_send()
                to_end(g, p, (me + k) % nt).wait_send()
        return carry

    lax.fori_loop(0, n * sides, drain_place, 0)
    for q in range(2):
        b = 2 * q + core
        for k in range(1, n):
            z_to(b, k).wait_send()
        for i in range(n):
            to_across_x(b, i).wait_send()
            for s in range(sides):
                to_mate_x(b, s, i).wait_send()


def fused(
    patches, grids, dest, norm_gain, qkv_weight, qkv_bias, proj_weight, proj_bias, merge_gain,
    w_first, b_first, w_second, b_second, text_embed,
):
    n, nt = lax.axis_size("dp"), lax.axis_size("tensor")
    seq_rows = text_embed.shape[0]
    sides = nt // 2
    rows, width = patches.shape
    span = qkv_weight.shape[2]
    heads = span // HEAD_DIM
    block = rows // n
    half = block // sides
    few = half // 4
    hidden, columns = w_second.shape
    wide, lanes = 256, 128
    pieces = hidden // wide
    steps = pieces * sides
    count = n * steps
    quarter = columns // nt
    piece = few // 2
    any_space = pl.BlockSpec(memory_space=pl.ANY)
    vmem = pl.BlockSpec(memory_space=pltpu.VMEM)
    smem = pl.BlockSpec(memory_space=pltpu.SMEM)
    dma = pltpu.SemaphoreType.DMA
    bf16, f32 = jnp.bfloat16, jnp.float32
    heads_shape = pltpu.VMEM((heads, rows, lanes), bf16)
    stack = pltpu.VMEM((count, half, wide), bf16)
    units = n * sides
    strips = span // 64
    slots = n * n * piece
    tiles = pltpu.VMEM((units, 2, half, quarter), bf16)
    one = pltpu.VMEM((units, 2, half, quarter // 2), bf16)
    moved = pltpu.VMEM((units, 2, n, n // sides, piece, quarter // 2), bf16)
    lags = (4, 3, 6, (0, 1, 6, 12))
    return pl.pallas_call(
        functools.partial(fused_kernel, seq_rows, lags),
        out_shape=jax.ShapeDtypeStruct(text_embed.shape, bf16),
        in_specs=[
            any_space, smem, vmem, vmem, any_space, vmem, any_space, vmem, vmem, any_space, vmem, any_space, vmem,
            any_space],
        out_specs=vmem,
        scratch_shapes=[
            pltpu.VMEM((rows, width), bf16),
            pltpu.VMEM((3, heads * lanes, width), bf16),
            pltpu.VMEM((3, heads * lanes), f32),
            pltpu.VMEM((nt, span, width), bf16),
            pltpu.VMEM((8, rows), jnp.int32),
            pltpu.VMEM((block, width), bf16),
            pltpu.VMEM((n, sides, half, width), bf16),
            heads_shape, heads_shape, heads_shape,
            pltpu.VMEM((block, span), f32),
            pltpu.VMEM((n, sides, half, span), bf16),
            pltpu.VMEM((n // 2, nt, half, span), bf16),
            pltpu.VMEM((n // 2, n, few, width), bf16),
            pltpu.VMEM((n, 8, slots), jnp.int32),
            pltpu.VMEM((n, 8, slots), jnp.int32),
            pltpu.VMEM((seq_rows, slots), bf16),
            pltpu.VMEM((seq_rows, lanes), f32),
            pltpu.VMEM((n, n, piece, columns), bf16),
            pltpu.VMEM((n, n, sides, few, width), bf16),
            pltpu.VMEM(w_first.shape, bf16),
            pltpu.VMEM(w_second.shape, bf16),
            pltpu.VMEM((count, half, wide), f32),
            stack, stack, stack, stack,
            pltpu.VMEM((2, half, hidden), bf16),
            pltpu.VMEM((2, 2, half, quarter), f32),
            tiles, tiles, one, one, moved, moved,
            dma((5,)), dma((3, heads)), dma((n,)), dma((n,)), dma, dma, dma((strips,)), dma((strips,)), dma((strips,)),
            dma((strips,)), dma((2, strips)), dma((2, strips)),
            dma((n, sides)), dma((n // 2, nt)), dma((n // 2, n)), dma((n // 2, n, sides)), dma((n // 2, n)),
            dma((n, n, sides)),
            dma((count,)), dma((count,)), dma((count,)), dma((count,)),
            dma((units, 2)), dma((units, 2)), dma((units, 2)), dma((units, 2)), dma((units, 2, n)), dma((units, 2, n)),
            dma((units, 2, nt)), dma((units, 2, nt)),
        ],
        compiler_params=pltpu.CompilerParams(
            collective_id=2, has_side_effects=True, vmem_limit_bytes=63 * 1024 * 1024
        ),
    )(
        patches, grids, dest, norm_gain, qkv_weight.swapaxes(1, 2), qkv_bias, proj_weight, proj_bias, merge_gain,
        w_first, b_first, w_second, b_second, text_embed,
    )


def local_fast(
    patches,
    grids,
    dest,
    norm_gain,
    qkv_weight,
    qkv_bias,
    proj_weight,
    proj_bias,
    merge_gain,
    w_first,
    b_first,
    w_second,
    b_second,
    text_embed,
):
    return fused(
        patches, grids, dest, norm_gain, qkv_weight, qkv_bias, proj_weight, proj_bias, merge_gain,
        w_first, b_first, w_second, b_second, text_embed)


def fits(patches, grids, dest, qkv_weight, w_first, w_second):
    n, nt = lax.axis_size("dp"), lax.axis_size("tensor")
    rows, width = patches.shape
    return (
        n == nt == 4
        and lax.axis_size("groups") == 2
        and grids.shape[0] == 1
        and rows == PATCHES
        and dest.shape[1] == MERGED
        and w_first.shape[0] == width
        and w_second.shape[0] % 256 == 0
        and w_second.shape[1] % 512 == 0
        and qkv_weight.shape[2] % 64 == 0
        and qkv_weight.shape[2] // 64 > n
    )


def chosen(*args):
    run = local_fast if fits(args[0], args[1], args[2], args[4], args[9], args[11]) else local
    return run(*args)


def solution(mesh):
    in_specs = (
        P(("groups", "dp"), None),
        P(("groups", "dp"), None),
        P(("groups", "dp"), None),
        P(),
        P(None, None, "tensor"),
        P(None, "tensor"),
        P("tensor", None),
        P(),
        P(),
        P("dp", "tensor"),
        P("tensor"),
        P("tensor", "dp"),
        P("tensor"),
        P(("groups", "dp"), "tensor"),
    )
    out_specs = P(("groups", "dp"), "tensor")
    return jax.shard_map(chosen, mesh=mesh, in_specs=in_specs, out_specs=out_specs, check_vma=False)
```

```python
import functools
import math

import jax
import jax.numpy as jnp
from jax import lax
from jax.experimental import pallas as pl
from jax.experimental.pallas import tpu as pltpu
from jax.sharding import PartitionSpec as P

MESH = pl.DeviceIdType.MESH

HEAD_DIM = 80
PATCHES = 1024
MERGED = 256


def rms_scale(values, gain):
    return values * lax.rsqrt(jnp.mean(values * values, axis=-1, keepdims=True) + 1e-06) * gain


def placement(dest, live_count, dp_count, seq_rows, capacity):
    merged_dev = dest.size
    live_rows = (jnp.arange(MERGED, dtype=jnp.int32)[None, :] < (live_count // 4)[:, None]).reshape(merged_dev)
    dest_flat = dest.reshape(merged_dev)
    shard_id = jnp.where(live_rows, dest_flat // seq_rows, dp_count)
    local_row = dest_flat % seq_rows
    index = jnp.arange(merged_dev, dtype=jnp.int32)
    earlier = (shard_id[:, None] == shard_id[None, :]) & (index[None, :] < index[:, None])
    rank = jnp.sum(earlier.astype(jnp.int32), axis=1)
    slot = jnp.where(live_rows & (rank < capacity), shard_id * capacity + rank, -1)
    hit = jnp.arange(dp_count * capacity, dtype=jnp.int32)[:, None] == slot[None, :]
    rows = jnp.max(jnp.where(hit, local_row[None, :], -1), axis=1)
    return hit.astype(jnp.bfloat16), rows


def attention(patches, live_count, norm_gain, qkv_weight, qkv_bias, images_dev, heads_dev):
    normed = rms_scale(patches.astype(jnp.float32), norm_gain).astype(jnp.bfloat16)
    projected = (
        jnp.einsum("rv,jvc->jrc", normed, qkv_weight, preferred_element_type=jnp.float32)
        + qkv_bias[:, None, :]
    )
    projected = projected.astype(jnp.bfloat16).reshape(3, images_dev, PATCHES, heads_dev, HEAD_DIM)
    scores = jnp.einsum(
        "iqhd,ikhd->ihqk", projected[0], projected[1], preferred_element_type=jnp.float32
    ) / math.sqrt(HEAD_DIM)
    live_keys = jnp.arange(PATCHES, dtype=jnp.int32)[None, :] < live_count[:, None]
    scores = jnp.where(live_keys[:, None, None, :], scores, jnp.float32(-1e30))
    peak_score = jnp.max(scores, axis=-1, keepdims=True)
    exponent = jnp.exp(scores - peak_score)
    weights = (exponent / jnp.sum(exponent, axis=-1, keepdims=True)).astype(jnp.bfloat16)
    attended = jnp.einsum(
        "ihqk,ikhd->iqhd", weights, projected[2], preferred_element_type=jnp.float32
    )
    return attended.astype(jnp.bfloat16).reshape(patches.shape[0], heads_dev * HEAD_DIM)


def merger_kernel(
    n, x_hbm, w1_hbm, bias, permute, w2_hbm, out_hbm,
    x, w1, w2, part, from_left, from_right, total, slots, acc, out,
    load_sem, sum_send, sum_recv, hid_send, hid_recv,
):
    chunks, _, block, wide = part.shape
    me = lax.axis_index("dp")
    left, right = lax.max(me - 1, 0), lax.min(me + 1, n - 1)
    has_left, has_right = me > 0, me < n - 1
    inner = has_left & has_right

    loads = [
        pltpu.make_async_copy(a, b, load_sem.at[i])
        for i, (a, b) in enumerate(((x_hbm, x), (w1_hbm, w1), (w2_hbm, w2)))
    ]
    for load in loads:
        load.start()

    barrier = pltpu.get_barrier_semaphore()

    @pl.when(has_left)
    def _():
        pl.semaphore_signal(barrier, inc=1, device_id={"dp": left}, device_id_type=MESH)

    @pl.when(has_right)
    def _():
        pl.semaphore_signal(barrier, inc=1, device_id={"dp": right}, device_id_type=MESH)

    pl.semaphore_wait(barrier, has_left.astype(jnp.int32) + has_right.astype(jnp.int32))

    def sum_right(c, b):
        return pltpu.make_async_remote_copy(
            part.at[c, b], from_left.at[c, b], sum_send.at[0, c, b], sum_recv.at[0, c, b],
            device_id={"dp": right}, device_id_type=MESH)

    def sum_left(c, b):
        return pltpu.make_async_remote_copy(
            part.at[c, b], from_right.at[c, b], sum_send.at[1, c, b], sum_recv.at[1, c, b],
            device_id={"dp": left}, device_id_type=MESH)

    def hid_right(c, b):
        return pltpu.make_async_remote_copy(
            slots.at[c, b], slots.at[c, b], hid_send.at[0, c, b], hid_recv.at[0, c, b],
            device_id={"dp": right}, device_id_type=MESH)

    def hid_left(c, b):
        return pltpu.make_async_remote_copy(
            slots.at[c, b], slots.at[c, b], hid_send.at[1, c, b], hid_recv.at[1, c, b],
            device_id={"dp": left}, device_id_type=MESH)

    def first(c):
        columns = pl.ds(pl.multiple_of(c * wide, wide), wide)

        def tile(b):
            part[c, b] = jnp.dot(
                x[pl.ds(pl.multiple_of(b * block, block), block), :], w1[:, columns],
                preferred_element_type=jnp.float32,
            ).astype(jnp.bfloat16)

        def up(i, carry):
            b = n - 1 - i
            tile(b)

            @pl.when((me == 0) & (b > 0))
            def _():
                sum_right(c, b).start()

            return carry

        def down(b, carry):
            tile(b)

            @pl.when((me == n - 1) & (b < n - 1))
            def _():
                sum_left(c, b).start()

            return carry

        @pl.when(me == 0)
        def _():
            lax.fori_loop(0, n, up, 0)

        @pl.when(me > 0)
        def _():
            lax.fori_loop(0, n, down, 0)

    def relay(c):
        def one(i, carry):
            b = n - 1 - i

            @pl.when(inner & (b > me))
            def _():
                sum_right(c, b).wait_recv()
                part[c, b] = (part[c, b].astype(jnp.float32) + from_left[c, b].astype(jnp.float32)).astype(jnp.bfloat16)
                sum_right(c, b).start()

            @pl.when(inner & (i < me))
            def _():
                sum_left(c, i).wait_recv()
                part[c, i] = (part[c, i].astype(jnp.float32) + from_right[c, i].astype(jnp.float32)).astype(jnp.bfloat16)
                sum_left(c, i).start()

            return carry

        lax.fori_loop(0, n, one, 0)

    def activate(c):
        total[...] = part[c, me].astype(jnp.float32) + bias[c]

        @pl.when(has_left)
        def _():
            sum_right(c, me).wait_recv()
            total[...] += from_left[c, me].astype(jnp.float32)

        @pl.when(has_right)
        def _():
            sum_left(c, me).wait_recv()
            total[...] += from_right[c, me].astype(jnp.float32)

        value = total[...]
        hidden = (0.5 * value * (1.0 + lax.erf(value * math.sqrt(0.5)))).astype(jnp.bfloat16)
        slots[c, me] = jnp.dot(permute[...], hidden, preferred_element_type=jnp.float32).astype(jnp.bfloat16)

        @pl.when(has_right)
        def _():
            hid_right(c, me).start()

        @pl.when(has_left)
        def _():
            hid_left(c, me).start()

    def spread(c):
        def one(k, carry):
            before, after = me - k, me + k

            @pl.when(before >= 0)
            def _():
                hid_right(c, before).wait_recv()

                @pl.when(has_right)
                def _():
                    hid_right(c, before).start()

            @pl.when(after < n)
            def _():
                hid_left(c, after).wait_recv()

                @pl.when(has_left)
                def _():
                    hid_left(c, after).start()

            return carry

        lax.fori_loop(1, n, one, 0)

    def second(c):
        depth = pl.ds(pl.multiple_of(c * wide, wide), wide)

        def one(b, carry):
            rows = pl.ds(pl.multiple_of(b * block, block), block)
            more = jnp.dot(slots[c, b], w2[depth, :], preferred_element_type=jnp.float32)

            @pl.when(c == 0)
            def _():
                acc[rows, :] = more

            @pl.when(c > 0)
            def _():
                acc[rows, :] += more

            return carry

        lax.fori_loop(0, n, one, 0)

    loads[0].wait()
    loads[1].wait()
    first(0)
    loads[2].wait()

    def step(s, carry):
        @pl.when(s + 1 < chunks)
        def _():
            first(s + 1)

        @pl.when(s < chunks)
        def _():
            relay(s)

        @pl.when((s >= 1) & (s <= chunks))
        def _():
            activate(s - 1)

        @pl.when(s >= 2)
        def _():
            spread(s - 2)
            second(s - 2)

        return carry

    lax.fori_loop(0, chunks + 2, step, 0)

    def finish(b, carry):
        rows = pl.ds(pl.multiple_of(b * block, block), block)
        out[rows, :] = acc[rows, :].astype(jnp.bfloat16)
        return carry

    lax.fori_loop(0, n, finish, 0)
    store = pltpu.make_async_copy(out, out_hbm, load_sem.at[0])
    store.start()

    def drain(c, carry):
        def one(b, inside):
            @pl.when(has_right & (b > me))
            def _():
                sum_right(c, b).wait_send()

            @pl.when(has_left & (b < me))
            def _():
                sum_left(c, b).wait_send()

            @pl.when(has_right & (b <= me))
            def _():
                hid_right(c, b).wait_send()

            @pl.when(has_left & (b >= me))
            def _():
                hid_left(c, b).wait_send()

            return inside

        return lax.fori_loop(0, n, one, carry)

    lax.fori_loop(0, chunks, drain, 0)
    store.wait()


def merger(x, w1, bias, permute, w2):
    n = lax.axis_size("dp")
    rows, depth = x.shape
    hidden, columns = w2.shape
    block = rows // n
    wide = 256 if hidden % 256 == 0 else 128
    chunks = hidden // wide
    any_space = pl.BlockSpec(memory_space=pl.ANY)
    vmem = pl.BlockSpec(memory_space=pltpu.VMEM)
    stack = pltpu.VMEM((chunks, n, block, wide), jnp.bfloat16)
    return pl.pallas_call(
        functools.partial(merger_kernel, n),
        out_shape=jax.ShapeDtypeStruct((rows, columns), jnp.bfloat16),
        in_specs=[any_space, any_space, vmem, vmem, any_space],
        out_specs=any_space,
        scratch_shapes=[
            pltpu.VMEM((rows, depth), jnp.bfloat16),
            pltpu.VMEM((depth, hidden), jnp.bfloat16),
            pltpu.VMEM((hidden, columns), jnp.bfloat16),
            stack,
            stack,
            stack,
            pltpu.VMEM((block, wide), jnp.float32),
            stack,
            pltpu.VMEM((rows, columns), jnp.float32),
            pltpu.VMEM((rows, columns), jnp.bfloat16),
            pltpu.SemaphoreType.DMA((3,)),
            pltpu.SemaphoreType.DMA((2, chunks, n)),
            pltpu.SemaphoreType.DMA((2, chunks, n)),
            pltpu.SemaphoreType.DMA((2, chunks, n)),
            pltpu.SemaphoreType.DMA((2, chunks, n)),
        ],
        compiler_params=pltpu.CompilerParams(
            collective_id=0, has_side_effects=True, vmem_limit_bytes=60 * 1024 * 1024
        ),
    )(x, w1, bias.reshape(chunks, 1, wide), permute, w2)


def place_kernel(
    n, y, out, half, across_sum, from_across, ready, landed, got,
    mate_send, mate_recv, across_send, across_recv, row_send, row_recv, end_send, end_recv,
):
    quarter = y.shape[3] // 4
    row, me = lax.axis_index("dp"), lax.axis_index("tensor")
    core, side = me % 2, me // 2
    mate, across = side * 2 + 1 - core, (1 - side) * 2 + core

    barrier = pltpu.get_barrier_semaphore()
    for k in range(1, 4):
        pl.semaphore_signal(barrier, inc=1, device_id={"tensor": (me + k) % 4}, device_id_type=MESH)
    for k in range(1, n):
        pl.semaphore_signal(barrier, inc=1, device_id={"dp": (row + k) % n}, device_id_type=MESH)
    pl.semaphore_wait(barrier, 3 + n - 1)

    def piece(index):
        return pl.ds(pl.multiple_of(index * quarter, quarter), quarter)

    def to_mate(i, j):
        return pltpu.make_async_remote_copy(
            y.at[i, :, :, piece((side + j) % 2 * 2 + 1 - core)], half.at[i, j], mate_send.at[i, j], mate_recv.at[i, j],
            device_id={"tensor": mate}, device_id_type=MESH)

    def to_across(i):
        return pltpu.make_async_remote_copy(
            across_sum.at[i], from_across.at[i], across_send.at[i], across_recv.at[i],
            device_id={"tensor": across}, device_id_type=MESH)

    def to_row(i, k):
        other = (row + k) % n
        return pltpu.make_async_remote_copy(
            ready.at[i, other], landed.at[row, i], row_send.at[i, k], row_recv.at[i, k],
            device_id={"dp": other}, device_id_type=MESH)

    def to_end(i, k, block):
        return pltpu.make_async_remote_copy(
            landed.at[block, i], got.at[me, i], end_send.at[i, k], end_recv.at[i, me],
            device_id={"tensor": block}, device_id_type=MESH)

    for i in range(n):
        for j in (1, 0):
            to_mate(i, j).start()

    for i in range(n):
        to_mate(i, 1).wait_recv()
        for s in range(n):
            across_sum[i, s] = (
                y[i, s, :, piece((1 - side) * 2 + core)].astype(jnp.float32) + half[i, 1, s].astype(jnp.float32)
            ).astype(jnp.bfloat16)
        to_across(i).start()

    for i in range(n):
        to_mate(i, 0).wait_recv()
        to_across(i).wait_recv()
        for s in range(n):
            ready[i, s] = (
                y[i, s, :, piece(me)].astype(jnp.float32)
                + half[i, 0, s].astype(jnp.float32)
                + from_across[i, s].astype(jnp.float32)
            ).astype(jnp.bfloat16)
        for k in range(1, n):
            to_row(i, k).start()
        landed[row, i] = ready[i, row]

    for i in range(n):
        for k in range(n):
            block = (row + n - k) % n
            if k:
                to_row(i, k).wait_recv()

            @pl.when(block == me)
            def _():
                got[me, i] = landed[block, i]

            @pl.when(block != me)
            def _():
                to_end(i, k, block).start()

    for i in range(n):
        for k in range(1, 4):
            other = (me + k) % 4
            pltpu.make_async_remote_copy(
                landed.at[0, i], got.at[other, i], end_send.at[i, 0], end_recv.at[i, other],
                device_id={"tensor": other}, device_id_type=MESH).wait_recv()
    for t in range(4):
        out[:, :, t * quarter:(t + 1) * quarter] = got[t]

    for i in range(n):
        for j in range(2):
            to_mate(i, j).wait_send()
        to_across(i).wait_send()
        for k in range(1, n):
            to_row(i, k).wait_send()
        for k in range(n):
            block = (row + n - k) % n

            @pl.when(block != me)
            def _():
                to_end(i, k, block).wait_send()


def place(second):
    n, _, capacity, columns = second.shape
    quarter = columns // 4
    vmem = pl.BlockSpec(memory_space=pltpu.VMEM)
    stack = pltpu.VMEM((n, n, capacity, quarter), jnp.bfloat16)
    return pl.pallas_call(
        functools.partial(place_kernel, n),
        out_shape=jax.ShapeDtypeStruct((n, capacity, columns), jnp.bfloat16),
        in_specs=[vmem],
        out_specs=vmem,
        scratch_shapes=[
            pltpu.VMEM((n, 2, n, capacity, quarter), jnp.bfloat16),
            stack,
            stack,
            stack,
            stack,
            stack,
            pltpu.SemaphoreType.DMA((n, 2)),
            pltpu.SemaphoreType.DMA((n, 2)),
            pltpu.SemaphoreType.DMA((n,)),
            pltpu.SemaphoreType.DMA((n,)),
            pltpu.SemaphoreType.DMA((n, n)),
            pltpu.SemaphoreType.DMA((n, n)),
            pltpu.SemaphoreType.DMA((n, n)),
            pltpu.SemaphoreType.DMA((n, n)),
        ],
        compiler_params=pltpu.CompilerParams(
            collective_id=1, has_side_effects=True, vmem_limit_bytes=40 * 1024 * 1024
        ),
    )(second)


def exchange(second, dp_count, tensor_count, capacity):
    if dp_count == tensor_count == 4 and capacity % 16 == 0 and second.shape[1] % 512 == 0:
        return place(second.reshape(dp_count, dp_count, capacity, -1)).reshape(dp_count * capacity, -1)
    second = lax.psum_scatter(second, "tensor", scatter_dimension=1, tiled=True)
    columns = second.shape[1]
    second = second.reshape(dp_count, dp_count, capacity, columns)
    second = lax.all_to_all(second, "dp", split_axis=1, concat_axis=0, tiled=False)
    blocks = dp_count // tensor_count
    second = second.reshape(tensor_count, blocks, dp_count * capacity, columns)
    second = lax.all_to_all(second, "tensor", split_axis=0, concat_axis=0, tiled=True)
    return second.transpose(2, 1, 0, 3).reshape(dp_count * capacity, -1)


def local(
    patches,
    grids,
    dest,
    norm_gain,
    qkv_weight,
    qkv_bias,
    proj_weight,
    proj_bias,
    merge_gain,
    w_first,
    b_first,
    w_second,
    b_second,
    text_embed,
):
    rows_dev, width = patches.shape
    images_dev = grids.shape[0]
    heads_dev = qkv_weight.shape[2] // HEAD_DIM
    dp_count = lax.axis_size("dp")
    tensor_count = lax.axis_size("tensor")
    seq_rows = text_embed.shape[0]
    capacity = images_dev * (MERGED // dp_count)
    live_count = grids[:, 0] * grids[:, 1]
    permute, slot_rows = placement(dest, live_count, dp_count, seq_rows, capacity)
    arrived_rows = lax.all_to_all(
        slot_rows.reshape(dp_count, capacity), "dp", split_axis=0, concat_axis=0, tiled=True
    ).reshape(-1)

    attended = attention(patches, live_count, norm_gain, qkv_weight, qkv_bias, images_dev, heads_dev)
    partial_value = jnp.dot(attended, proj_weight, preferred_element_type=jnp.float32).astype(jnp.bfloat16)
    summed = lax.psum_scatter(partial_value, "tensor", scatter_dimension=0, tiled=True).astype(jnp.float32)
    part = rows_dev // tensor_count
    own = lax.dynamic_slice_in_dim(patches, lax.axis_index("tensor") * part, part, 0)
    resid = own.astype(jnp.float32) + summed + proj_bias
    merged_in = rms_scale(resid, merge_gain).astype(jnp.bfloat16).reshape(part // 4, 4 * width)
    sliced = lax.all_to_all(
        merged_in.reshape(part // 4, dp_count, 4 * width // dp_count), "dp", split_axis=1, concat_axis=0, tiled=False
    )
    received = lax.all_gather(sliced, "tensor", axis=1, tiled=False)
    received = received.reshape(-1, 4 * width // dp_count)
    second = merger(received, w_first, b_first, permute, w_second)
    visual = exchange(second, dp_count, tensor_count, capacity)
    visual = (visual.astype(jnp.float32) + b_second).astype(jnp.bfloat16)
    hit = jnp.arange(seq_rows, dtype=jnp.int32)[:, None] == arrived_rows[None, :]
    placed = jnp.dot(hit.astype(jnp.bfloat16), visual, preferred_element_type=jnp.float32).astype(jnp.bfloat16)
    return jnp.where(jnp.any(hit, axis=1)[:, None], placed, text_embed)


def fused_kernel(
    seq_rows, lags,
    patches_hbm, grids, dest, gain, wqkv_hbm, bqkv, wproj_hbm, bproj, mgain, w1_hbm, bias, w2_hbm, bias2, text_hbm,
    final,
    patches, wqkv, bpad, wproj, target, normed, raws, qs, ks, vs, att_f32, att_out, att_in, slices, rows_tbl, arrived, hit_out, any_out, out, x,
    w1, w2, own, to_r, to_l, from_l, from_r, hidden, keep, give, from_mate, cross, from_across, ready, landed,
    load_sem, head_sem, tbl_send, tbl_recv, pm_send, pm_recv, pa_send, pa_recv, py_send, py_recv, pd_send, pd_recv,
    att_send, att_recv, z_send, fm_send, fa_send, x_recv,
    r_send, r_recv, l_send, l_recv, mate_send, mate_recv, across_send, across_recv,
    row_send, row_recv, end_send, end_recv,
):
    n, _, sides, few, width = x.shape
    nt = 2 * sides
    rows = patches.shape[0]
    block = rows // n
    half = block // sides
    merged = dest.shape[1]
    heads = qs.shape[0]
    lanes = qs.shape[2]
    count, _, wide = own.shape
    steps = count // n
    pieces = steps // sides
    pair = n // sides
    quarter = keep.shape[3]
    piece = ready.shape[4]
    row, me, group = lax.axis_index("dp"), lax.axis_index("tensor"), lax.axis_index("groups")
    core, side = me % 2, me // 2
    mate, across = side * 2 + 1 - core, (1 - side) * 2 + core
    left, right = lax.max(row - 1, 0), lax.min(row + 1, n - 1)
    has_left, has_right = row > 0, row < n - 1
    bf16, f32 = jnp.bfloat16, jnp.float32

    load_x = pltpu.make_async_copy(patches_hbm, patches, load_sem.at[0])
    load_p = pltpu.make_async_copy(wproj_hbm, wproj.at[me], load_sem.at[1])
    load_1 = pltpu.make_async_copy(w1_hbm, w1, load_sem.at[2])
    load_2 = pltpu.make_async_copy(w2_hbm, w2, load_sem.at[3])
    load_t = pltpu.make_async_copy(text_hbm, final, load_sem.at[4])
    load_w = [
        pltpu.make_async_copy(
            wqkv_hbm.at[j, h * HEAD_DIM:(h + 1) * HEAD_DIM], wqkv.at[j, h * lanes:h * lanes + HEAD_DIM],
            head_sem.at[j, h])
        for j in range(3) for h in range(heads)
    ]
    load_p.start()
    load_x.start()
    for load in load_w:
        load.start()

    barrier = pltpu.get_barrier_semaphore()
    for k in range(1, nt):
        pl.semaphore_signal(barrier, inc=1, device_id={"tensor": (me + k) % nt}, device_id_type=MESH)
    for k in range(1, n):
        pl.semaphore_signal(barrier, inc=1, device_id={"dp": (row + k) % n}, device_id_type=MESH)
    pl.semaphore_signal(barrier, inc=1, device_id={"groups": 1 - group}, device_id_type=MESH)

    pl.semaphore_wait(barrier, nt - 1 + n - 1 + 1)

    def remote(source, to, send, recv, device):
        return pltpu.make_async_remote_copy(source, to, send, recv, device_id=device, device_id_type=MESH)

    strips = pa_send.shape[0]
    span = wproj.shape[1] // (2 * strips)

    def strip(g, a):
        return pl.ds(pl.multiple_of((g * strips + a) * span, span), span)

    def same(ref, send, recv, device):
        return remote(ref, ref, send, recv, device)

    proj_mate = same(wproj.at[me], pm_send, pm_recv, {"tensor": mate})
    proj_across = [
        same(wproj.at[me, strip(group, a)], pa_send.at[a], pa_recv.at[a], {"tensor": across}) for a in range(strips)]

    def proj_got(a):
        return same(wproj.at[across, strip(group, a)], pa_send.at[a], pa_recv.at[a], {"tensor": across})

    def proj_peer(a):
        return same(wproj.at[across, strip(group, a)], py_send.at[a], py_recv.at[a], {"groups": 1 - group})

    def proj_peer_got(a):
        return same(wproj.at[across, strip(1 - group, a)], py_send.at[a], py_recv.at[a], {"groups": 1 - group})

    def proj_diag(g, a, at):
        return same(wproj.at[across, strip(g, a)], pd_send.at[at, a], pd_recv.at[at, a], {"tensor": mate})

    def proj_pass(a):
        proj_got(a).wait_recv()
        proj_peer(a).start()
        proj_diag(group, a, 0).start()

    load_p.wait()
    for copy in proj_across:
        copy.start()
    proj_mate.start()

    live = grids[0, 0] * grids[0, 1]
    dest_row = dest[...].astype(f32)

    def shards(value):
        total = jnp.zeros_like(value)
        for s in range(1, n):
            total += jnp.where(value >= float(s * seq_rows), 1.0, 0.0)
        return total

    square = (merged, merged)
    first_at = lax.broadcasted_iota(jnp.int32, square, 0)
    second_at = lax.broadcasted_iota(jnp.int32, square, 1)
    dest_col = jnp.sum(jnp.where(first_at == second_at, dest_row, 0.0), axis=1, keepdims=True)
    shard_row, shard_col = shards(dest_row), shards(dest_col)
    rank_col = jnp.sum(
        jnp.where((shard_row == shard_col) & (second_at < first_at), 1.0, 0.0), axis=1, keepdims=True)
    live_col = lax.broadcasted_iota(jnp.int32, (merged, 1), 0) * 4 < live
    rank_i, shard_i = rank_col.astype(jnp.int32), shard_col.astype(jnp.int32)
    slot_i = rank_i // piece * block + shard_i // 2 * half + shard_i % 2 * piece + rank_i % piece
    base_col = jnp.where(live_col, slot_i, -rows).astype(f32)

    ones_at = lax.broadcasted_iota(jnp.int32, (1, lanes), 1) == HEAD_DIM
    for j in range(3):
        for h in range(heads):
            bpad[j:j + 1, h * lanes:(h + 1) * lanes] = jnp.where(ones_at, 0.0 if j == 1 else 1.0, 0.0)
            bpad[j:j + 1, h * lanes:h * lanes + HEAD_DIM] = bqkv[j:j + 1, h * HEAD_DIM:(h + 1) * HEAD_DIM]
            wqkv[j, h * lanes + HEAD_DIM:(h + 1) * lanes, :] = jnp.zeros((lanes - HEAD_DIM, width), bf16)

    patch_at = lax.broadcasted_iota(jnp.int32, (1, rows), 1)
    row4 = lax.broadcasted_iota(jnp.int32, (merged, 1), 0) * 4
    inside = (patch_at >= row4) & (patch_at < row4 + 4)
    base_row = jnp.sum(jnp.where(inside, base_col, 0.0), axis=0, keepdims=True).astype(jnp.int32)
    target[...] = jnp.broadcast_to(base_row + patch_at % 4 * few, target.shape)

    slots = rows_tbl.shape[2]
    code_col = jnp.where(live_col, shard_col * slots + rank_col + (row * (slots // n)).astype(f32), -1.0)
    lane_at = lax.broadcasted_iota(jnp.int32, (merged, n * slots), 1).astype(f32)
    local_col = dest_col - shard_col * seq_rows
    table = jnp.sum(jnp.where(lane_at == code_col, local_col + 1.0, 0.0), axis=0, keepdims=True) - 1.0
    for s in range(n):
        rows_tbl[s] = jnp.broadcast_to(table[:, s * slots:(s + 1) * slots], (8, slots)).astype(jnp.int32)
    arrived[row] = rows_tbl[row]

    def send_table(k):
        to = (row + k) % n
        return remote(rows_tbl.at[to], arrived.at[row], tbl_send.at[k], tbl_recv.at[row], {"dp": to})

    for k in range(1, n):
        send_table(k).start()

    load_x.wait()
    for load in load_w:
        load.wait()
    load_1.start()
    load_2.start()
    load_t.start()

    mask_at = lax.broadcasted_iota(jnp.int32, (block, lanes), 1) == HEAD_DIM

    def project(b, carry):
        @pl.when(b >= 1)
        def _():
            proj_pass(lax.max(b, 1) - 1)

        at = pl.ds(pl.multiple_of(b * block, block), block)
        hit = jnp.where(
            target[0:1, :] == lax.broadcasted_iota(jnp.int32, (block, rows), 0) + b * block, 1.0, 0.0)
        valid = jnp.sum(hit, axis=1, keepdims=True)
        raw = jnp.dot(hit.astype(bf16), patches[...], preferred_element_type=f32)
        for s in range(sides):
            raws[b, s] = raw[s * half:(s + 1) * half, :].astype(bf16)
        normed[...] = rms_scale(raw, gain[...].reshape(1, width)).astype(bf16)
        for j, store in enumerate((qs, ks, vs)):
            acc = lax.dot_general(
                normed[...], wqkv[j], (((1,), (1,)), ((), ())), preferred_element_type=f32) + bpad[j:j + 1, :]
            for h in range(heads):
                value = acc[:, h * lanes:(h + 1) * lanes]
                if j == 1:
                    value = jnp.where(mask_at, jnp.where(valid > 0.5, 0.0, -1e30), value)
                store[h, at, :] = value.astype(bf16)
        return carry

    lax.fori_loop(0, n, project, 0)

    proj_pass(n - 1)

    scale = math.log2(math.e) / math.sqrt(HEAD_DIM)

    def att_to(b, s):
        return remote(
            att_out.at[b, s], att_in.at[b // 2, me], att_send.at[b, s], att_recv.at[b // 2, me],
            {"tensor": s * 2 + b % 2})

    def att_got(b, source):
        return remote(
            att_out.at[b, 0], att_in.at[b // 2, source], att_send.at[b, 0], att_recv.at[b // 2, source],
            {"tensor": mate})

    def z_to(b, k):
        to = (row + k) % n
        return remote(
            slices.at[b // 2, to], x.at[b, row, side], z_send.at[b // 2, k], x_recv.at[b, row, side], {"dp": to})

    def to_mate_x(b, s, i):
        return same(x.at[b, i, s], fm_send.at[b // 2, i, s], x_recv.at[b, i, s], {"tensor": mate})

    def to_across_x(b, i):
        return same(x.at[b, i, side], fa_send.at[b // 2, i], x_recv.at[b, i, side], {"tensor": across})

    def x_got(b, s, i):
        return same(x.at[b, i, s], fm_send.at[b // 2, i, s], x_recv.at[b, i, s], {"tensor": mate})

    def forward(b):
        for k in range(1, n):
            source = (row + n - k) % n
            x_got(b, side, source).wait_recv()
            to_across_x(b, source).start()
            to_mate_x(b, side, source).start()

    def attend(it, carry):
        @pl.when(it < n)
        def _():
            b = lax.min(it, n - 1)
            at = pl.ds(pl.multiple_of(b * block, block), block)
            for h in range(heads):
                scores = lax.dot_general(
                    qs[h, at, :], ks[h], (((1,), (1,)), ((), ())), preferred_element_type=f32)
                peak = jnp.max(scores, axis=1, keepdims=True)
                weights = jnp.exp2((scores - peak) * scale).astype(bf16)
                mixed = jnp.dot(weights, vs[h], preferred_element_type=f32)
                mixed = mixed * (1.0 / mixed[:, HEAD_DIM:HEAD_DIM + 1])
                att_f32[:, h * HEAD_DIM:(h + 1) * HEAD_DIM] = mixed[:, 0:HEAD_DIM]
            for s in range(sides):
                att_out[b, s] = att_f32[s * half:(s + 1) * half, :].astype(bf16)
                owner = s * 2 + b % 2

                @pl.when(owner != me)
                def _():
                    att_to(b, s).start()

                @pl.when(owner == me)
                def _():
                    att_in[b // 2, me] = att_out[b, s]

        @pl.when(it == 0)
        def _():
            for a in range(n, strips):
                proj_pass(a)
            for a in range(n):
                proj_peer_got(a).wait_recv()
                proj_diag(1 - group, a, 1).start()

        @pl.when(it == 1)
        def _():
            for a in range(n, strips):
                proj_peer_got(a).wait_recv()
                proj_diag(1 - group, a, 1).start()
            proj_mate.wait_recv()
            for a in range(strips):
                proj_diag(group, a, 0).wait_recv()
                proj_diag(1 - group, a, 1).wait_recv()

        @pl.when((it == n - 1) & (core == 0))
        def _():
            forward(0)

        last = lax.max(it, 1) - 1

        @pl.when((it >= 1) & (last % 2 == core))
        def _():
            for k in range(1, nt):
                att_got(last, (me + k) % nt).wait_recv()
            total = raws[last, side].astype(f32) + bproj[...].reshape(1, width)
            for t in range(nt):
                total += jnp.dot(att_in[last // 2, t], wproj[t], preferred_element_type=f32)
            done = rms_scale(total, mgain[...].reshape(1, width)).astype(bf16)
            for k in range(n):
                slices[last // 2, k] = done[k * few:(k + 1) * few, :]
            for k in range(n - 1, 0, -1):
                z_to(last, k).start()
            x[last, row, side] = slices[last // 2, row]
            to_across_x(last, row).start()
            to_mate_x(last, side, row).start()

        return carry

    lax.fori_loop(0, n + 1, attend, 0)

    def forward_across(b):
        for k in range(n):
            source = (row + n - k) % n
            x_got(b, 1 - side, source).wait_recv()
            to_mate_x(b, 1 - side, source).start()

    def await_x(b):
        @pl.when(b % 2 != core)
        def _():
            for s in range(sides):
                for i in range(n):
                    x_got(b, s, i).wait_recv()

    def go_right(c):
        return remote(to_r.at[c], from_l.at[c], r_send.at[c], r_recv.at[c], {"dp": right})

    def go_left(c):
        return remote(to_l.at[c], from_r.at[c], l_send.at[c], l_recv.at[c], {"dp": left})

    def first(b, j):
        columns = pl.ds(pl.multiple_of(j * wide, wide), wide)
        partial = jnp.dot(x[b].reshape(block, width), w1[:, columns], preferred_element_type=f32)
        for h in range(sides):
            own[b * steps + h * pieces + j] = partial[h * half:(h + 1) * half, :]

    def begin(c):
        @pl.when(row == 0)
        def _():
            to_r[c] = own[c].astype(bf16)
            go_right(c).start()

        @pl.when(row == n - 1)
        def _():
            to_l[c] = own[c].astype(bf16)
            go_left(c).start()

    def relay(stage, c):
        @pl.when(row == stage)
        def _():
            go_right(c).wait_recv()
            to_r[c] = (own[c] + from_l[c].astype(f32)).astype(bf16)
            go_right(c).start()

        @pl.when(row == n - 1 - stage)
        def _():
            go_left(c).wait_recv()
            to_l[c] = (own[c] + from_r[c].astype(f32)).astype(bf16)
            go_left(c).start()

    def activate(c):
        columns = pl.ds(pl.multiple_of(c % pieces * wide, wide), wide)

        @pl.when(row == n - 1)
        def _():
            go_right(c).wait_recv()

        @pl.when(row == 0)
        def _():
            go_left(c).wait_recv()

        @pl.when(has_left)
        def _():
            own[c] += from_l[c].astype(f32)

        @pl.when(has_right)
        def _():
            own[c] += from_r[c].astype(f32)

        value = own[c] + bias[columns].reshape(1, wide)
        hidden[c // pieces % 2, :, columns] = (0.5 * value * (1.0 + lax.erf(value * math.sqrt(0.5)))).astype(bf16)

    def columns_of(s, c):
        return pl.ds(pl.multiple_of((s * 2 + c) * quarter, quarter), quarter)

    def to_mate(b, s):
        return remote(give.at[b, s], from_mate.at[b, s], mate_send.at[b, s], mate_recv.at[b, s], {"tensor": mate})

    def to_across(g, p):
        return remote(
            cross.at[g, p], from_across.at[g, p], across_send.at[g, p], across_recv.at[g, p], {"tensor": across})

    def to_row(g, p, k):
        to = (row + k) % n
        return remote(
            ready.at[g, p, to], landed.at[g, p, row], row_send.at[g, p, k], row_recv.at[g, p, row], {"dp": to})

    def quarter_of(t):
        return pl.ds(pl.multiple_of(t * quarter, quarter), quarter)

    thin = cross.shape[3]

    def columns_in(t, p):
        return pl.ds(pl.multiple_of(t * quarter + p * thin, thin), thin)

    def to_end(g, p, d):
        at = pl.ds(g % sides * pair, pair)
        return remote(
            landed.at[g, p, d], out.at[at, g // sides, :, columns_in(me, p)], end_send.at[g, p, d],
            end_recv.at[g, p, me], {"tensor": d})

    def product(g, s, c):
        return jnp.dot(hidden[g % 2], w2[:, columns_of(s, c)], preferred_element_type=f32)

    def second(g):
        give[g, 1 - side] = product(g, 1 - side, 1 - core).astype(bf16)
        to_mate(g, 1 - side).start()
        keep[g % 2, 1 - side] = product(g, 1 - side, core)

    def chip_sum(g):
        to_mate(g, 1 - side).wait_recv()
        for p in range(2):
            at = slice(p * thin, (p + 1) * thin)
            cross[g, p] = (
                keep[g % 2, 1 - side, :, at] + from_mate[g, 1 - side, :, at].astype(f32)).astype(bf16)
            to_across(g, p).start()
        give[g, side] = product(g, side, 1 - core).astype(bf16)
        to_mate(g, side).start()
        keep[g % 2, side] = product(g, side, core)

    def spread(g):
        to_mate(g, side).wait_recv()
        for p in range(2):
            at = slice(p * thin, (p + 1) * thin)
            value = keep[g % 2, side, :, at] + from_mate[g, side, :, at].astype(f32)
            to_across(g, p).wait_recv()
            value = (value + from_across[g, p].astype(f32)).astype(bf16)
            for s in range(n):
                for i in range(pair):
                    begin_at = (i * n + s) * piece
                    ready[g, p, s, i] = value[begin_at:begin_at + piece, :]
            for k in range(n - 1, 0, -1):
                to_row(g, p, k).start()
            landed[g, p, row] = ready[g, p, row]

    def deliver(g):
        for p in range(2):
            for k in range(n):
                source = (row + n - k) % n
                if k:
                    remote(
                        ready.at[g, p, 0], landed.at[g, p, source], row_send.at[g, p, 0],
                        row_recv.at[g, p, source], {"dp": left},
                    ).wait_recv()

                @pl.when(source == me)
                def _():
                    out[pl.ds(g % sides * pair, pair), g // sides, :, columns_in(me, p)] = landed[g, p, source]

                @pl.when(source != me)
                def _():
                    to_end(g, p, source).start()

    lead, hop, fill, offsets = lags

    @pl.when(core == 0)
    def _():
        forward_across(0)

    @pl.when(core == 1)
    def _():
        forward(1)

    for k in range(1, n):
        source = (row + n - k) % n
        remote(rows_tbl.at[0], arrived.at[source], tbl_send.at[0], tbl_recv.at[source], {"dp": source}).wait_recv()

    at_slot = arrived[0, 0:1, :]
    for i in range(1, n):
        at_slot = jnp.maximum(at_slot, arrived[i, 0:1, :])
    match = jnp.where(
        lax.broadcasted_iota(jnp.int32, hit_out.shape, 0) == at_slot, 1.0, 0.0)
    hit_out[...] = match.astype(bf16)
    any_out[...] = jnp.broadcast_to(jnp.max(match, axis=1, keepdims=True), any_out.shape)

    load_1.wait()
    load_2.wait()
    load_t.wait()
    after = tuple(zip(offsets, (second, chip_sum, spread, deliver)))

    def step(u, carry):
        @pl.when((u < count) & (u % steps < pieces))
        def _():
            @pl.when(u % steps == 0)
            def _():
                await_x(u // steps)

            first(u // steps, u % steps)

        @pl.when(u < count)
        def _():
            begin(u)

        @pl.when((u == 1) & (core == 1))
        def _():
            forward_across(1)

        @pl.when(u == 8)
        def _():
            forward(2 + core)

        @pl.when(u == 12)
        def _():
            forward_across(2 + core)

        for stage in range(1, n - 1):
            late = lead + (stage - 1) * hop

            @pl.when((u >= late) & (u < count + late))
            def _():
                relay(stage, u - late)

        @pl.when((u >= lead + fill) & (u < count + lead + fill))
        def _():
            activate(u - lead - fill)

        for offset, work in after:
            late = lead + fill + offset + pieces - 1

            @pl.when((u >= late) & (u < count + late) & (lax.max(u - late, 0) % pieces == 0))
            def _():
                work((u - late) // pieces)

        return carry

    lax.fori_loop(0, count + lead + fill + offsets[-1], step, 0)

    for k in range(nt):
        source = (me + k) % nt

        if k:
            def gather(g, carry):
                for p in range(2):
                    remote(
                        landed.at[g, p, 0],
                        out.at[pl.ds(g % sides * pair, pair), g // sides, :, columns_in(source, p)],
                        end_send.at[g, p, 0], end_recv.at[g, p, source], {"tensor": mate},
                    ).wait_recv()
                return carry

            lax.fori_loop(0, n * sides, gather, 0)
        columns = pl.ds(pl.multiple_of(source * quarter, quarter), quarter)
        rows_in = out[:, :, :, columns].reshape(hit_out.shape[1], quarter)
        placed = jnp.dot(hit_out[...], rows_in, preferred_element_type=f32) + bias2[columns].reshape(1, quarter)
        final[:, columns] = jnp.where(any_out[:, 0:1] > 0.5, placed.astype(bf16), final[:, columns])

    def drain(c, carry):
        @pl.when(has_right)
        def _():
            go_right(c).wait_send()

        @pl.when(has_left)
        def _():
            go_left(c).wait_send()

        return carry

    lax.fori_loop(0, count, drain, 0)
    proj_mate.wait_send()
    for a in range(strips):
        proj_across[a].wait_send()
        proj_peer(a).wait_send()
        proj_diag(group, a, 0).wait_send()
        proj_diag(1 - group, a, 1).wait_send()
    for k in range(1, n):
        send_table(k).wait_send()
    for b in range(n):
        for s in range(sides):
            @pl.when(s * 2 + b % 2 != me)
            def _():
                att_to(b, s).wait_send()


    def drain_place(g, carry):
        for p in range(2):
            to_mate(g, p).wait_send()
            to_across(g, p).wait_send()
            for k in range(1, n):
                to_row(g, p, k).wait_send()
                to_end(g, p, (me + k) % nt).wait_send()
        return carry

    lax.fori_loop(0, n * sides, drain_place, 0)
    for q in range(2):
        b = 2 * q + core
        for k in range(1, n):
            z_to(b, k).wait_send()
        for i in range(n):
            to_across_x(b, i).wait_send()
            for s in range(sides):
                to_mate_x(b, s, i).wait_send()


def fused(
    patches, grids, dest, norm_gain, qkv_weight, qkv_bias, proj_weight, proj_bias, merge_gain,
    w_first, b_first, w_second, b_second, text_embed,
):
    n, nt = lax.axis_size("dp"), lax.axis_size("tensor")
    seq_rows = text_embed.shape[0]
    sides = nt // 2
    rows, width = patches.shape
    span = qkv_weight.shape[2]
    heads = span // HEAD_DIM
    block = rows // n
    half = block // sides
    few = half // 4
    hidden, columns = w_second.shape
    wide, lanes = 256, 128
    pieces = hidden // wide
    steps = pieces * sides
    count = n * steps
    quarter = columns // nt
    piece = few // 2
    any_space = pl.BlockSpec(memory_space=pl.ANY)
    vmem = pl.BlockSpec(memory_space=pltpu.VMEM)
    smem = pl.BlockSpec(memory_space=pltpu.SMEM)
    dma = pltpu.SemaphoreType.DMA
    bf16, f32 = jnp.bfloat16, jnp.float32
    heads_shape = pltpu.VMEM((heads, rows, lanes), bf16)
    stack = pltpu.VMEM((count, half, wide), bf16)
    units = n * sides
    strips = span // 64
    slots = n * n * piece
    tiles = pltpu.VMEM((units, 2, half, quarter), bf16)
    one = pltpu.VMEM((units, 2, half, quarter // 2), bf16)
    moved = pltpu.VMEM((units, 2, n, n // sides, piece, quarter // 2), bf16)
    lags = (4, 3, 6, (0, 1, 6, 12))
    return pl.pallas_call(
        functools.partial(fused_kernel, seq_rows, lags),
        out_shape=jax.ShapeDtypeStruct(text_embed.shape, bf16),
        in_specs=[
            any_space, smem, vmem, vmem, any_space, vmem, any_space, vmem, vmem, any_space, vmem, any_space, vmem,
            any_space],
        out_specs=vmem,
        scratch_shapes=[
            pltpu.VMEM((rows, width), bf16),
            pltpu.VMEM((3, heads * lanes, width), bf16),
            pltpu.VMEM((3, heads * lanes), f32),
            pltpu.VMEM((nt, span, width), bf16),
            pltpu.VMEM((8, rows), jnp.int32),
            pltpu.VMEM((block, width), bf16),
            pltpu.VMEM((n, sides, half, width), bf16),
            heads_shape, heads_shape, heads_shape,
            pltpu.VMEM((block, span), f32),
            pltpu.VMEM((n, sides, half, span), bf16),
            pltpu.VMEM((n // 2, nt, half, span), bf16),
            pltpu.VMEM((n // 2, n, few, width), bf16),
            pltpu.VMEM((n, 8, slots), jnp.int32),
            pltpu.VMEM((n, 8, slots), jnp.int32),
            pltpu.VMEM((seq_rows, slots), bf16),
            pltpu.VMEM((seq_rows, lanes), f32),
            pltpu.VMEM((n, n, piece, columns), bf16),
            pltpu.VMEM((n, n, sides, few, width), bf16),
            pltpu.VMEM(w_first.shape, bf16),
            pltpu.VMEM(w_second.shape, bf16),
            pltpu.VMEM((count, half, wide), f32),
            stack, stack, stack, stack,
            pltpu.VMEM((2, half, hidden), bf16),
            pltpu.VMEM((2, 2, half, quarter), f32),
            tiles, tiles, one, one, moved, moved,
            dma((5,)), dma((3, heads)), dma((n,)), dma((n,)), dma, dma, dma((strips,)), dma((strips,)), dma((strips,)),
            dma((strips,)), dma((2, strips)), dma((2, strips)),
            dma((n, sides)), dma((n // 2, nt)), dma((n // 2, n)), dma((n // 2, n, sides)), dma((n // 2, n)),
            dma((n, n, sides)),
            dma((count,)), dma((count,)), dma((count,)), dma((count,)),
            dma((units, 2)), dma((units, 2)), dma((units, 2)), dma((units, 2)), dma((units, 2, n)), dma((units, 2, n)),
            dma((units, 2, nt)), dma((units, 2, nt)),
        ],
        compiler_params=pltpu.CompilerParams(
            collective_id=2, has_side_effects=True, vmem_limit_bytes=63 * 1024 * 1024
        ),
    )(
        patches, grids, dest, norm_gain, qkv_weight.swapaxes(1, 2), qkv_bias, proj_weight, proj_bias, merge_gain,
        w_first, b_first, w_second, b_second, text_embed,
    )


def local_fast(
    patches,
    grids,
    dest,
    norm_gain,
    qkv_weight,
    qkv_bias,
    proj_weight,
    proj_bias,
    merge_gain,
    w_first,
    b_first,
    w_second,
    b_second,
    text_embed,
):
    return fused(
        patches, grids, dest, norm_gain, qkv_weight, qkv_bias, proj_weight, proj_bias, merge_gain,
        w_first, b_first, w_second, b_second, text_embed)


def fits(patches, grids, dest, qkv_weight, w_first, w_second):
    n, nt = lax.axis_size("dp"), lax.axis_size("tensor")
    rows, width = patches.shape
    return (
        n == nt == 4
        and lax.axis_size("groups") == 2
        and grids.shape[0] == 1
        and rows == PATCHES
        and dest.shape[1] == MERGED
        and w_first.shape[0] == width
        and w_second.shape[0] % 256 == 0
        and w_second.shape[1] % 512 == 0
        and qkv_weight.shape[2] % 64 == 0
        and qkv_weight.shape[2] // 64 > n
    )


def chosen(*args):
    run = local_fast if fits(args[0], args[1], args[2], args[4], args[9], args[11]) else local
    return run(*args)


def solution(mesh):
    in_specs = (
        P(("groups", "dp"), None),
        P(("groups", "dp"), None),
        P(("groups", "dp"), None),
        P(),
        P(None, None, "tensor"),
        P(None, "tensor"),
        P("tensor", None),
        P(),
        P(),
        P("dp", "tensor"),
        P("tensor"),
        P("tensor", "dp"),
        P("tensor"),
        P(("groups", "dp"), "tensor"),
    )
    out_specs = P(("groups", "dp"), "tensor")
    return jax.shard_map(chosen, mesh=mesh, in_specs=in_specs, out_specs=out_specs, check_vma=False)
```
